8 devices in a mesh: bz: 2 (over z, y), by: 2 (over x), bx: 2 (over core).
Axes of the slice: x: 2, y: 2, z: 1, core: 2. Of those that a mesh axis runs over, the one named last changes fastest.
Arguments:
- positions: float32 [13824, 3], P(('bz', 'by', 'bx'))
- velocities: float32 [13824, 3], P(('bz', 'by', 'bx'))
- forces: float32 [13824, 3], P(('bz', 'by', 'bx'))
- atom_ids: int32 [13824], P(('bz', 'by', 'bx'))
- valid_mask: int32 [13824], P(('bz', 'by', 'bx'))
Outputs:
- output 1: float32 [13824, 3], P(('bz', 'by', 'bx'))
- output 2: float32 [13824, 3], P(('bz', 'by', 'bx'))
- output 3: float32 [13824, 3], P(('bz', 'by', 'bx'))
- output 4: int32 [13824], P(('bz', 'by', 'bx'))
- output 5: int32 [13824], P(('bz', 'by', 'bx'))
- output 6: float32 [], replicated
All inputs are finite; a program needn't handle non-finite values.
Results may differ from the reference program's by a relative error of at most 0.001.
Values sent between devices are 32-bit elements.
A program may use at most 1 GiB of HBM per device.

```python
import jax
import jax.numpy as jnp
import numpy as np
from jax import lax

NUM_X = 2
NUM_Y = 2
NUM_Z = 2
SITES = 12
CUT_TENTHS = 25
NUM_BRICKS = NUM_X * NUM_Y * NUM_Z
CAPACITY = SITES * SITES * SITES
TOTAL_SLOTS = NUM_BRICKS * CAPACITY
DENSITY = 0.8442
SPACING = (1.0 / DENSITY) ** (1.0 / 3.0)
BRICK_SIDE = SITES * SPACING
RCUT = CUT_TENTHS / 10.0
TIME_STEP = 0.005


def brick_linear(coords):
    return (coords[..., 2] * NUM_Y + coords[..., 1]) * NUM_X + coords[..., 0]


def site_linear(coords, grid_dims):
    return (coords[..., 2] * grid_dims[1] + coords[..., 1]) * grid_dims[0] + coords[..., 0]


def neighbour_table():
    choices = [[-1, 0, 1] if axis_len >= 3 else [0, 1] for axis_len in (NUM_X, NUM_Y, NUM_Z)]
    offset_rows = [[step_x, step_y, step_z] for step_z in choices[2] for step_y in choices[1] for step_x in choices[0]]
    return np.array(offset_rows, dtype=np.int32)


def pair_terms(dist_sq, pair_mask):
    safe_sq = jnp.where(pair_mask, dist_sq, 1.0)
    inv_r2 = 1.0 / safe_sq
    inv_r6 = inv_r2 * inv_r2 * inv_r2
    pair_dist = jnp.sqrt(safe_sq)
    cut_inv6 = RCUT ** -6
    u_cut = 4.0 * (cut_inv6 * cut_inv6 - cut_inv6)
    du_cut = (-48.0 * cut_inv6 * cut_inv6 + 24.0 * cut_inv6) / RCUT
    energy = 4.0 * (inv_r6 * inv_r6 - inv_r6) - u_cut - (pair_dist - RCUT) * du_cut
    f_over_r = (48.0 * inv_r6 * inv_r6 - 24.0 * inv_r6) * inv_r2 + du_cut / pair_dist
    return jnp.where(pair_mask, energy, 0.0), jnp.where(pair_mask, f_over_r, 0.0)


def setup_inputs(seed: int = 0) -> dict:
    rng_keys = jax.random.split(jax.random.key(seed), 10)
    brick_ids = jnp.arange(NUM_BRICKS)
    brick_xyz = jnp.stack([brick_ids % NUM_X, (brick_ids // NUM_X) % NUM_Y, brick_ids // (NUM_X * NUM_Y)], axis=-1)
    local_idx = jnp.arange(CAPACITY)
    local_xyz = jnp.stack([local_idx % SITES, (local_idx // SITES) % SITES, local_idx // (SITES * SITES)], axis=-1)
    brick_dims = jnp.array([NUM_X, NUM_Y, NUM_Z])
    grid_dims = brick_dims * SITES
    site_xyz = brick_xyz[:, None, :] * SITES + local_xyz[None, :, :]
    site_global = site_linear(site_xyz, grid_dims)
    centre = grid_dims // 3
    radius = jnp.min(grid_dims) * 3 // 8
    rel_site = (site_xyz - centre + grid_dims // 2) % grid_dims - grid_dims // 2
    inside = jnp.sum(rel_site * rel_site, axis=-1) <= radius * radius
    vapour = jax.random.randint(rng_keys[0], (NUM_BRICKS, CAPACITY), 0, 8) == 0
    occupied = inside | vapour
    face_bits = jax.random.randint(rng_keys[1], (NUM_BRICKS, 3), 0, 2)
    face_bits = face_bits.at[0].set(1)
    unit_steps = jnp.eye(3, dtype=jnp.int32)
    lower_nbr = brick_linear((brick_xyz[:, None, :] - unit_steps[None, :, :]) % brick_dims)
    minus_ok = face_bits[lower_nbr, jnp.arange(3)[None, :]] == 0
    plus_ok = face_bits == 1
    at_top = local_xyz == SITES - 1
    bottom = local_xyz == 0
    direction = (at_top[None] & plus_ok[:, None, :]).astype(jnp.int32) - (bottom[None] & minus_ok[:, None, :]).astype(jnp.int32)
    border = at_top | bottom
    eligible = jnp.all((~border[None]) | (direction != 0), axis=-1) & jnp.any(direction != 0, axis=-1)
    lottery = jax.random.randint(rng_keys[2], (NUM_BRICKS, CAPACITY), 0, 4) == 0
    forced = (brick_ids == 0)[:, None]
    migrant = eligible & ((lottery & occupied) | forced)
    vacant = jnp.zeros((TOTAL_SLOTS,), jnp.int32)
    for subset_bits in range(1, 8):
        subset_sel = jnp.array([subset_bits & 1, (subset_bits >> 1) & 1, (subset_bits >> 2) & 1], jnp.int32)
        site_step = direction * subset_sel
        is_hit = migrant & jnp.all((subset_sel == 0) | (direction != 0), axis=-1)
        target = site_linear((site_xyz + site_step) % grid_dims, grid_dims)
        vacant = vacant.at[jnp.where(is_hit, target, TOTAL_SLOTS)].max(1, mode="drop")
    vacated = vacant[site_global] == 1
    present = (occupied | migrant) & (~vacated)
    id_perm = jax.random.permutation(rng_keys[3], TOTAL_SLOTS).astype(jnp.int32)
    site_ids = id_perm[site_global]
    centre_pos = (site_xyz + 0.5) * SPACING
    jitter = jax.random.uniform(rng_keys[4], (NUM_BRICKS, CAPACITY, 3), minval=-0.05, maxval=0.05) * SPACING
    face_pos = (site_xyz + (direction > 0).astype(jnp.int32)) * SPACING
    inset = jax.random.uniform(rng_keys[5], (NUM_BRICKS, CAPACITY, 3), minval=0.005, maxval=0.015)
    outset = jax.random.uniform(rng_keys[6], (NUM_BRICKS, CAPACITY, 3), minval=0.005, maxval=0.015)
    thermal = jax.random.normal(rng_keys[7], (NUM_BRICKS, CAPACITY, 3), jnp.float32) * 1.2
    crossing = migrant[..., None] & (direction != 0)
    new_pos = jnp.where(crossing, face_pos + direction * inset, centre_pos + jitter)
    half_vel = jnp.where(crossing, direction * (inset + outset) / TIME_STEP, thermal)
    old_pos = new_pos - TIME_STEP * half_vel
    old_frc = jax.random.normal(rng_keys[8], (NUM_BRICKS, CAPACITY, 3), jnp.float32) * 30.0
    old_vel = half_vel - 0.5 * TIME_STEP * old_frc
    rank_key = jnp.where(present, site_ids, TOTAL_SLOTS + local_idx[None, :])
    sort_order = jnp.argsort(rank_key, axis=1)

    def take_flat(values):
        return jnp.take_along_axis(values, sort_order, axis=1)

    def take_vec(values):
        return jnp.take_along_axis(values, sort_order[..., None], axis=1)

    is_live = take_flat(present)
    live_vec = is_live[..., None]
    return {
        "positions": jnp.where(live_vec, take_vec(old_pos), 0.0).reshape(TOTAL_SLOTS, 3).astype(jnp.float32),
        "velocities": jnp.where(live_vec, take_vec(old_vel), 0.0).reshape(TOTAL_SLOTS, 3).astype(jnp.float32),
        "forces": jnp.where(live_vec, take_vec(old_frc), 0.0).reshape(TOTAL_SLOTS, 3).astype(jnp.float32),
        "atom_ids": jnp.where(is_live, take_flat(site_ids), 0).reshape(TOTAL_SLOTS).astype(jnp.int32),
        "valid_mask": is_live.reshape(TOTAL_SLOTS).astype(jnp.int32),
    }


def reference(positions, velocities, forces, atom_ids, valid_mask):
    is_live = valid_mask == 1
    box_len = BRICK_SIDE * jnp.array([NUM_X, NUM_Y, NUM_Z], jnp.float32)
    v_half = velocities + 0.5 * TIME_STEP * forces
    moved_pos = positions + TIME_STEP * v_half
    moved_pos = moved_pos - box_len * jnp.floor(moved_pos / box_len)
    cell_idx = jnp.clip(jnp.floor(moved_pos / BRICK_SIDE).astype(jnp.int32), 0, jnp.array([NUM_X - 1, NUM_Y - 1, NUM_Z - 1]))
    dest_brick = jnp.where(is_live, brick_linear(cell_idx), NUM_BRICKS)
    sort_order = jnp.argsort(dest_brick * TOTAL_SLOTS + atom_ids)
    dest_sorted = dest_brick[sort_order]
    counts = jax.ops.segment_sum(jnp.ones_like(dest_brick), dest_brick, NUM_BRICKS + 1)
    first_slot = jnp.cumsum(counts) - counts
    slot_rank = jnp.arange(TOTAL_SLOTS) - first_slot[dest_sorted]
    dest_slot = jnp.where(dest_sorted < NUM_BRICKS, dest_sorted * CAPACITY + slot_rank, TOTAL_SLOTS)

    def scatter_rows(values):
        return jnp.zeros_like(values).at[dest_slot].set(values[sort_order], mode="drop")

    new_pos = scatter_rows(moved_pos)
    vel_sorted = scatter_rows(v_half)
    new_ids = scatter_rows(atom_ids)
    new_valid = scatter_rows(is_live.astype(jnp.int32))
    pos_blocks = new_pos.reshape(NUM_BRICKS, CAPACITY, 3)
    id_blocks = new_ids.reshape(NUM_BRICKS, CAPACITY)
    live_blocks = new_valid.reshape(NUM_BRICKS, CAPACITY) == 1
    shifts = neighbour_table()

    def brick_forces(brick_idx):
        brick_x = brick_idx % NUM_X
        brick_y = (brick_idx // NUM_X) % NUM_Y
        brick_z = brick_idx // (NUM_X * NUM_Y)
        nbr_bricks = (((brick_z + shifts[:, 2]) % NUM_Z) * NUM_Y + (brick_y + shifts[:, 1]) % NUM_Y) * NUM_X + (brick_x + shifts[:, 0]) % NUM_X
        src_pos = pos_blocks[nbr_bricks].reshape(-1, 3)
        src_ids = id_blocks[nbr_bricks].reshape(-1)
        src_live = live_blocks[nbr_bricks].reshape(-1)
        own_pos = pos_blocks[brick_idx]
        own_ids = id_blocks[brick_idx]
        own_live = live_blocks[brick_idx]
        pair_delta = own_pos[:, None, :] - src_pos[None, :, :]
        pair_delta = pair_delta - box_len * jnp.floor(pair_delta / box_len + 0.5)
        dist_sq = jnp.sum(pair_delta * pair_delta, axis=-1)
        pair_mask = own_live[:, None] & src_live[None, :] & (own_ids[:, None] != src_ids[None, :]) & (dist_sq < RCUT * RCUT)
        pair_energy, f_over_r = pair_terms(dist_sq, pair_mask)
        return jnp.sum(f_over_r[:, :, None] * pair_delta, axis=1), jnp.sum(pair_energy)

    new_frc, brick_energy = lax.map(brick_forces, jnp.arange(NUM_BRICKS))
    new_frc = new_frc.reshape(TOTAL_SLOTS, 3)
    new_vel = vel_sorted + 0.5 * TIME_STEP * new_frc
    return (new_pos, new_vel, new_frc, new_ids, new_valid, 0.5 * jnp.sum(brick_energy))
```

```python
import functools

import jax
import jax.numpy as jnp
from jax import lax
from jax.experimental import pallas as pl
from jax.experimental.pallas import tpu as pltpu
from jax.sharding import PartitionSpec as P

TIME_STEP = 0.005
RCUT = 2.5
DENSITY = 0.8442
SPACING = (1.0 / DENSITY) ** (1.0 / 3.0)
SITES = 12
BRICK = SITES * SPACING
BOX = 2.0 * BRICK
BRICK_AXES = ("bz", "by", "bx")
CAP = SITES ** 3
KPAD = 1792
MESH_ID = pl.DeviceIdType.MESH
F32 = jnp.float32
BF16 = jnp.bfloat16
CUT6 = RCUT ** -6
U_CUT = 4.0 * (CUT6 * CUT6 - CUT6)
DU_CUT = (-48.0 * CUT6 * CUT6 + 24.0 * CUT6) / RCUT
DELTAS = [(d >> 2 & 1, d >> 1 & 1, d & 1) for d in range(1, 8)]
SHIFTS = [(dx, dy) for dy in range(-2, 3) for dx in range(-2, 3)]
NF = 7


def iota(shape, dim):
    return lax.broadcasted_iota(jnp.int32, shape, dim)


def split3(x):
    hi = x.astype(BF16).astype(F32)
    rest = x - hi
    mid = rest.astype(BF16).astype(F32)
    return hi, mid, rest - mid


def dot_nt(a, b):
    return lax.dot_general(a, b, (((1,), (1,)), ((), ())), preferred_element_type=F32)


def dot_nn(a, b):
    return lax.dot_general(a, b, (((1,), (0,)), ((), ())), preferred_element_type=F32)


def buf_shape(delta):
    return (NF * (8 if delta[0] else 16), 128 if delta[1] else 256)


def to_delta(g, delta):
    dz, dy, dx = delta
    if dx:
        xf = iota(g.shape, 1) & 15
        g = jnp.where(xf < 3, pltpu.roll(g, 244, 1), jnp.where(xf >= 13, pltpu.roll(g, 12, 1), 0.0))
    if dz:
        row = iota((8, 256), 0)
        g = jnp.where(row < 3, pltpu.roll(g[8:16], 4, 0), jnp.where(row >= 5, pltpu.roll(g[0:8], 4, 0), 0.0))
    if dy:
        lane = iota((g.shape[0], 128), 1)
        g = jnp.where(lane < 48, pltpu.roll(g[:, 128:], 64, 1), jnp.where(lane >= 80, pltpu.roll(g[:, :128], 64, 1), 0.0))
    return g


def from_delta(b, delta):
    dz, dy, _ = delta
    if dy:
        lane = iota(b.shape, 1)
        b = jnp.concatenate([jnp.where(lane < 48, b, 0.0), jnp.where(lane >= 80, b, 0.0)], axis=1)
    if dz:
        row = iota(b.shape, 0)
        b = jnp.concatenate([jnp.where(row < 3, b, 0.0), jnp.where(row >= 5, b, 0.0)], axis=0)
    return b


def kernel(pos_ref, vel_ref, frc_ref, id_ref, val_ref, opos_ref, ovel_ref, ofrc_ref, oid_ref, oval_ref, oen_ref, *scratch):
    sbufs = scratch[0:7]
    rbufs = scratch[7:14]
    atom_ref, g_ref, t_ref, q_ref, ebuf, send_sem, recv_sem, esend_sem, erecv_sem = scratch[14:]
    bz, by, bx = lax.axis_index("bz"), lax.axis_index("by"), lax.axis_index("bx")

    def partner(delta):
        return (lax.rem(bz + delta[0], 2), lax.rem(by + delta[1], 2), lax.rem(bx + delta[2], 2))

    barrier = pltpu.get_barrier_semaphore()
    for delta in DELTAS:
        pl.semaphore_signal(barrier, inc=1, device_id=partner(delta), device_id_type=MESH_ID)

    v_half = vel_ref[...] + (0.5 * TIME_STEP) * frc_ref[...]
    moved = pos_ref[...] + TIME_STEP * v_half
    moved = moved - BOX * jnp.floor(moved * (1.0 / BOX))
    axis_row = iota((3, 1), 0)
    coord = jnp.where(axis_row == 0, bx, jnp.where(axis_row == 1, by, bz)).astype(F32)
    brick_lo = coord * BRICK
    rel = moved - brick_lo
    rel = jnp.where(rel < -0.5 * BRICK, rel + BOX, jnp.where(rel >= 1.5 * BRICK, rel - BOX, rel))
    cell = jnp.floor(rel * (1.0 / SPACING)).astype(jnp.int32) + 2
    live = val_ref[...] == 1
    ids = id_ref[...]
    atom_ref[:, pl.ds(KPAD - 128, 128)] = jnp.zeros((atom_ref.shape[0], 128), F32)
    zi = jnp.where(live, cell[2:3, :], 0)
    lo = jnp.where(live, cell[1:2, :] * 16 + cell[0:1, :], 0)
    rows = list(split3(moved)) + list(split3(v_half))
    for k in range(6):
        atom_ref[8 * k:8 * k + 3, 0:CAP] = rows[k]
    atom_ref[48:49, 0:CAP] = (ids >> 7).astype(F32)
    atom_ref[49:50, 0:CAP] = (ids & 127).astype(F32)
    atom_ref[50:51, 0:CAP] = zi.astype(F32)
    atom_ref[51:52, 0:CAP] = lo.astype(F32)

    zrow = atom_ref[50:51, :]
    lrow = atom_ref[51:52, :]
    zmask = jnp.broadcast_to(zrow, (16, KPAD)) == iota((16, KPAD), 0).astype(F32)
    onehot = jnp.where(jnp.broadcast_to(lrow, (256, KPAD)) == iota((256, KPAD), 0).astype(F32), 1.0, 0.0).astype(BF16)

    def spread(row_idx):
        return jnp.where(zmask, jnp.broadcast_to(atom_ref[row_idx:row_idx + 1, :], (16, KPAD)), 0.0).astype(BF16)

    order = [8 * k + c for k in range(6) for c in range(3)] + [48, 49]
    lhs = jnp.concatenate([spread(i) for i in order], axis=0)
    binned = dot_nt(lhs, onehot)
    g_ref[0:48, :] = binned[0:48] + binned[48:96] + binned[96:144]
    g_ref[48:96, :] = binned[144:192] + binned[192:240] + binned[240:288]
    g_ref[96:112, :] = binned[288:304] * 128.0 + binned[304:320]

    for k, delta in enumerate(DELTAS):
        rz = 8 if delta[0] else 16
        for f in range(NF):
            sbufs[k][f * rz:(f + 1) * rz, :] = to_delta(g_ref[16 * f:16 * f + 16, :], delta)
    pl.semaphore_wait(barrier, 7)
    copies = []
    for k, delta in enumerate(DELTAS):
        copy = pltpu.make_async_remote_copy(src_ref=sbufs[k], dst_ref=rbufs[k], send_sem=send_sem.at[k], recv_sem=recv_sem.at[k], device_id=partner(delta), device_id_type=MESH_ID)
        copy.start()
        copies.append(copy)
    for copy in copies:
        copy.wait_recv()
    fields = []
    for f in range(NF):
        acc = g_ref[16 * f:16 * f + 16, :]
        for k, delta in enumerate(DELTAS):
            rz = 8 if delta[0] else 16
            acc = acc + from_delta(rbufs[k][f * rz:(f + 1) * rz, :], delta)
        fields.append(acc)

    present = fields[0] != 0.0
    lane = iota((16, 256), 1)
    frame = [lane & 15, lane >> 4, iota((16, 256), 0)]
    los = [bx, by, bz]
    local = []
    for c in range(3):
        u = fields[c] - los[c].astype(F32) * BRICK
        u = jnp.where(u < -0.5 * BRICK, u + BOX, jnp.where(u >= 1.5 * BRICK, u - BOX, u))
        local.append(jnp.where(present, u, 1000.0 + 10.0 * frame[c].astype(F32)))

    for s, (dx, dy) in enumerate(SHIFTS):
        for h in range(2):
            left = 32 + 96 * h + 16 * dy + dx
            for c in range(3):
                rolled = pltpu.roll(local[c], (256 - left) % 256, 1)
                t_ref[3 * s + c, pl.ds(h, 16, stride=2), :] = rolled[:, 0:128]
    for h in range(2):
        left = 32 + 96 * h
        for f in range(NF):
            rolled = pltpu.roll(fields[f], (256 - left) % 256, 1)
            q_ref[f, pl.ds(h, 16, stride=2), :] = rolled[:, 0:128]

    base = SHIFTS.index((0, 0))
    mine = [t_ref[3 * base + c, 4:28, :] for c in range(3)]

    def pair(carry, nbr):
        fx, fy, fz, sw, s6, sr, sn = carry
        ex, ey, ez = mine[0] - nbr[0], mine[1] - nbr[1], mine[2] - nbr[2]
        r2 = ex * ex + ey * ey + ez * ez
        near = r2 < RCUT * RCUT
        inv = jnp.where(near, lax.rsqrt(r2), 0.0)
        i2 = inv * inv
        i6 = i2 * i2 * i2
        w = i6 * (i6 - 0.5)
        fr = w * i2 + (DU_CUT / 48.0) * inv
        return (fx + fr * ex, fy + fr * ey, fz + fr * ez, sw + w, s6 + i6, sr + r2 * inv, sn + jnp.where(near, 1.0, 0.0))

    def load(s, dz):
        return [t_ref[3 * s + c, 4 + 2 * dz:28 + 2 * dz, :] for c in range(3)]

    carry = tuple(jnp.zeros((24, 128), F32) for _ in range(7))
    for s, (dx, dy) in enumerate(SHIFTS):
        twos = (abs(dx) == 2) + (abs(dy) == 2)
        if twos == 2:
            continue
        for dz in (range(-2, 3) if twos == 0 else range(-1, 2)):
            if (dx, dy, dz) != (0, 0, 0):
                carry = pair(carry, load(s, dz))
    low_x = (iota((24, 128), 1) & 15) < 8
    row24 = iota((24, 128), 0)
    low_y = (row24 & 1) == 0
    low_z = row24 < 12
    idx = SHIFTS.index
    for dz in range(-1, 2):
        a, b, c2, d = load(idx((-2, -2)), dz), load(idx((2, -2)), dz), load(idx((-2, 2)), dz), load(idx((2, 2)), dz)
        carry = pair(carry, [jnp.where(low_y, jnp.where(low_x, a[c], b[c]), jnp.where(low_x, c2[c], d[c])) for c in range(3)])
    for dy in range(-1, 2):
        a, b, c2, d = load(idx((-2, dy)), -2), load(idx((2, dy)), -2), load(idx((-2, dy)), 2), load(idx((2, dy)), 2)
        carry = pair(carry, [jnp.where(low_z, jnp.where(low_x, a[c], b[c]), jnp.where(low_x, c2[c], d[c])) for c in range(3)])
    for dx in range(-1, 2):
        a, b, c2, d = load(idx((dx, -2)), -2), load(idx((dx, 2)), -2), load(idx((dx, -2)), 2), load(idx((dx, 2)), 2)
        carry = pair(carry, [jnp.where(low_z, jnp.where(low_y, a[c], b[c]), jnp.where(low_y, c2[c], d[c])) for c in range(3)])
    force = [48.0 * carry[c] for c in range(3)]

    lane24 = iota((24, 128), 1)
    x24 = lane24 & 15
    own = (lane24 < 96) & (x24 >= 2) & (x24 < 14) & (q_ref[0, 4:28, :] != 0.0)
    energy = 4.0 * (carry[3] - 0.5 * carry[4]) - DU_CUT * carry[5] + (RCUT * DU_CUT - U_CUT) * carry[6]
    energy = jnp.where(own, 0.5 * energy, 0.0)
    me = bz * 4 + by * 2 + bx
    ebuf[me, :, :] = energy[0:8] + energy[8:16] + energy[16:24]
    ecopies = []
    for k, delta in enumerate(DELTAS):
        copy = pltpu.make_async_remote_copy(src_ref=ebuf.at[me], dst_ref=ebuf.at[me], send_sem=esend_sem.at[k], recv_sem=erecv_sem.at[k], device_id=partner(delta), device_id_type=MESH_ID)
        copy.start()
        ecopies.append(copy)

    idv = jnp.where(own, q_ref[6, 4:28, :], -1.0)
    id_int = idv.astype(jnp.int32)
    id_hi = jnp.where(own, id_int >> 7, -1).astype(F32)
    id_lo = jnp.where(own, id_int & 127, -1).astype(F32)

    def flat(x, n):
        return jnp.concatenate([jnp.broadcast_to(x[r:r + 1, :], (n, 128)) for r in range(24)], axis=1)

    hot_hi = jnp.where(flat(id_hi, 128) == iota((128, 3072), 0).astype(F32), 1.0, 0.0).astype(BF16)
    lo_eq = flat(id_lo, 128) == iota((128, 3072), 0).astype(F32)
    hot_lo = jnp.where(lo_eq, 1.0, 0.0).astype(BF16)
    table = dot_nt(hot_lo, hot_hi).astype(BF16)
    r128, c128 = iota((128, 128), 0), iota((128, 128), 1)
    below = dot_nn(jnp.where(c128 < r128, 1.0, 0.0).astype(BF16), table)
    total = dot_nn(jnp.ones((128, 128), BF16), table).astype(BF16)
    before = dot_nn(total, jnp.where(r128 < c128, 1.0, 0.0).astype(BF16))
    rank_tab = below + before
    tab_hi = jnp.floor(rank_tab * (1.0 / 256.0)) * 256.0
    tab_lo = rank_tab - tab_hi
    looked = dot_nn(tab_hi.astype(BF16), hot_hi) + dot_nn(tab_lo.astype(BF16), hot_hi)
    rank = jnp.sum(jnp.where(lo_eq, looked, 0.0), axis=0, keepdims=True)
    any_own = flat(jnp.where(own, 1.0, 0.0), 1) > 0.5
    rank_hi = jnp.floor(rank * (1.0 / 256.0))
    rank_lo = jnp.where(any_own, rank - 256.0 * rank_hi, -1.0)
    rank_hi = jnp.where(any_own, rank_hi, -1.0)

    hot_slot = jnp.where(jnp.broadcast_to(rank_lo, (256, 3072)) == iota((256, 3072), 0).astype(F32), 1.0, 0.0).astype(BF16)
    hi_mask = jnp.broadcast_to(rank_hi, (8, 3072)) == iota((8, 3072), 0).astype(F32)
    outs = []
    for c in range(3):
        outs += list(split3(q_ref[c, 4:28, :]))
    for c in range(3):
        outs += list(split3(q_ref[3 + c, 4:28, :] + (0.5 * TIME_STEP) * force[c]))
    for c in range(3):
        outs += list(split3(force[c]))
    outs += [id_hi, id_lo, jnp.where(own, 1.0, 0.0)]
    lhs = jnp.concatenate([jnp.where(hi_mask, flat(x, 8), 0.0) for x in outs], axis=0).astype(BF16)
    slots = dot_nt(lhs, hot_slot)

    def field(i):
        return slots[8 * i:8 * i + 8, :]

    def put(ref, row, x):
        for h in range(7):
            n = 256 if h < 6 else CAP - 1536
            ref[row:row + 1, 256 * h:256 * h + n] = x[h:h + 1, 0:n].astype(ref.dtype)

    for c in range(3):
        put(opos_ref, c, field(3 * c) + field(3 * c + 1) + field(3 * c + 2))
        put(ovel_ref, c, field(9 + 3 * c) + field(10 + 3 * c) + field(11 + 3 * c))
        put(ofrc_ref, c, field(18 + 3 * c) + field(19 + 3 * c) + field(20 + 3 * c))
    put(oid_ref, 0, field(27) * 128.0 + field(28))
    put(oval_ref, 0, field(29))

    for copy in ecopies:
        copy.wait_recv()
    acc = ebuf[0]
    for k in range(1, 8):
        acc = acc + ebuf[k]
    oen_ref[...] = jnp.sum(jnp.sum(acc, axis=0, keepdims=True), axis=1, keepdims=True)
    for copy in copies + ecopies:
        copy.wait_send()


def solution(mesh):
    row_spec = P(BRICK_AXES, None)
    flat_spec = P(BRICK_AXES)
    vmem = pl.BlockSpec(memory_space=pltpu.VMEM)

    def local_step(pos, vel, frc, ids, valid):
        f3 = jax.ShapeDtypeStruct((3, CAP), F32)
        i1 = jax.ShapeDtypeStruct((1, CAP), jnp.int32)
        outs = pl.pallas_call(
            kernel,
            out_shape=(f3, f3, f3, i1, i1, jax.ShapeDtypeStruct((1, 1), F32)),
            in_specs=[vmem] * 5,
            out_specs=(vmem,) * 6,
            scratch_shapes=[pltpu.VMEM(buf_shape(d), F32) for d in DELTAS] * 2 + [
                pltpu.VMEM((56, KPAD), F32),
                pltpu.VMEM((112, 256), F32),
                pltpu.VMEM((75, 32, 128), F32),
                pltpu.VMEM((NF, 32, 128), F32),
                pltpu.VMEM((8, 8, 128), F32),
                pltpu.SemaphoreType.DMA((7,)),
                pltpu.SemaphoreType.DMA((7,)),
                pltpu.SemaphoreType.DMA((7,)),
                pltpu.SemaphoreType.DMA((7,)),
            ],
            compiler_params=pltpu.CompilerParams(collective_id=0, has_side_effects=True),
        )(pos.T, vel.T, frc.T, ids[None, :], valid[None, :])
        return outs[0].T, outs[1].T, outs[2].T, outs[3][0], outs[4][0], outs[5][0, 0]

    return jax.shard_map(local_step, mesh=mesh, in_specs=(row_spec, row_spec, row_spec, flat_spec, flat_spec), out_specs=(row_spec, row_spec, row_spec, flat_spec, flat_spec, P()), check_vma=False)
```

```python
import functools

import jax
import jax.numpy as jnp
from jax import lax
from jax.experimental import pallas as pl
from jax.experimental.pallas import tpu as pltpu
from jax.sharding import PartitionSpec as P

TIME_STEP = 0.005
RCUT = 2.5
DENSITY = 0.8442
SPACING = (1.0 / DENSITY) ** (1.0 / 3.0)
SITES = 12
BRICK = SITES * SPACING
BOX = 2.0 * BRICK
BRICK_AXES = ("bz", "by", "bx")
CAP = SITES ** 3
KPAD = 1792
MESH_ID = pl.DeviceIdType.MESH
F32 = jnp.float32
BF16 = jnp.bfloat16
CUT6 = RCUT ** -6
U_CUT = 4.0 * (CUT6 * CUT6 - CUT6)
DU_CUT = (-48.0 * CUT6 * CUT6 + 24.0 * CUT6) / RCUT
DELTAS = [(d >> 2 & 1, d >> 1 & 1, d & 1) for d in range(1, 8)]
SEND_ORDER = [(1, 1, 0), (1, 1, 1), (0, 1, 0), (1, 0, 0), (0, 1, 1), (1, 0, 1), (0, 0, 1)]
SHIFTS = [(dx, dy) for dy in range(-2, 3) for dx in range(-2, 3)]
NF = 7


def iota(shape, dim):
    return lax.broadcasted_iota(jnp.int32, shape, dim)


def split3(x):
    hi = x.astype(BF16).astype(F32)
    rest = x - hi
    mid = rest.astype(BF16).astype(F32)
    return hi, mid, rest - mid


def dot_nt(a, b):
    return lax.dot_general(a, b, (((1,), (1,)), ((), ())), preferred_element_type=F32)


def dot_nn(a, b):
    return lax.dot_general(a, b, (((1,), (0,)), ((), ())), preferred_element_type=F32)


def tile_of(delta):
    return 8 if delta[0] else 16, 128 if delta[1] else 256


def pos_arrays(delta):
    return 2 if delta[2] and (delta[0] or delta[1]) else 3


def vel_arrays(delta):
    return 1 if delta[0] or delta[1] else 4


def to_delta(g, delta):
    dz, dy, dx = delta
    if dx:
        xf = iota(g.shape, 1) & 15
        g = jnp.where(xf < 3, pltpu.roll(g, 244, 1), jnp.where(xf >= 13, pltpu.roll(g, 12, 1), 0.0))
    if dz:
        row = iota((8, 256), 0)
        g = jnp.where(row < 3, pltpu.roll(g[8:16], 4, 0), jnp.where(row >= 5, pltpu.roll(g[0:8], 4, 0), 0.0))
    if dy:
        lane = iota((g.shape[0], 128), 1)
        g = jnp.where(lane < 48, pltpu.roll(g[:, 128:], 64, 1), jnp.where(lane >= 80, pltpu.roll(g[:, :128], 64, 1), 0.0))
    return g


def wide(b):
    lane = iota(b.shape, 1)
    return jnp.concatenate([jnp.where(lane < 48, b, 0.0), jnp.where(lane >= 80, b, 0.0)], axis=1)


def tall(b):
    row = iota(b.shape, 0)
    return jnp.concatenate([jnp.where(row < 3, b, 0.0), jnp.where(row >= 5, b, 0.0)], axis=0)


def pack_pos(f, delta):
    if pos_arrays(delta) == 3:
        return f
    return [f[0] + pltpu.roll(f[1], 6, 1), f[2]]


def unpack_pos(a, delta):
    if pos_arrays(delta) == 3:
        return a
    n = a[0].shape[1]
    xf = iota(a[0].shape, 1) & 15
    edge = (xf < 3) | (xf >= 13)
    return [jnp.where(edge, a[0], 0.0), jnp.where(edge, pltpu.roll(a[0], n - 6, 1), 0.0), a[1]]


def pack_vel(f, delta):
    dz, dy, _ = delta
    if dz:
        row = iota(f[0].shape, 0)
        out = jnp.zeros_like(f[0])
        for k in range(4):
            out = jnp.where(row == 2 * k, jnp.broadcast_to(f[k][2:3], out.shape), out)
            out = jnp.where(row == 2 * k + 1, jnp.broadcast_to(f[k][5:6], out.shape), out)
        return [out]
    if dy:
        group = iota(f[0].shape, 1) >> 4
        out = jnp.where((group == 2) | (group == 5), f[0], 0.0)
        out = jnp.where((group == 3) | (group == 6), pltpu.roll(f[1], 16, 1), out)
        out = jnp.where((group == 4) | (group == 7), pltpu.roll(f[2], 32, 1), out)
        out = jnp.where(group == 0, pltpu.roll(f[3], 96, 1), out)
        return [jnp.where(group == 1, pltpu.roll(f[3], 64, 1), out)]
    return f


def unpack_vel(a, delta):
    dz, dy, _ = delta
    if dz:
        row = iota(a[0].shape, 0)
        return [jnp.where(row == 2, jnp.broadcast_to(a[0][2 * k:2 * k + 1], a[0].shape), jnp.where(row == 5, jnp.broadcast_to(a[0][2 * k + 1:2 * k + 2], a[0].shape), 0.0)) for k in range(4)]
    if dy:
        group = iota(a[0].shape, 1) >> 4
        low, high = group == 2, group == 5
        both = low | high
        last = jnp.where(low, pltpu.roll(a[0], 32, 1), jnp.where(high, pltpu.roll(a[0], 64, 1), 0.0))
        return [jnp.where(both, a[0], 0.0), jnp.where(both, pltpu.roll(a[0], 112, 1), 0.0), jnp.where(both, pltpu.roll(a[0], 96, 1), 0.0), last]
    return a


def merge(own, parts):
    flat = own + parts[(0, 0, 1)] + wide(parts[(0, 1, 0)] + parts[(0, 1, 1)])
    return flat + tall(parts[(1, 0, 0)] + parts[(1, 0, 1)] + wide(parts[(1, 1, 0)] + parts[(1, 1, 1)]))


def kernel(pos_ref, vel_ref, frc_ref, id_ref, val_ref, opos_ref, ovel_ref, ofrc_ref, oid_ref, oval_ref, oen_ref, *scratch):
    psend, precv, vsend, vrecv = (scratch[7 * i:7 * i + 7] for i in range(4))
    atom_ref, g_ref, t_ref, q_ref, ebuf, psend_sem, precv_sem, vsend_sem, vrecv_sem, esend_sem, erecv_sem = scratch[28:]
    bz, by, bx = lax.axis_index("bz"), lax.axis_index("by"), lax.axis_index("bx")

    def partner(delta):
        return (lax.rem(bz + delta[0], 2), lax.rem(by + delta[1], 2), lax.rem(bx + delta[2], 2))

    barrier = pltpu.get_barrier_semaphore()
    for delta in DELTAS:
        pl.semaphore_signal(barrier, inc=1, device_id=partner(delta), device_id_type=MESH_ID)

    v_half = vel_ref[...] + (0.5 * TIME_STEP) * frc_ref[...]
    moved = pos_ref[...] + TIME_STEP * v_half
    moved = moved - BOX * jnp.floor(moved * (1.0 / BOX))
    axis_row = iota((3, 1), 0)
    coord = jnp.where(axis_row == 0, bx, jnp.where(axis_row == 1, by, bz)).astype(F32)
    brick_lo = coord * BRICK
    rel = moved - brick_lo
    rel = jnp.where(rel < -0.5 * BRICK, rel + BOX, jnp.where(rel >= 1.5 * BRICK, rel - BOX, rel))
    cell = jnp.floor(rel * (1.0 / SPACING)).astype(jnp.int32) + 2
    live = val_ref[...].reshape(1, CAP) == 1
    ids = id_ref[...].reshape(1, CAP)
    atom_ref[:, pl.ds(KPAD - 128, 128)] = jnp.zeros((atom_ref.shape[0], 128), F32)
    zi = jnp.where(live, cell[2:3, :], 0)
    lo = jnp.where(live, cell[1:2, :] * 16 + cell[0:1, :], 0)
    rows = list(split3(moved)) + list(split3(v_half))
    for k in range(6):
        atom_ref[8 * k:8 * k + 3, 0:CAP] = rows[k]
    atom_ref[48:49, 0:CAP] = (ids >> 7).astype(F32)
    atom_ref[49:50, 0:CAP] = (ids & 127).astype(F32)
    atom_ref[50:51, 0:CAP] = zi.astype(F32)
    atom_ref[51:52, 0:CAP] = lo.astype(F32)

    zrow = atom_ref[50:51, :]
    lrow = atom_ref[51:52, :]
    zmask = jnp.broadcast_to(zrow, (16, KPAD)) == iota((16, KPAD), 0).astype(F32)
    onehot = jnp.where(jnp.broadcast_to(lrow, (256, KPAD)) == iota((256, KPAD), 0).astype(F32), 1.0, 0.0).astype(BF16)

    def spread(row_idx):
        return jnp.where(zmask, jnp.broadcast_to(atom_ref[row_idx:row_idx + 1, :], (16, KPAD)), 0.0).astype(BF16)

    def exchange(src, dst, ssem, rsem):
        copies = {}
        for delta in SEND_ORDER:
            k = DELTAS.index(delta)
            copies[delta] = pltpu.make_async_remote_copy(src_ref=src[k], dst_ref=dst[k], send_sem=ssem.at[k], recv_sem=rsem.at[k], device_id=partner(delta), device_id_type=MESH_ID)
            copies[delta].start()
        return copies

    def fill(bufs, fields, pack):
        for k, delta in enumerate(DELTAS):
            rz = tile_of(delta)[0]
            for i, arr in enumerate(pack([to_delta(f, delta) for f in fields], delta)):
                bufs[k][i * rz:(i + 1) * rz, :] = arr

    def gather(own, bufs, count, unpack):
        parts = {}
        for k, delta in enumerate(DELTAS):
            rz = tile_of(delta)[0]
            parts[delta] = unpack([bufs[k][i * rz:(i + 1) * rz, :] for i in range(count(delta))], delta)
        return [merge(own[f], {d: parts[d][f] for d in DELTAS}) for f in range(len(own))]

    lhs = jnp.concatenate([spread(8 * k + c) for k in range(3) for c in range(3)], axis=0)
    binned = dot_nt(lhs, onehot)
    pos_own = [binned[16 * c:16 * c + 16] + binned[48 + 16 * c:64 + 16 * c] + binned[96 + 16 * c:112 + 16 * c] for c in range(3)]
    fill(psend, pos_own, pack_pos)
    for c in range(3):
        g_ref[16 * c:16 * c + 16, :] = pos_own[c]
    pl.semaphore_wait(barrier, 7)
    copies = exchange(psend, precv, psend_sem, precv_sem)

    lhs = jnp.concatenate([spread(8 * k + c) for k in range(3, 6) for c in range(3)] + [spread(48), spread(49)], axis=0)
    binned = dot_nt(lhs, onehot)
    vel_own = [binned[16 * c:16 * c + 16] + binned[48 + 16 * c:64 + 16 * c] + binned[96 + 16 * c:112 + 16 * c] for c in range(3)]
    vel_own.append(binned[144:160] * 128.0 + binned[160:176])
    fill(vsend, vel_own, pack_vel)
    for c in range(4):
        g_ref[48 + 16 * c:64 + 16 * c, :] = vel_own[c]
    vcopies = exchange(vsend, vrecv, vsend_sem, vrecv_sem)

    for delta in DELTAS:
        copies[delta].wait_recv()
    fields = gather([g_ref[16 * c:16 * c + 16, :] for c in range(3)], precv, pos_arrays, unpack_pos)

    present = fields[0] != 0.0
    lane = iota((16, 256), 1)
    frame = [lane & 15, lane >> 4, iota((16, 256), 0)]
    los = [bx, by, bz]
    local = []
    for c in range(3):
        u = fields[c] - los[c].astype(F32) * BRICK
        u = jnp.where(u < -0.5 * BRICK, u + BOX, jnp.where(u >= 1.5 * BRICK, u - BOX, u))
        local.append(jnp.where(present, u, 1000.0 + 10.0 * frame[c].astype(F32)))

    for s, (dx, dy) in enumerate(SHIFTS):
        for h in range(2):
            left = 32 + 96 * h + 16 * dy + dx
            for c in range(3):
                rolled = pltpu.roll(local[c], (256 - left) % 256, 1)
                t_ref[3 * s + c, pl.ds(h, 16, stride=2), :] = rolled[:, 0:128]

    def keep(f, x):
        for h in range(2):
            rolled = pltpu.roll(x, (256 - 32 - 96 * h) % 256, 1)
            q_ref[f, pl.ds(h, 16, stride=2), :] = rolled[:, 0:128]

    for c in range(3):
        keep(c, fields[c])

    base = SHIFTS.index((0, 0))
    mine = [t_ref[3 * base + c, 4:28, :] for c in range(3)]

    def pair(carry, nbr):
        fx, fy, fz, sw, s6, sr, sn = carry
        ex, ey, ez = mine[0] - nbr[0], mine[1] - nbr[1], mine[2] - nbr[2]
        r2 = ex * ex + ey * ey + ez * ez
        near = r2 < RCUT * RCUT
        inv = jnp.where(near, lax.rsqrt(r2), 0.0)
        i2 = inv * inv
        i6 = i2 * i2 * i2
        w = i6 * (i6 - 0.5)
        fr = w * i2 + (DU_CUT / 48.0) * inv
        return (fx + fr * ex, fy + fr * ey, fz + fr * ez, sw + w, s6 + i6, sr + r2 * inv, sn + jnp.where(near, 1.0, 0.0))

    def load(s, dz):
        return [t_ref[3 * s + c, 4 + 2 * dz:28 + 2 * dz, :] for c in range(3)]

    carry = tuple(jnp.zeros((24, 128), F32) for _ in range(7))
    for s, (dx, dy) in enumerate(SHIFTS):
        twos = (abs(dx) == 2) + (abs(dy) == 2)
        if twos == 2:
            continue
        for dz in (range(-2, 3) if twos == 0 else range(-1, 2)):
            if (dx, dy, dz) != (0, 0, 0):
                carry = pair(carry, load(s, dz))
    low_x = (iota((24, 128), 1) & 15) < 8
    row24 = iota((24, 128), 0)
    low_y = (row24 & 1) == 0
    low_z = row24 < 12
    idx = SHIFTS.index
    for dz in range(-1, 2):
        a, b, c2, d = load(idx((-2, -2)), dz), load(idx((2, -2)), dz), load(idx((-2, 2)), dz), load(idx((2, 2)), dz)
        carry = pair(carry, [jnp.where(low_y, jnp.where(low_x, a[c], b[c]), jnp.where(low_x, c2[c], d[c])) for c in range(3)])
    for dy in range(-1, 2):
        a, b, c2, d = load(idx((-2, dy)), -2), load(idx((2, dy)), -2), load(idx((-2, dy)), 2), load(idx((2, dy)), 2)
        carry = pair(carry, [jnp.where(low_z, jnp.where(low_x, a[c], b[c]), jnp.where(low_x, c2[c], d[c])) for c in range(3)])
    for dx in range(-1, 2):
        a, b, c2, d = load(idx((dx, -2)), -2), load(idx((dx, 2)), -2), load(idx((dx, -2)), 2), load(idx((dx, 2)), 2)
        carry = pair(carry, [jnp.where(low_z, jnp.where(low_y, a[c], b[c]), jnp.where(low_y, c2[c], d[c])) for c in range(3)])
    force = [48.0 * carry[c] for c in range(3)]

    lane24 = iota((24, 128), 1)
    x24 = lane24 & 15
    own = (lane24 < 96) & (x24 >= 2) & (x24 < 14) & (q_ref[0, 4:28, :] != 0.0)
    energy = 4.0 * (carry[3] - 0.5 * carry[4]) - DU_CUT * carry[5] + (RCUT * DU_CUT - U_CUT) * carry[6]
    energy = jnp.where(own, 0.5 * energy, 0.0)
    me = bz * 4 + by * 2 + bx
    ebuf[me, :, :] = energy[0:8] + energy[8:16] + energy[16:24]
    ecopies = []
    for k, delta in enumerate(DELTAS):
        copy = pltpu.make_async_remote_copy(src_ref=ebuf.at[me], dst_ref=ebuf.at[me], send_sem=esend_sem.at[k], recv_sem=erecv_sem.at[k], device_id=partner(delta), device_id_type=MESH_ID)
        copy.start()
        ecopies.append(copy)

    for delta in DELTAS:
        vcopies[delta].wait_recv()
    for f, x in enumerate(gather([g_ref[48 + 16 * c:64 + 16 * c, :] for c in range(4)], vrecv, vel_arrays, unpack_vel)):
        keep(3 + f, x)

    idv = jnp.where(own, q_ref[6, 4:28, :], -1.0)
    id_int = idv.astype(jnp.int32)
    id_hi = jnp.where(own, id_int >> 7, -1).astype(F32)
    id_lo = jnp.where(own, id_int & 127, -1).astype(F32)

    def flat(x, n):
        return jnp.concatenate([jnp.broadcast_to(x[r:r + 1, :], (n, 128)) for r in range(24)], axis=1)

    hot_hi = jnp.where(flat(id_hi, 128) == iota((128, 3072), 0).astype(F32), 1.0, 0.0).astype(BF16)
    lo_eq = flat(id_lo, 128) == iota((128, 3072), 0).astype(F32)
    hot_lo = jnp.where(lo_eq, 1.0, 0.0).astype(BF16)
    table = dot_nt(hot_lo, hot_hi).astype(BF16)
    r128, c128 = iota((128, 128), 0), iota((128, 128), 1)
    below = dot_nn(jnp.where(c128 < r128, 1.0, 0.0).astype(BF16), table)
    total = dot_nn(jnp.ones((128, 128), BF16), table).astype(BF16)
    before = dot_nn(total, jnp.where(r128 < c128, 1.0, 0.0).astype(BF16))
    rank_tab = below + before
    tab_hi = jnp.floor(rank_tab * (1.0 / 256.0)) * 256.0
    tab_lo = rank_tab - tab_hi
    looked = dot_nn(tab_hi.astype(BF16), hot_hi) + dot_nn(tab_lo.astype(BF16), hot_hi)
    rank = jnp.sum(jnp.where(lo_eq, looked, 0.0), axis=0, keepdims=True)
    any_own = flat(jnp.where(own, 1.0, 0.0), 1) > 0.5
    rank_hi = jnp.floor(rank * (1.0 / 256.0))
    rank_lo = jnp.where(any_own, rank - 256.0 * rank_hi, -1.0)
    rank_hi = jnp.where(any_own, rank_hi, -1.0)

    hot_slot = jnp.where(jnp.broadcast_to(rank_lo, (256, 3072)) == iota((256, 3072), 0).astype(F32), 1.0, 0.0).astype(BF16)
    hi_mask = jnp.broadcast_to(rank_hi, (8, 3072)) == iota((8, 3072), 0).astype(F32)
    outs = []
    for c in range(3):
        outs += list(split3(q_ref[c, 4:28, :]))
    for c in range(3):
        outs += list(split3(q_ref[3 + c, 4:28, :] + (0.5 * TIME_STEP) * force[c]))
    for c in range(3):
        outs += list(split3(force[c]))
    outs += [id_hi, id_lo, jnp.where(own, 1.0, 0.0)]
    lhs = jnp.concatenate([jnp.where(hi_mask, flat(x, 8), 0.0) for x in outs], axis=0).astype(BF16)
    slots = dot_nt(lhs, hot_slot)

    def field(i):
        return slots[8 * i:8 * i + 8, :]

    def put(ref, row, x):
        for h in range(7):
            n = 256 if h < 6 else CAP - 1536
            ref[row:row + 1, 256 * h:256 * h + n] = x[h:h + 1, 0:n].astype(ref.dtype)

    for c in range(3):
        put(opos_ref, c, field(3 * c) + field(3 * c + 1) + field(3 * c + 2))
        put(ovel_ref, c, field(9 + 3 * c) + field(10 + 3 * c) + field(11 + 3 * c))
        put(ofrc_ref, c, field(18 + 3 * c) + field(19 + 3 * c) + field(20 + 3 * c))
    put(oid_ref, 0, field(27) * 128.0 + field(28))
    put(oval_ref, 0, field(29))

    for copy in ecopies:
        copy.wait_recv()
    acc = ebuf[0]
    for k in range(1, 8):
        acc = acc + ebuf[k]
    oen_ref[...] = jnp.sum(jnp.sum(acc, axis=0, keepdims=True), axis=1, keepdims=True)
    for copy in list(copies.values()) + list(vcopies.values()) + ecopies:
        copy.wait_send()


def finish(pos_ref, vel_ref, frc_ref, id_ref, val_ref, en_ref, opos_ref, ovel_ref, ofrc_ref, oid_ref, oval_ref, oen_ref):
    opos_ref[...] = pos_ref[...]
    ovel_ref[...] = vel_ref[...]
    ofrc_ref[...] = frc_ref[...]
    oid_ref[...] = id_ref[...].reshape(CAP)
    oval_ref[...] = val_ref[...].reshape(CAP)
    oen_ref[...] = en_ref[...]


def solution(mesh):
    row_spec = P(BRICK_AXES, None)
    flat_spec = P(BRICK_AXES)
    vmem = pl.BlockSpec(memory_space=pltpu.VMEM)

    def local_step(pos, vel, frc, ids, valid):
        f3 = jax.ShapeDtypeStruct((3, CAP), F32)
        i1 = jax.ShapeDtypeStruct((CAP,), jnp.int32)
        outs = pl.pallas_call(
            kernel,
            out_shape=(pltpu.VMEM((3, CAP), F32),) * 3 + (pltpu.VMEM((1, CAP), jnp.int32),) * 2 + (pltpu.VMEM((1, 1), F32),),
            in_specs=[vmem] * 5,
            out_specs=(vmem,) * 6,
            scratch_shapes=[pltpu.VMEM((pos_arrays(d) * tile_of(d)[0], tile_of(d)[1]), F32) for d in DELTAS] * 2 + [pltpu.VMEM((vel_arrays(d) * tile_of(d)[0], tile_of(d)[1]), F32) for d in DELTAS] * 2 + [
                pltpu.VMEM((56, KPAD), F32),
                pltpu.VMEM((112, 256), F32),
                pltpu.VMEM((75, 32, 128), F32),
                pltpu.VMEM((NF, 32, 128), F32),
                pltpu.VMEM((8, 8, 128), F32),
                pltpu.SemaphoreType.DMA((7,)),
                pltpu.SemaphoreType.DMA((7,)),
                pltpu.SemaphoreType.DMA((7,)),
                pltpu.SemaphoreType.DMA((7,)),
                pltpu.SemaphoreType.DMA((7,)),
                pltpu.SemaphoreType.DMA((7,)),
            ],
            compiler_params=pltpu.CompilerParams(collective_id=0, has_side_effects=True),
        )(pos.T, vel.T, frc.T, ids, valid)
        outs = pl.pallas_call(
            finish,
            out_shape=(f3, f3, f3, i1, i1, jax.ShapeDtypeStruct((1, 1), F32)),
            in_specs=[vmem] * 6,
            out_specs=(vmem,) * 6,
            compiler_params=pltpu.CompilerParams(vmem_limit_bytes=4 << 20),
        )(*outs)
        return outs[0].T, outs[1].T, outs[2].T, outs[3], outs[4], outs[5][0, 0]

    return jax.shard_map(local_step, mesh=mesh, in_specs=(row_spec, row_spec, row_spec, flat_spec, flat_spec), out_specs=(row_spec, row_spec, row_spec, flat_spec, flat_spec, P()), check_vma=False)
```

```python
import functools

import jax
import jax.numpy as jnp
from jax import lax
from jax.experimental import pallas as pl
from jax.experimental.pallas import tpu as pltpu
from jax.sharding import PartitionSpec as P

TIME_STEP = 0.005
RCUT = 2.5
DENSITY = 0.8442
SPACING = (1.0 / DENSITY) ** (1.0 / 3.0)
SITES = 12
BRICK = SITES * SPACING
BOX = 2.0 * BRICK
BRICK_AXES = ("bz", "by", "bx")
CAP = SITES ** 3
KPAD = 1792
MESH_ID = pl.DeviceIdType.MESH
F32 = jnp.float32
BF16 = jnp.bfloat16
CUT6 = RCUT ** -6
U_CUT = 4.0 * (CUT6 * CUT6 - CUT6)
DU_CUT = (-48.0 * CUT6 * CUT6 + 24.0 * CUT6) / RCUT
DELTAS = [(d >> 2 & 1, d >> 1 & 1, d & 1) for d in range(1, 8)]
SEND_ORDER = [(1, 1, 0), (1, 1, 1), (0, 1, 0), (1, 0, 0), (0, 1, 1), (1, 0, 1), (0, 0, 1)]
SHIFTS = [(dx, dy) for dy in range(-2, 3) for dx in range(-2, 3)]
NF = 7


def iota(shape, dim):
    return lax.broadcasted_iota(jnp.int32, shape, dim)


def split3(x):
    hi = x.astype(BF16).astype(F32)
    rest = x - hi
    mid = rest.astype(BF16).astype(F32)
    return hi, mid, rest - mid


def dot_nt(a, b):
    return lax.dot_general(a, b, (((1,), (1,)), ((), ())), preferred_element_type=F32)


def dot_nn(a, b):
    return lax.dot_general(a, b, (((1,), (0,)), ((), ())), preferred_element_type=F32)


def tile_of(delta):
    return 8 if delta[0] else 16, 128 if delta[1] else 256


def pos_arrays(delta):
    return 2 if delta[2] and (delta[0] or delta[1]) else 3


def vel_arrays(delta):
    return 1 if delta[0] or delta[1] else 4


def to_delta(g, delta):
    dz, dy, dx = delta
    if dx:
        xf = iota(g.shape, 1) & 15
        g = jnp.where(xf < 3, pltpu.roll(g, 244, 1), jnp.where(xf >= 13, pltpu.roll(g, 12, 1), 0.0))
    if dz:
        row = iota((8, 256), 0)
        g = jnp.where(row < 3, pltpu.roll(g[8:16], 4, 0), jnp.where(row >= 5, pltpu.roll(g[0:8], 4, 0), 0.0))
    if dy:
        lane = iota((g.shape[0], 128), 1)
        g = jnp.where(lane < 48, pltpu.roll(g[:, 128:], 64, 1), jnp.where(lane >= 80, pltpu.roll(g[:, :128], 64, 1), 0.0))
    return g


def wide(b):
    lane = iota(b.shape, 1)
    return jnp.concatenate([jnp.where(lane < 48, b, 0.0), jnp.where(lane >= 80, b, 0.0)], axis=1)


def tall(b):
    row = iota(b.shape, 0)
    return jnp.concatenate([jnp.where(row < 3, b, 0.0), jnp.where(row >= 5, b, 0.0)], axis=0)


def pack_pos(f, delta):
    if pos_arrays(delta) == 3:
        return f
    return [f[0] + pltpu.roll(f[1], 6, 1), f[2]]


def unpack_pos(a, delta):
    if pos_arrays(delta) == 3:
        return a
    n = a[0].shape[1]
    xf = iota(a[0].shape, 1) & 15
    edge = (xf < 3) | (xf >= 13)
    return [jnp.where(edge, a[0], 0.0), jnp.where(edge, pltpu.roll(a[0], n - 6, 1), 0.0), a[1]]


def pack_vel(f, delta):
    dz, dy, _ = delta
    if dz:
        row = iota(f[0].shape, 0)
        out = jnp.zeros_like(f[0])
        for k in range(4):
            out = jnp.where(row == 2 * k, jnp.broadcast_to(f[k][2:3], out.shape), out)
            out = jnp.where(row == 2 * k + 1, jnp.broadcast_to(f[k][5:6], out.shape), out)
        return [out]
    if dy:
        group = iota(f[0].shape, 1) >> 4
        out = jnp.where((group == 2) | (group == 5), f[0], 0.0)
        out = jnp.where((group == 3) | (group == 6), pltpu.roll(f[1], 16, 1), out)
        out = jnp.where((group == 4) | (group == 7), pltpu.roll(f[2], 32, 1), out)
        out = jnp.where(group == 0, pltpu.roll(f[3], 96, 1), out)
        return [jnp.where(group == 1, pltpu.roll(f[3], 64, 1), out)]
    return f


def unpack_vel(a, delta):
    dz, dy, _ = delta
    if dz:
        row = iota(a[0].shape, 0)
        return [jnp.where(row == 2, jnp.broadcast_to(a[0][2 * k:2 * k + 1], a[0].shape), jnp.where(row == 5, jnp.broadcast_to(a[0][2 * k + 1:2 * k + 2], a[0].shape), 0.0)) for k in range(4)]
    if dy:
        group = iota(a[0].shape, 1) >> 4
        low, high = group == 2, group == 5
        both = low | high
        last = jnp.where(low, pltpu.roll(a[0], 32, 1), jnp.where(high, pltpu.roll(a[0], 64, 1), 0.0))
        return [jnp.where(both, a[0], 0.0), jnp.where(both, pltpu.roll(a[0], 112, 1), 0.0), jnp.where(both, pltpu.roll(a[0], 96, 1), 0.0), last]
    return a


def merge(own, parts):
    flat = own + parts[(0, 0, 1)] + wide(parts[(0, 1, 0)] + parts[(0, 1, 1)])
    return flat + tall(parts[(1, 0, 0)] + parts[(1, 0, 1)] + wide(parts[(1, 1, 0)] + parts[(1, 1, 1)]))


def kernel(pos_ref, vel_ref, frc_ref, id_ref, val_ref, opos_ref, ovel_ref, ofrc_ref, oid_ref, oval_ref, oen_ref, *scratch):
    psend, precv, vsend, vrecv = (scratch[7 * i:7 * i + 7] for i in range(4))
    atom_ref, g_ref, t_ref, q_ref, p_ref, ebuf, psend_sem, precv_sem, vsend_sem, vrecv_sem, esend_sem, erecv_sem = scratch[28:]
    bz, by, bx = lax.axis_index("bz"), lax.axis_index("by"), lax.axis_index("bx")

    def partner(delta):
        return (lax.rem(bz + delta[0], 2), lax.rem(by + delta[1], 2), lax.rem(bx + delta[2], 2))

    barrier = pltpu.get_barrier_semaphore()
    for delta in DELTAS:
        pl.semaphore_signal(barrier, inc=1, device_id=partner(delta), device_id_type=MESH_ID)

    v_half = vel_ref[...] + (0.5 * TIME_STEP) * frc_ref[...]
    moved = pos_ref[...] + TIME_STEP * v_half
    moved = moved - BOX * jnp.floor(moved * (1.0 / BOX))
    axis_row = iota((3, 1), 0)
    coord = jnp.where(axis_row == 0, bx, jnp.where(axis_row == 1, by, bz)).astype(F32)
    brick_lo = coord * BRICK
    rel = moved - brick_lo
    rel = jnp.where(rel < -0.5 * BRICK, rel + BOX, jnp.where(rel >= 1.5 * BRICK, rel - BOX, rel))
    cell = jnp.floor(rel * (1.0 / SPACING)).astype(jnp.int32) + 2
    live = val_ref[...].reshape(1, CAP) == 1
    ids = id_ref[...].reshape(1, CAP)
    atom_ref[:, pl.ds(KPAD - 128, 128)] = jnp.zeros((atom_ref.shape[0], 128), F32)
    zi = jnp.where(live, cell[2:3, :], 0)
    lo = jnp.where(live, cell[1:2, :] * 16 + cell[0:1, :], 0)
    rows = list(split3(moved)) + list(split3(v_half))
    for k in range(6):
        atom_ref[8 * k:8 * k + 3, 0:CAP] = rows[k]
    atom_ref[48:49, 0:CAP] = (ids >> 7).astype(F32)
    atom_ref[49:50, 0:CAP] = (ids & 127).astype(F32)
    atom_ref[50:51, 0:CAP] = zi.astype(F32)
    atom_ref[51:52, 0:CAP] = lo.astype(F32)

    zrow = atom_ref[50:51, :]
    lrow = atom_ref[51:52, :]
    zmask = jnp.broadcast_to(zrow, (16, KPAD)) == iota((16, KPAD), 0).astype(F32)
    onehot = jnp.where(jnp.broadcast_to(lrow, (256, KPAD)) == iota((256, KPAD), 0).astype(F32), 1.0, 0.0).astype(BF16)

    def spread(row_idx):
        return jnp.where(zmask, jnp.broadcast_to(atom_ref[row_idx:row_idx + 1, :], (16, KPAD)), 0.0).astype(BF16)

    def exchange(src, dst, ssem, rsem):
        copies = {}
        for delta in SEND_ORDER:
            k = DELTAS.index(delta)
            copies[delta] = pltpu.make_async_remote_copy(src_ref=src[k], dst_ref=dst[k], send_sem=ssem.at[k], recv_sem=rsem.at[k], device_id=partner(delta), device_id_type=MESH_ID)
            copies[delta].start()
        return copies

    def fill(bufs, fields, pack):
        for k, delta in enumerate(DELTAS):
            rz = tile_of(delta)[0]
            for i, arr in enumerate(pack([to_delta(f, delta) for f in fields], delta)):
                bufs[k][i * rz:(i + 1) * rz, :] = arr

    def gather(own, bufs, count, unpack):
        parts = {}
        for k, delta in enumerate(DELTAS):
            rz = tile_of(delta)[0]
            parts[delta] = unpack([bufs[k][i * rz:(i + 1) * rz, :] for i in range(count(delta))], delta)
        return [merge(own[f], {d: parts[d][f] for d in DELTAS}) for f in range(len(own))]

    lhs = jnp.concatenate([spread(8 * k + c) for k in range(3) for c in range(3)], axis=0)
    binned = dot_nt(lhs, onehot)
    pos_own = [binned[16 * c:16 * c + 16] + binned[48 + 16 * c:64 + 16 * c] + binned[96 + 16 * c:112 + 16 * c] for c in range(3)]
    fill(psend, pos_own, pack_pos)
    for c in range(3):
        g_ref[16 * c:16 * c + 16, :] = pos_own[c]
    pl.semaphore_wait(barrier, 7)
    copies = exchange(psend, precv, psend_sem, precv_sem)

    lhs = jnp.concatenate([spread(8 * k + c) for k in range(3, 6) for c in range(3)] + [spread(48), spread(49)], axis=0)
    binned = dot_nt(lhs, onehot)
    vel_own = [binned[16 * c:16 * c + 16] + binned[48 + 16 * c:64 + 16 * c] + binned[96 + 16 * c:112 + 16 * c] for c in range(3)]
    vel_own.append(binned[144:160] * 128.0 + binned[160:176])
    fill(vsend, vel_own, pack_vel)
    for c in range(4):
        g_ref[48 + 16 * c:64 + 16 * c, :] = vel_own[c]
    vcopies = exchange(vsend, vrecv, vsend_sem, vrecv_sem)

    for delta in DELTAS:
        copies[delta].wait_recv()
    fields = gather([g_ref[16 * c:16 * c + 16, :] for c in range(3)], precv, pos_arrays, unpack_pos)

    present = fields[0] != 0.0
    lane = iota((16, 256), 1)
    frame = [lane & 15, lane >> 4, iota((16, 256), 0)]
    los = [bx, by, bz]
    local = []
    for c in range(3):
        u = fields[c] - los[c].astype(F32) * BRICK
        u = jnp.where(u < -0.5 * BRICK, u + BOX, jnp.where(u >= 1.5 * BRICK, u - BOX, u))
        local.append(jnp.where(present, u, 1000.0 + 10.0 * frame[c].astype(F32)))

    def shift_in(s):
        dx, dy = SHIFTS[s]
        for h in range(2):
            left = 32 + 96 * h + 16 * dy + dx
            for c in range(3):
                rolled = pltpu.roll(local[c], (256 - left) % 256, 1)
                t_ref[3 * s + c, pl.ds(h, 16, stride=2), :] = rolled[:, 0:128]

    def keep(f, x):
        for h in range(2):
            rolled = pltpu.roll(x, (256 - 32 - 96 * h) % 256, 1)
            q_ref[f, pl.ds(h, 16, stride=2), :] = rolled[:, 0:128]

    def load(dx, dy, dz):
        s = SHIFTS.index((dx, dy))
        return [t_ref[3 * s + c, 4 + 2 * dz:28 + 2 * dz, :] for c in range(3)]

    low_x = (iota((24, 128), 1) & 15) < 8
    row24 = iota((24, 128), 0)
    low_y = (row24 & 1) == 0
    low_z = row24 < 12

    def pick(mask, p, q):
        return [jnp.where(mask, p[c], q[c]) for c in range(3)]

    def half(dx, dy, dz):
        return dy > 0 or (dy == 0 and (dx > 0 or (dx == 0 and dz > 0)))

    offsets = [(dx, dy, dz) for dx, dy in SHIFTS for dz in range(-2, 3) if (dx, dy, dz) != (0, 0, 0) and (abs(dx) == 2) + (abs(dy) == 2) + (abs(dz) == 2) <= 1]
    first = [functools.partial(load, *d) for d in offsets if half(*d)]
    second = [functools.partial(load, *d) for d in offsets if not half(*d)]
    for dz in range(-1, 2):
        first.append(lambda dz=dz: pick(low_x, load(-2, 2, dz), load(2, 2, dz)))
        second.append(lambda dz=dz: pick(low_x, load(-2, -2, dz), load(2, -2, dz)))
    for dx in range(-1, 2):
        first.append(lambda dx=dx: pick(low_z, load(dx, 2, -2), load(dx, 2, 2)))
        second.append(lambda dx=dx: pick(low_z, load(dx, -2, -2), load(dx, -2, 2)))
    for dy in (1, -1):
        (first if dy == 1 else second).append(lambda dy=dy: pick(low_z, pick(low_x, load(-2, dy, -2), load(2, dy, -2)), pick(low_x, load(-2, dy, 2), load(2, dy, 2))))
    first.append(lambda: pick(low_z, load(2, 0, -2), load(2, 0, 2)))
    second.append(lambda: pick(low_z, load(-2, 0, -2), load(-2, 0, 2)))

    for s, (dx, dy) in enumerate(SHIFTS):
        if dy > 0 or (dy == 0 and dx >= 0):
            shift_in(s)
    mine = load(0, 0, 0)

    def apart(nbr):
        ex, ey, ez = mine[0] - nbr[0], mine[1] - nbr[1], mine[2] - nbr[2]
        r2 = ex * ex + ey * ey + ez * ez
        near = r2 < RCUT * RCUT
        return ex, ey, ez, r2, near, jnp.where(near, lax.rsqrt(r2), 0.0)

    sw, sr, sn = (jnp.zeros((24, 128), F32) for _ in range(3))
    for i, nbr in enumerate(first):
        ex, ey, ez, r2, near, inv = apart(nbr())
        i2 = inv * inv
        i6 = i2 * i2 * i2
        sw = sw + i6 * (i6 - 1.0)
        sr = sr + r2 * inv
        sn = sn + jnp.where(near, 1.0, 0.0)
        for k, x in enumerate((ex, ey, ez, inv)):
            p_ref[4 * i + k] = x
    keep(0, fields[0])
    lane24 = iota((24, 128), 1)
    x24 = lane24 & 15
    own = (lane24 < 96) & (x24 >= 2) & (x24 < 14) & (q_ref[0, 4:28, :] != 0.0)
    energy = 4.0 * sw - DU_CUT * sr + (RCUT * DU_CUT - U_CUT) * sn
    energy = jnp.where(own, energy, 0.0)
    me = bz * 4 + by * 2 + bx
    ebuf[me, :, :] = energy[0:8] + energy[8:16] + energy[16:24]
    ecopies = []
    for delta in SEND_ORDER:
        k = DELTAS.index(delta)
        copy = pltpu.make_async_remote_copy(src_ref=ebuf.at[me], dst_ref=ebuf.at[me], send_sem=esend_sem.at[k], recv_sem=erecv_sem.at[k], device_id=partner(delta), device_id_type=MESH_ID)
        copy.start()
        ecopies.append(copy)

    for delta in DELTAS:
        vcopies[delta].wait_recv()
    for f, x in enumerate(gather([g_ref[48 + 16 * c:64 + 16 * c, :] for c in range(4)], vrecv, vel_arrays, unpack_vel)):
        keep(3 + f, x)
    for c in range(1, 3):
        keep(c, fields[c])

    for s, (dx, dy) in enumerate(SHIFTS):
        if not (dy > 0 or (dy == 0 and dx >= 0)):
            shift_in(s)

    def push(acc, ex, ey, ez, inv):
        i2 = inv * inv
        i6 = i2 * i2 * i2
        fr = (i6 * (i6 - 0.5)) * i2 + (DU_CUT / 48.0) * inv
        return (acc[0] + fr * ex, acc[1] + fr * ey, acc[2] + fr * ez)

    acc = tuple(jnp.zeros((24, 128), F32) for _ in range(3))
    for i in range(len(first)):
        acc = push(acc, *(p_ref[4 * i + k] for k in range(4)))
    for nbr in second:
        ex, ey, ez, r2, near, inv = apart(nbr())
        acc = push(acc, ex, ey, ez, inv)
    force = [48.0 * acc[c] for c in range(3)]

    idv = jnp.where(own, q_ref[6, 4:28, :], -1.0)
    id_int = idv.astype(jnp.int32)
    id_hi = jnp.where(own, id_int >> 7, -1).astype(F32)
    id_lo = jnp.where(own, id_int & 127, -1).astype(F32)

    def flat(x, n):
        return jnp.concatenate([jnp.broadcast_to(x[r:r + 1, :], (n, 128)) for r in range(24)], axis=1)

    hot_hi = jnp.where(flat(id_hi, 128) == iota((128, 3072), 0).astype(F32), 1.0, 0.0).astype(BF16)
    lo_eq = flat(id_lo, 128) == iota((128, 3072), 0).astype(F32)
    hot_lo = jnp.where(lo_eq, 1.0, 0.0).astype(BF16)
    table = dot_nt(hot_lo, hot_hi).astype(BF16)
    r128, c128 = iota((128, 128), 0), iota((128, 128), 1)
    below = dot_nn(jnp.where(c128 < r128, 1.0, 0.0).astype(BF16), table)
    total = dot_nn(jnp.ones((128, 128), BF16), table).astype(BF16)
    before = dot_nn(total, jnp.where(r128 < c128, 1.0, 0.0).astype(BF16))
    rank_tab = below + before
    tab_hi = jnp.floor(rank_tab * (1.0 / 256.0)) * 256.0
    tab_lo = rank_tab - tab_hi
    looked = dot_nn(tab_hi.astype(BF16), hot_hi) + dot_nn(tab_lo.astype(BF16), hot_hi)
    rank = jnp.sum(jnp.where(lo_eq, looked, 0.0), axis=0, keepdims=True)
    any_own = flat(jnp.where(own, 1.0, 0.0), 1) > 0.5
    rank_hi = jnp.floor(rank * (1.0 / 256.0))
    rank_lo = jnp.where(any_own, rank - 256.0 * rank_hi, -1.0)
    rank_hi = jnp.where(any_own, rank_hi, -1.0)

    hot_slot = jnp.where(jnp.broadcast_to(rank_lo, (256, 3072)) == iota((256, 3072), 0).astype(F32), 1.0, 0.0).astype(BF16)
    hi_mask = jnp.broadcast_to(rank_hi, (8, 3072)) == iota((8, 3072), 0).astype(F32)
    outs = []
    for c in range(3):
        outs += list(split3(q_ref[c, 4:28, :]))
    for c in range(3):
        outs += list(split3(q_ref[3 + c, 4:28, :] + (0.5 * TIME_STEP) * force[c]))
    for c in range(3):
        outs += list(split3(force[c]))
    outs += [id_hi, id_lo, jnp.where(own, 1.0, 0.0)]
    lhs = jnp.concatenate([jnp.where(hi_mask, flat(x, 8), 0.0) for x in outs], axis=0).astype(BF16)
    slots = dot_nt(lhs, hot_slot)

    def field(i):
        return slots[8 * i:8 * i + 8, :]

    def put(ref, row, x):
        for h in range(7):
            n = 256 if h < 6 else CAP - 1536
            ref[row:row + 1, 256 * h:256 * h + n] = x[h:h + 1, 0:n].astype(ref.dtype)

    for c in range(3):
        put(opos_ref, c, field(3 * c) + field(3 * c + 1) + field(3 * c + 2))
        put(ovel_ref, c, field(9 + 3 * c) + field(10 + 3 * c) + field(11 + 3 * c))
        put(ofrc_ref, c, field(18 + 3 * c) + field(19 + 3 * c) + field(20 + 3 * c))
    put(oid_ref, 0, field(27) * 128.0 + field(28))
    put(oval_ref, 0, field(29))

    for copy in ecopies:
        copy.wait_recv()
    acc = ebuf[0]
    for k in range(1, 8):
        acc = acc + ebuf[k]
    oen_ref[...] = jnp.sum(jnp.sum(acc, axis=0, keepdims=True), axis=1, keepdims=True)
    for copy in list(copies.values()) + list(vcopies.values()) + ecopies:
        copy.wait_send()


def finish(pos_ref, vel_ref, frc_ref, id_ref, val_ref, en_ref, opos_ref, ovel_ref, ofrc_ref, oid_ref, oval_ref, oen_ref):
    opos_ref[...] = pos_ref[...]
    ovel_ref[...] = vel_ref[...]
    ofrc_ref[...] = frc_ref[...]
    oid_ref[...] = id_ref[...].reshape(CAP)
    oval_ref[...] = val_ref[...].reshape(CAP)
    oen_ref[...] = en_ref[...]


def solution(mesh):
    row_spec = P(BRICK_AXES, None)
    flat_spec = P(BRICK_AXES)
    vmem = pl.BlockSpec(memory_space=pltpu.VMEM)

    def local_step(pos, vel, frc, ids, valid):
        f3 = jax.ShapeDtypeStruct((3, CAP), F32)
        i1 = jax.ShapeDtypeStruct((CAP,), jnp.int32)
        outs = pl.pallas_call(
            kernel,
            out_shape=(pltpu.VMEM((3, CAP), F32),) * 3 + (pltpu.VMEM((1, CAP), jnp.int32),) * 2 + (pltpu.VMEM((1, 1), F32),),
            in_specs=[vmem] * 5,
            out_specs=(vmem,) * 6,
            scratch_shapes=[pltpu.VMEM((pos_arrays(d) * tile_of(d)[0], tile_of(d)[1]), F32) for d in DELTAS] * 2 + [pltpu.VMEM((vel_arrays(d) * tile_of(d)[0], tile_of(d)[1]), F32) for d in DELTAS] * 2 + [
                pltpu.VMEM((56, KPAD), F32),
                pltpu.VMEM((112, 256), F32),
                pltpu.VMEM((75, 32, 128), F32),
                pltpu.VMEM((NF, 32, 128), F32),
                pltpu.VMEM((192, 24, 128), F32),
                pltpu.VMEM((8, 8, 128), F32),
                pltpu.SemaphoreType.DMA((7,)),
                pltpu.SemaphoreType.DMA((7,)),
                pltpu.SemaphoreType.DMA((7,)),
                pltpu.SemaphoreType.DMA((7,)),
                pltpu.SemaphoreType.DMA((7,)),
                pltpu.SemaphoreType.DMA((7,)),
            ],
            compiler_params=pltpu.CompilerParams(collective_id=0, has_side_effects=True),
        )(pos.T, vel.T, frc.T, ids, valid)
        outs = pl.pallas_call(
            finish,
            out_shape=(f3, f3, f3, i1, i1, jax.ShapeDtypeStruct((1, 1), F32)),
            in_specs=[vmem] * 6,
            out_specs=(vmem,) * 6,
            compiler_params=pltpu.CompilerParams(vmem_limit_bytes=4 << 20),
        )(*outs)
        return outs[0].T, outs[1].T, outs[2].T, outs[3], outs[4], outs[5][0, 0]

    return jax.shard_map(local_step, mesh=mesh, in_specs=(row_spec, row_spec, row_spec, flat_spec, flat_spec), out_specs=(row_spec, row_spec, row_spec, flat_spec, flat_spec, P()), check_vma=False)
```

```python
import functools

import jax
import jax.numpy as jnp
from jax import lax
from jax.experimental import pallas as pl
from jax.experimental.pallas import tpu as pltpu
from jax.sharding import PartitionSpec as P

TIME_STEP = 0.005
RCUT = 2.5
DENSITY = 0.8442
SPACING = (1.0 / DENSITY) ** (1.0 / 3.0)
SITES = 12
BRICK = SITES * SPACING
BOX = 2.0 * BRICK
BRICK_AXES = ("bz", "by", "bx")
CAP = SITES ** 3
KPAD = 1792
MESH_ID = pl.DeviceIdType.MESH
F32 = jnp.float32
BF16 = jnp.bfloat16
CUT6 = RCUT ** -6
U_CUT = 4.0 * (CUT6 * CUT6 - CUT6)
DU_CUT = (-48.0 * CUT6 * CUT6 + 24.0 * CUT6) / RCUT
DELTAS = [(d >> 2 & 1, d >> 1 & 1, d & 1) for d in range(1, 8)]
SEND_ORDER = [(1, 1, 0), (1, 1, 1), (0, 1, 0), (1, 0, 0), (0, 1, 1), (1, 0, 1), (0, 0, 1)]
SHIFTS = [(dx, dy) for dy in range(-2, 3) for dx in range(-2, 3)]
NF = 7


def iota(shape, dim):
    return lax.broadcasted_iota(jnp.int32, shape, dim)


def split3(x):
    hi = x.astype(BF16).astype(F32)
    rest = x - hi
    mid = rest.astype(BF16).astype(F32)
    return hi, mid, rest - mid


def dot_nt(a, b):
    return lax.dot_general(a, b, (((1,), (1,)), ((), ())), preferred_element_type=F32)


def dot_split(a, b, true):
    cut = a.shape[1] // 512 * 256
    return dot_nt(a[:, :cut], b[:, :cut]) + jnp.where(true, dot_nt(a[:, cut:], b[:, cut:]), 0.0)


def dot_nn(a, b):
    return lax.dot_general(a, b, (((1,), (0,)), ((), ())), preferred_element_type=F32)


def tile_of(delta):
    return 8 if delta[0] else 16, 128 if delta[1] else 256


def pos_arrays(delta):
    return 2 if delta[2] and (delta[0] or delta[1]) else 3


def vel_arrays(delta):
    return 1 if delta[0] or delta[1] else 4


def offsets_of(arrays):
    starts, row = {}, 0
    for delta in DELTAS:
        starts[delta] = row
        rz, lanes = tile_of(delta)
        row += arrays(delta) * rz * lanes // 128
    return starts, row


def to_delta(g, delta):
    dz, dy, dx = delta
    if dx:
        xf = iota(g.shape, 1) & 15
        g = jnp.where(xf < 3, pltpu.roll(g, 244, 1), jnp.where(xf >= 13, pltpu.roll(g, 12, 1), 0.0))
    if dz:
        row = iota((8, 256), 0)
        g = jnp.where(row < 3, pltpu.roll(g[8:16], 4, 0), jnp.where(row >= 5, pltpu.roll(g[0:8], 4, 0), 0.0))
    if dy:
        lane = iota((g.shape[0], 128), 1)
        g = jnp.where(lane < 48, pltpu.roll(g[:, 128:], 64, 1), jnp.where(lane >= 80, pltpu.roll(g[:, :128], 64, 1), 0.0))
    return g


def wide(b):
    lane = iota(b.shape, 1)
    return jnp.concatenate([jnp.where(lane < 48, b, 0.0), jnp.where(lane >= 80, b, 0.0)], axis=1)


def tall(b):
    row = iota(b.shape, 0)
    return jnp.concatenate([jnp.where(row < 3, b, 0.0), jnp.where(row >= 5, b, 0.0)], axis=0)


def pack_pos(f, delta):
    if pos_arrays(delta) == 3:
        return f
    return [f[0] + pltpu.roll(f[1], 6, 1), f[2]]


def unpack_pos(a, delta):
    if pos_arrays(delta) == 3:
        return a
    n = a[0].shape[1]
    xf = iota(a[0].shape, 1) & 15
    edge = (xf < 3) | (xf >= 13)
    return [jnp.where(edge, a[0], 0.0), jnp.where(edge, pltpu.roll(a[0], n - 6, 1), 0.0), a[1]]


def pack_vel(f, delta):
    dz, dy, _ = delta
    if dz:
        row = iota(f[0].shape, 0)
        out = jnp.zeros_like(f[0])
        for k in range(4):
            out = jnp.where(row == 2 * k, jnp.broadcast_to(f[k][2:3], out.shape), out)
            out = jnp.where(row == 2 * k + 1, jnp.broadcast_to(f[k][5:6], out.shape), out)
        return [out]
    if dy:
        group = iota(f[0].shape, 1) >> 4
        out = jnp.where((group == 2) | (group == 5), f[0], 0.0)
        out = jnp.where((group == 3) | (group == 6), pltpu.roll(f[1], 16, 1), out)
        out = jnp.where((group == 4) | (group == 7), pltpu.roll(f[2], 32, 1), out)
        out = jnp.where(group == 0, pltpu.roll(f[3], 96, 1), out)
        return [jnp.where(group == 1, pltpu.roll(f[3], 64, 1), out)]
    return f


def unpack_vel(a, delta):
    dz, dy, _ = delta
    if dz:
        row = iota(a[0].shape, 0)
        return [jnp.where(row == 2, jnp.broadcast_to(a[0][2 * k:2 * k + 1], a[0].shape), jnp.where(row == 5, jnp.broadcast_to(a[0][2 * k + 1:2 * k + 2], a[0].shape), 0.0)) for k in range(4)]
    if dy:
        group = iota(a[0].shape, 1) >> 4
        low, high = group == 2, group == 5
        both = low | high
        last = jnp.where(low, pltpu.roll(a[0], 32, 1), jnp.where(high, pltpu.roll(a[0], 64, 1), 0.0))
        return [jnp.where(both, a[0], 0.0), jnp.where(both, pltpu.roll(a[0], 112, 1), 0.0), jnp.where(both, pltpu.roll(a[0], 96, 1), 0.0), last]
    return a


def merge(own, parts):
    flat = own + parts[(0, 0, 1)] + wide(parts[(0, 1, 0)] + parts[(0, 1, 1)])
    return flat + tall(parts[(1, 0, 0)] + parts[(1, 0, 1)] + wide(parts[(1, 1, 0)] + parts[(1, 1, 1)]))


def kernel(pos_hbm, vel_hbm, frc_hbm, id_hbm, val_hbm, opos_ref, ovel_ref, ofrc_ref, oid_ref, oval_ref, oen_ref, *scratch):
    psend, precv, vsend, vrecv, pos_ref, vel_ref, frc_ref, id_ref, val_ref, in_sem, atom_ref, g_ref, t_ref, q_ref, p_ref, ebuf, psend_sem, precv_sem, vsend_sem, vrecv_sem, esend_sem, erecv_sem = scratch
    loads = [pltpu.make_async_copy(src, dst, in_sem.at[i]) for i, (src, dst) in enumerate(((vel_hbm, vel_ref), (frc_hbm, frc_ref), (pos_hbm, pos_ref), (val_hbm, val_ref), (id_hbm, id_ref)))]
    for copy in loads:
        copy.start()
    bz, by, bx = lax.axis_index("bz"), lax.axis_index("by"), lax.axis_index("bx")

    true = bz >= 0

    def partner(delta):
        return (lax.rem(bz + delta[0], 2), lax.rem(by + delta[1], 2), lax.rem(bx + delta[2], 2))

    barrier = pltpu.get_barrier_semaphore()
    for delta in DELTAS:
        pl.semaphore_signal(barrier, inc=1, device_id=partner(delta), device_id_type=MESH_ID)

    for copy in loads:
        copy.wait()
    v_half = vel_ref[...] + (0.5 * TIME_STEP) * frc_ref[...]
    moved = pos_ref[...] + TIME_STEP * v_half
    moved = moved - BOX * jnp.floor(moved * (1.0 / BOX))
    axis_row = iota((3, 1), 0)
    coord = jnp.where(axis_row == 0, bx, jnp.where(axis_row == 1, by, bz)).astype(F32)
    brick_lo = coord * BRICK
    rel = moved - brick_lo
    rel = jnp.where(rel < -0.5 * BRICK, rel + BOX, jnp.where(rel >= 1.5 * BRICK, rel - BOX, rel))
    cell = jnp.floor(rel * (1.0 / SPACING)).astype(jnp.int32) + 2
    live = val_ref[...].reshape(1, CAP) == 1
    ids = id_ref[...].reshape(1, CAP)
    atom_ref[:, pl.ds(KPAD - 128, 128)] = jnp.zeros((atom_ref.shape[0], 128), F32)
    zi = jnp.where(live, cell[2:3, :], 0)
    lo = jnp.where(live, cell[1:2, :] * 16 + cell[0:1, :], 0)
    rows = list(split3(moved)) + list(split3(v_half))
    for k in range(6):
        atom_ref[8 * k:8 * k + 3, 0:CAP] = rows[k]
    atom_ref[48:49, 0:CAP] = (ids >> 7).astype(F32)
    atom_ref[49:50, 0:CAP] = (ids & 127).astype(F32)
    atom_ref[50:51, 0:CAP] = zi.astype(F32)
    atom_ref[51:52, 0:CAP] = lo.astype(F32)

    zrow = atom_ref[50:51, :]
    lrow = atom_ref[51:52, :]
    zmask = jnp.broadcast_to(zrow, (16, KPAD)) == iota((16, KPAD), 0).astype(F32)
    onehot = jnp.where(jnp.broadcast_to(lrow, (256, KPAD)) == iota((256, KPAD), 0).astype(F32), 1.0, 0.0).astype(BF16)

    def spread(row_idx):
        return jnp.where(zmask, jnp.broadcast_to(atom_ref[row_idx:row_idx + 1, :], (16, KPAD)), 0.0).astype(BF16)

    def exchange(src, dst, ssem, rsem, arrays):
        starts, total = offsets_of(arrays)
        for delta in SEND_ORDER:
            rz, lanes = tile_of(delta)
            part = pl.ds(starts[delta], arrays(delta) * rz * lanes // 128)
            pltpu.make_async_remote_copy(src_ref=src.at[part], dst_ref=dst.at[part], send_sem=ssem, recv_sem=rsem, device_id=partner(delta), device_id_type=MESH_ID).start()
        return pltpu.make_async_remote_copy(src_ref=src, dst_ref=dst, send_sem=ssem, recv_sem=rsem, device_id=partner(DELTAS[0]), device_id_type=MESH_ID)

    def fill(buf, fields, pack, arrays):
        starts, _ = offsets_of(arrays)
        for delta in DELTAS:
            rz, lanes = tile_of(delta)
            row = starts[delta]
            for arr in pack([to_delta(f, delta) for f in fields], delta):
                for j in range(lanes // 128):
                    buf[row:row + rz, :] = arr[:, 128 * j:128 * j + 128]
                    row += rz

    def gather(own, buf, arrays, unpack):
        starts, _ = offsets_of(arrays)
        parts = {}
        for delta in DELTAS:
            rz, lanes = tile_of(delta)
            row = starts[delta]
            arrs = []
            for i in range(arrays(delta)):
                pieces = [buf[row + rz * j:row + rz * j + rz, :] for j in range(lanes // 128)]
                row += rz * len(pieces)
                arrs.append(pieces[0] if len(pieces) == 1 else jnp.concatenate(pieces, axis=1))
            parts[delta] = unpack(arrs, delta)
        return [merge(own[f], {d: parts[d][f] for d in DELTAS}) for f in range(len(own))]

    lhs = jnp.concatenate([spread(8 * k + c) for k in range(3) for c in range(3)], axis=0)
    binned = dot_split(lhs, onehot, true)
    pos_own = [binned[16 * c:16 * c + 16] + binned[48 + 16 * c:64 + 16 * c] + binned[96 + 16 * c:112 + 16 * c] for c in range(3)]
    fill(psend, pos_own, pack_pos, pos_arrays)
    for c in range(3):
        g_ref[16 * c:16 * c + 16, :] = pos_own[c]
    pl.semaphore_wait(barrier, 7)
    pos_all = exchange(psend, precv, psend_sem, precv_sem, pos_arrays)

    lhs = jnp.concatenate([spread(8 * k + c) for k in range(3, 6) for c in range(3)] + [spread(48), spread(49)], axis=0)
    binned = dot_split(lhs, onehot, true)
    vel_own = [binned[16 * c:16 * c + 16] + binned[48 + 16 * c:64 + 16 * c] + binned[96 + 16 * c:112 + 16 * c] for c in range(3)]
    vel_own.append(binned[144:160] * 128.0 + binned[160:176])
    fill(vsend, vel_own, pack_vel, vel_arrays)
    for c in range(4):
        g_ref[48 + 16 * c:64 + 16 * c, :] = vel_own[c]
    vel_all = exchange(vsend, vrecv, vsend_sem, vrecv_sem, vel_arrays)

    pos_all.wait_recv()
    fields = gather([g_ref[16 * c:16 * c + 16, :] for c in range(3)], precv, pos_arrays, unpack_pos)

    present = fields[0] != 0.0
    lane = iota((16, 256), 1)
    frame = [lane & 15, lane >> 4, iota((16, 256), 0)]
    los = [bx, by, bz]
    local = []
    for c in range(3):
        u = fields[c] - los[c].astype(F32) * BRICK
        u = jnp.where(u < -0.5 * BRICK, u + BOX, jnp.where(u >= 1.5 * BRICK, u - BOX, u))
        local.append(jnp.where(present, u, 64.0 + 4.0 * frame[c].astype(F32)))

    def shift_in(s):
        dx, dy = SHIFTS[s]
        for h in range(2):
            left = 32 + 96 * h + 16 * dy + dx
            for c in range(3):
                rolled = pltpu.roll(local[c], (256 - left) % 256, 1)
                t_ref[3 * s + c, pl.ds(h, 16, stride=2), :] = rolled[:, 0:128]

    def keep(f, x):
        for h in range(2):
            rolled = pltpu.roll(x, (256 - 32 - 96 * h) % 256, 1)
            q_ref[f, pl.ds(h, 16, stride=2), :] = rolled[:, 0:128]

    def load(dx, dy, dz):
        s = SHIFTS.index((dx, dy))
        return [t_ref[3 * s + c, 4 + 2 * dz:28 + 2 * dz, :] for c in range(3)]

    low_x = (iota((24, 128), 1) & 15) < 8
    row24 = iota((24, 128), 0)
    low_y = (row24 & 1) == 0
    low_z = row24 < 12

    def pick(mask, p, q):
        return [jnp.where(mask, p[c], q[c]) for c in range(3)]

    def half(dx, dy, dz):
        return dy > 0 or (dy == 0 and (dx > 0 or (dx == 0 and dz > 0)))

    offsets = [(dx, dy, dz) for dx, dy in SHIFTS for dz in range(-2, 3) if (dx, dy, dz) != (0, 0, 0) and (abs(dx) == 2) + (abs(dy) == 2) + (abs(dz) == 2) <= 1]
    first = [functools.partial(load, *d) for d in offsets if half(*d)]
    second = [functools.partial(load, *d) for d in offsets if not half(*d)]
    for dz in range(-1, 2):
        first.append(lambda dz=dz: pick(low_x, load(-2, 2, dz), load(2, 2, dz)))
        second.append(lambda dz=dz: pick(low_x, load(-2, -2, dz), load(2, -2, dz)))
    for dx in range(-1, 2):
        first.append(lambda dx=dx: pick(low_z, load(dx, 2, -2), load(dx, 2, 2)))
        second.append(lambda dx=dx: pick(low_z, load(dx, -2, -2), load(dx, -2, 2)))
    for dy in (1, -1):
        (first if dy == 1 else second).append(lambda dy=dy: pick(low_z, pick(low_x, load(-2, dy, -2), load(2, dy, -2)), pick(low_x, load(-2, dy, 2), load(2, dy, 2))))
    first.append(lambda: pick(low_z, load(2, 0, -2), load(2, 0, 2)))
    second.append(lambda: pick(low_z, load(-2, 0, -2), load(-2, 0, 2)))

    for s, (dx, dy) in enumerate(SHIFTS):
        if dy > 0 or (dy == 0 and dx >= 0):
            shift_in(s)
    mine = load(0, 0, 0)

    def apart(nbr):
        ex, ey, ez = mine[0] - nbr[0], mine[1] - nbr[1], mine[2] - nbr[2]
        r2 = ex * ex + ey * ey + ez * ez
        r2 = jnp.minimum(r2, RCUT * RCUT)
        return ex, ey, ez, r2, lax.rsqrt(r2)

    sw, sr = jnp.zeros((24, 128), F32), jnp.zeros((24, 128), F32)
    for i, nbr in enumerate(first):
        ex, ey, ez, r2, inv = apart(nbr())
        i2 = inv * inv
        i6 = i2 * i2 * i2
        sw = sw + i6 * (i6 - 1.0)
        sr = sr + r2 * inv
        for k, x in enumerate((ex, ey, ez, inv)):
            p_ref[4 * i + k] = x
    keep(0, fields[0])
    lane24 = iota((24, 128), 1)
    x24 = lane24 & 15
    own = (lane24 < 96) & (x24 >= 2) & (x24 < 14) & (q_ref[0, 4:28, :] != 0.0)
    energy = 4.0 * sw - DU_CUT * sr + (RCUT * DU_CUT - U_CUT) * len(first)
    energy = jnp.where(own, energy, 0.0)
    me = bz * 4 + by * 2 + bx
    ebuf[me, :, :] = energy[0:8] + energy[8:16] + energy[16:24]
    for delta in SEND_ORDER:
        pltpu.make_async_remote_copy(src_ref=ebuf.at[me], dst_ref=ebuf.at[me], send_sem=esend_sem, recv_sem=erecv_sem, device_id=partner(delta), device_id_type=MESH_ID).start()
    energy_all = pltpu.make_async_remote_copy(src_ref=ebuf.at[pl.ds(0, 7)], dst_ref=ebuf.at[pl.ds(0, 7)], send_sem=esend_sem, recv_sem=erecv_sem, device_id=partner(DELTAS[0]), device_id_type=MESH_ID)

    vel_all.wait_recv()
    for f, x in enumerate(gather([g_ref[48 + 16 * c:64 + 16 * c, :] for c in range(4)], vrecv, vel_arrays, unpack_vel)):
        keep(3 + f, x)
    for c in range(1, 3):
        keep(c, fields[c])

    for s, (dx, dy) in enumerate(SHIFTS):
        if not (dy > 0 or (dy == 0 and dx >= 0)):
            shift_in(s)

    def push(acc, ex, ey, ez, inv):
        i2 = inv * inv
        i6 = i2 * i2 * i2
        fr = (i6 * (i6 - 0.5)) * i2 + (DU_CUT / 48.0) * inv
        return (acc[0] + fr * ex, acc[1] + fr * ey, acc[2] + fr * ez)

    acc = tuple(jnp.zeros((24, 128), F32) for _ in range(3))
    for i in range(len(first)):
        acc = push(acc, *(p_ref[4 * i + k] for k in range(4)))
    for nbr in second:
        ex, ey, ez, r2, inv = apart(nbr())
        acc = push(acc, ex, ey, ez, inv)
    force = [48.0 * acc[c] for c in range(3)]

    idv = jnp.where(own, q_ref[6, 4:28, :], -1.0)
    id_int = idv.astype(jnp.int32)
    id_hi = jnp.where(own, id_int >> 7, -1).astype(F32)
    id_lo = jnp.where(own, id_int & 127, -1).astype(F32)

    def flat(x, n):
        return jnp.concatenate([jnp.broadcast_to(x[r:r + 1, :], (n, 128)) for r in range(24)], axis=1)

    hot_hi = jnp.where(flat(id_hi, 128) == iota((128, 3072), 0).astype(F32), 1.0, 0.0).astype(BF16)
    lo_eq = flat(id_lo, 128) == iota((128, 3072), 0).astype(F32)
    hot_lo = jnp.where(lo_eq, 1.0, 0.0).astype(BF16)
    table = dot_split(hot_lo, hot_hi, true).astype(BF16)
    r128, c128 = iota((128, 128), 0), iota((128, 128), 1)
    below = dot_nn(jnp.where(c128 < r128, 1.0, 0.0).astype(BF16), table)
    total = dot_nn(jnp.ones((128, 128), BF16), table).astype(BF16)
    before = dot_nn(total, jnp.where(r128 < c128, 1.0, 0.0).astype(BF16))
    rank_tab = below + before
    tab_hi = jnp.floor(rank_tab * (1.0 / 256.0)) * 256.0
    tab_lo = rank_tab - tab_hi
    tabs = jnp.concatenate([tab_hi, tab_lo], axis=1).astype(BF16)
    hot2 = jnp.concatenate([hot_hi, hot_hi], axis=0)
    looked = jnp.concatenate([dot_nn(tabs, hot2[:, :1536]), dot_nn(tabs, hot2[:, 1536:])], axis=1)
    rank = jnp.sum(jnp.where(lo_eq, looked, 0.0), axis=0, keepdims=True)
    any_own = flat(jnp.where(own, 1.0, 0.0), 1) > 0.5
    rank_hi = jnp.floor(rank * (1.0 / 256.0))
    rank_lo = jnp.where(any_own, rank - 256.0 * rank_hi, -1.0)
    rank_hi = jnp.where(any_own, rank_hi, -1.0)

    hot_slot = jnp.where(jnp.broadcast_to(rank_lo, (256, 3072)) == iota((256, 3072), 0).astype(F32), 1.0, 0.0).astype(BF16)
    hi_mask = jnp.broadcast_to(rank_hi, (8, 3072)) == iota((8, 3072), 0).astype(F32)
    outs = []
    for c in range(3):
        outs += list(split3(q_ref[c, 4:28, :]))
    for c in range(3):
        outs += list(split3(q_ref[3 + c, 4:28, :] + (0.5 * TIME_STEP) * force[c]))
    for c in range(3):
        outs += list(split3(force[c]))
    outs += [id_hi, id_lo, jnp.where(own, 1.0, 0.0)]
    lhs = jnp.concatenate([jnp.where(hi_mask, flat(x, 8), 0.0) for x in outs], axis=0).astype(BF16)
    slots = dot_split(lhs, hot_slot, true)

    def field(i):
        return slots[8 * i:8 * i + 8, :]

    def put(ref, row, x):
        for h in range(7):
            n = 256 if h < 6 else CAP - 1536
            ref[row:row + 1, 256 * h:256 * h + n] = x[h:h + 1, 0:n].astype(ref.dtype)

    for c in range(3):
        put(opos_ref, c, field(3 * c) + field(3 * c + 1) + field(3 * c + 2))
        put(ovel_ref, c, field(9 + 3 * c) + field(10 + 3 * c) + field(11 + 3 * c))
        put(ofrc_ref, c, field(18 + 3 * c) + field(19 + 3 * c) + field(20 + 3 * c))
    put(oid_ref, 0, field(27) * 128.0 + field(28))
    put(oval_ref, 0, field(29))

    for copy in (pos_all, vel_all, energy_all):
        copy.wait_send()
    energy_all.wait_recv()
    acc = ebuf[0]
    for k in range(1, 8):
        acc = acc + ebuf[k]
    oen_ref[...] = jnp.sum(jnp.sum(acc, axis=0, keepdims=True), axis=1, keepdims=True)


def finish(pos_ref, vel_ref, frc_ref, id_ref, val_ref, en_ref, opos_ref, ovel_ref, ofrc_ref, oid_ref, oval_ref, oen_ref):
    opos_ref[...] = pos_ref[...]
    ovel_ref[...] = vel_ref[...]
    ofrc_ref[...] = frc_ref[...]
    oid_ref[...] = id_ref[...].reshape(CAP)
    oval_ref[...] = val_ref[...].reshape(CAP)
    oen_ref[...] = en_ref[...]


def solution(mesh):
    row_spec = P(BRICK_AXES, None)
    flat_spec = P(BRICK_AXES)
    vmem = pl.BlockSpec(memory_space=pltpu.VMEM)

    def local_step(pos, vel, frc, ids, valid):
        f3 = jax.ShapeDtypeStruct((3, CAP), F32)
        i1 = jax.ShapeDtypeStruct((CAP,), jnp.int32)
        outs = pl.pallas_call(
            kernel,
            out_shape=(pltpu.VMEM((3, CAP), F32),) * 3 + (pltpu.VMEM((1, CAP), jnp.int32),) * 2 + (pltpu.VMEM((1, 1), F32),),
            in_specs=[pl.BlockSpec(memory_space=pltpu.HBM)] * 5,
            out_specs=(vmem,) * 6,
            scratch_shapes=[pltpu.VMEM((offsets_of(pos_arrays)[1], 128), F32)] * 2 + [pltpu.VMEM((offsets_of(vel_arrays)[1], 128), F32)] * 2 + [
                pltpu.VMEM((3, CAP), F32),
                pltpu.VMEM((3, CAP), F32),
                pltpu.VMEM((3, CAP), F32),
                pltpu.VMEM((CAP,), jnp.int32),
                pltpu.VMEM((CAP,), jnp.int32),
                pltpu.SemaphoreType.DMA((5,)),
                pltpu.VMEM((56, KPAD), F32),
                pltpu.VMEM((112, 256), F32),
                pltpu.VMEM((75, 32, 128), F32),
                pltpu.VMEM((NF, 32, 128), F32),
                pltpu.VMEM((192, 24, 128), F32),
                pltpu.VMEM((8, 8, 128), F32),
                pltpu.SemaphoreType.DMA,
                pltpu.SemaphoreType.DMA,
                pltpu.SemaphoreType.DMA,
                pltpu.SemaphoreType.DMA,
                pltpu.SemaphoreType.DMA,
                pltpu.SemaphoreType.DMA,
            ],
            compiler_params=pltpu.CompilerParams(collective_id=0, has_side_effects=True),
        )(pos.T, vel.T, frc.T, ids, valid)
        outs = pl.pallas_call(
            finish,
            out_shape=(f3, f3, f3, i1, i1, jax.ShapeDtypeStruct((1, 1), F32)),
            in_specs=[vmem] * 6,
            out_specs=(vmem,) * 6,
            compiler_params=pltpu.CompilerParams(vmem_limit_bytes=4 << 20),
        )(*outs)
        return outs[0].T, outs[1].T, outs[2].T, outs[3], outs[4], outs[5][0, 0]

    return jax.shard_map(local_step, mesh=mesh, in_specs=(row_spec, row_spec, row_spec, flat_spec, flat_spec), out_specs=(row_spec, row_spec, row_spec, flat_spec, flat_spec, P()), check_vma=False)
```

```python
import functools

import jax
import jax.numpy as jnp
from jax import lax
from jax.experimental import pallas as pl
from jax.experimental.pallas import tpu as pltpu
from jax.sharding import PartitionSpec as P

TIME_STEP = 0.005
RCUT = 2.5
DENSITY = 0.8442
SPACING = (1.0 / DENSITY) ** (1.0 / 3.0)
SITES = 12
BRICK = SITES * SPACING
BOX = 2.0 * BRICK
BRICK_AXES = ("bz", "by", "bx")
CAP = SITES ** 3
KPAD = 1792
MESH_ID = pl.DeviceIdType.MESH
F32 = jnp.float32
BF16 = jnp.bfloat16
CUT6 = RCUT ** -6
U_CUT = 4.0 * (CUT6 * CUT6 - CUT6)
DU_CUT = (-48.0 * CUT6 * CUT6 + 24.0 * CUT6) / RCUT
DELTAS = [(d >> 2 & 1, d >> 1 & 1, d & 1) for d in range(1, 8)]
SEND_ORDER = [(1, 1, 0), (1, 1, 1), (0, 1, 0), (1, 0, 0), (0, 1, 1), (1, 0, 1), (0, 0, 1)]
SHIFTS = [(dx, dy) for dy in range(-2, 3) for dx in range(-2, 3)]
NF = 7


def iota(shape, dim):
    return lax.broadcasted_iota(jnp.int32, shape, dim)


def split3(x):
    hi = x.astype(BF16).astype(F32)
    rest = x - hi
    mid = rest.astype(BF16).astype(F32)
    return hi, mid, rest - mid


def dot_nt(a, b):
    return lax.dot_general(a, b, (((1,), (1,)), ((), ())), preferred_element_type=F32)


def dot_split(a, b, true):
    cut = a.shape[1] // 512 * 256
    return dot_nt(a[:, :cut], b[:, :cut]) + jnp.where(true, dot_nt(a[:, cut:], b[:, cut:]), 0.0)


def dot_nn(a, b):
    return lax.dot_general(a, b, (((1,), (0,)), ((), ())), preferred_element_type=F32)


def tile_of(delta):
    return 8 if delta[0] else 16, 128 if delta[1] else 256


def pos_arrays(delta):
    return 3


def vel_arrays(delta):
    return 1 if delta[0] or delta[1] else 4


def offsets_of(arrays):
    starts, row = {}, 0
    for delta in DELTAS:
        starts[delta] = row
        row += part_rows(arrays, delta)
    return starts, row


def part_rows(arrays, delta):
    rz, lanes = tile_of(delta)
    if arrays is pos_arrays:
        rz = 6 if delta[0] else 14
    return arrays(delta) * rz * lanes // 128


def to_delta(g_ref, f, delta):
    dz, dy, dx = delta
    first = 24 * f + 4
    halves = []
    for h in range(2):
        if dz:
            row = iota((8, 128), 0)
            halves.append(jnp.where(row < 3, g_ref[h, first + 12:first + 20, :], jnp.where(row >= 5, g_ref[h, first - 4:first + 4, :], 0.0)))
        else:
            halves.append(g_ref[h, first:first + 16, :])
    lane = iota(halves[0].shape, 1)
    xf = lane & 15

    def along_x(x, turn):
        if not dx:
            return pltpu.roll(x, turn, 1) if turn else x
        return jnp.where(xf < 3, pltpu.roll(x, (turn + 116) % 128, 1), jnp.where(xf >= 13, pltpu.roll(x, turn + 12, 1), 0.0))

    if dy:
        return [jnp.where(lane < 48, along_x(halves[1], 64), jnp.where(lane >= 80, along_x(halves[0], 64), 0.0))]
    return [along_x(x, 0) for x in halves]


def wide(b):
    lane = iota(b.shape, 1)
    return [jnp.where(lane < 48, b, 0.0), jnp.where(lane >= 80, b, 0.0)]


def tall(b):
    row = iota(b.shape, 0)
    return jnp.concatenate([jnp.where(row < 3, b, 0.0), jnp.where(row >= 5, b, 0.0)], axis=0)


def same(f, delta):
    return f


def pack_vel(f, delta):
    dz, dy, _ = delta
    if dz:
        row = iota(f[0][0].shape, 0)
        outs = []
        for j in range(len(f[0])):
            out = jnp.zeros_like(f[0][j])
            for k in range(4):
                out = jnp.where(row == 2 * k, jnp.broadcast_to(f[k][j][2:3], out.shape), out)
                out = jnp.where(row == 2 * k + 1, jnp.broadcast_to(f[k][j][5:6], out.shape), out)
            outs.append(out)
        return [outs]
    if dy:
        f = [x[0] for x in f]
        group = iota(f[0].shape, 1) >> 4
        out = jnp.where((group == 2) | (group == 5), f[0], 0.0)
        out = jnp.where((group == 3) | (group == 6), pltpu.roll(f[1], 16, 1), out)
        out = jnp.where((group == 4) | (group == 7), pltpu.roll(f[2], 32, 1), out)
        out = jnp.where(group == 0, pltpu.roll(f[3], 96, 1), out)
        return [[jnp.where(group == 1, pltpu.roll(f[3], 64, 1), out)]]
    return f


def unpack_vel(a, delta):
    dz, dy, _ = delta
    if dz:
        row = iota(a[0][0].shape, 0)
        return [[jnp.where(row == 2, jnp.broadcast_to(x[2 * k:2 * k + 1], x.shape), jnp.where(row == 5, jnp.broadcast_to(x[2 * k + 1:2 * k + 2], x.shape), 0.0)) for x in a[0]] for k in range(4)]
    if dy:
        x = a[0][0]
        group = iota(x.shape, 1) >> 4
        low, high = group == 2, group == 5
        both = low | high
        last = jnp.where(low, pltpu.roll(x, 32, 1), jnp.where(high, pltpu.roll(x, 64, 1), 0.0))
        return [[jnp.where(both, x, 0.0)], [jnp.where(both, pltpu.roll(x, 112, 1), 0.0)], [jnp.where(both, pltpu.roll(x, 96, 1), 0.0)], [last]]
    return a


def merge(own, parts):
    near = wide(parts[(0, 1, 0)][0] + parts[(0, 1, 1)][0])
    far = wide(parts[(1, 1, 0)][0] + parts[(1, 1, 1)][0])
    return jnp.concatenate([(own[h] + parts[(0, 0, 1)][h] + near[h]) + tall(parts[(1, 0, 0)][h] + parts[(1, 0, 1)][h] + far[h]) for h in range(2)], axis=1)


def kernel(pos_hbm, vel_hbm, frc_hbm, id_hbm, val_hbm, opos_ref, ovel_ref, ofrc_ref, oid_ref, oval_ref, oen_ref, *scratch):
    psend, precv, vsend, vrecv, pos_ref, vel_ref, frc_ref, id_ref, val_ref, in_sem, atom_ref, g_ref, t_ref, q_ref, p_ref, ebuf, psend_sem, precv_sem, vsend_sem, vrecv_sem, esend_sem, erecv_sem = scratch
    loads = [pltpu.make_async_copy(src, dst, in_sem.at[i]) for i, (src, dst) in enumerate(((vel_hbm, vel_ref), (frc_hbm, frc_ref), (pos_hbm, pos_ref), (val_hbm, val_ref), (id_hbm, id_ref)))]
    for copy in loads:
        copy.start()
    bz, by, bx = lax.axis_index("bz"), lax.axis_index("by"), lax.axis_index("bx")

    true = bz >= 0

    def partner(delta):
        return (lax.rem(bz + delta[0], 2), lax.rem(by + delta[1], 2), lax.rem(bx + delta[2], 2))

    barrier = pltpu.get_barrier_semaphore()
    for delta in DELTAS:
        pl.semaphore_signal(barrier, inc=1, device_id=partner(delta), device_id_type=MESH_ID)

    for f in range(NF):
        for h in range(2):
            g_ref[h, 24 * f:24 * f + 4, :] = jnp.zeros((4, 128), F32)
            g_ref[h, 24 * f + 20:24 * f + 24, :] = jnp.zeros((4, 128), F32)

    for copy in loads:
        copy.wait()
    v_half = vel_ref[...] + (0.5 * TIME_STEP) * frc_ref[...]
    moved = pos_ref[...] + TIME_STEP * v_half
    moved = moved - BOX * jnp.floor(moved * (1.0 / BOX))
    axis_row = iota((3, 1), 0)
    coord = jnp.where(axis_row == 0, bx, jnp.where(axis_row == 1, by, bz)).astype(F32)
    brick_lo = coord * BRICK
    rel = moved - brick_lo
    rel = jnp.where(rel < -0.5 * BRICK, rel + BOX, jnp.where(rel >= 1.5 * BRICK, rel - BOX, rel))
    cell = jnp.floor(rel * (1.0 / SPACING)).astype(jnp.int32) + 2
    live = val_ref[...].reshape(1, CAP) == 1
    ids = id_ref[...].reshape(1, CAP)
    atom_ref[:, pl.ds(KPAD - 128, 128)] = jnp.zeros((atom_ref.shape[0], 128), F32)
    zi = jnp.where(live, cell[2:3, :], 0)
    lo = jnp.where(live, cell[1:2, :] * 16 + cell[0:1, :], 0)
    rows = list(split3(moved)) + list(split3(v_half))
    for k in range(6):
        atom_ref[8 * k:8 * k + 3, 0:CAP] = rows[k]
    atom_ref[48:49, 0:CAP] = (ids >> 7).astype(F32)
    atom_ref[49:50, 0:CAP] = (ids & 127).astype(F32)
    atom_ref[50:51, 0:CAP] = zi.astype(F32)
    atom_ref[51:52, 0:CAP] = lo.astype(F32)

    zrow = atom_ref[50:51, :]
    lrow = atom_ref[51:52, :]
    zmask = jnp.broadcast_to(zrow, (16, KPAD)) == iota((16, KPAD), 0).astype(F32)
    onehot = jnp.where(jnp.broadcast_to(lrow, (256, KPAD)) == iota((256, KPAD), 0).astype(F32), 1.0, 0.0).astype(BF16)

    def spread(row_idx):
        return jnp.where(zmask, jnp.broadcast_to(atom_ref[row_idx:row_idx + 1, :], (16, KPAD)), 0.0).astype(BF16)

    def exchange(src, dst, ssem, rsem, arrays):
        starts, total = offsets_of(arrays)
        shift = 8 if arrays is pos_arrays else 0
        for delta in SEND_ORDER:
            rz, lanes = tile_of(delta)
            part = pl.ds(starts[delta], part_rows(arrays, delta))
            pltpu.make_async_remote_copy(src_ref=src.at[part], dst_ref=dst.at[pl.ds(starts[delta] + shift, part_rows(arrays, delta))], send_sem=ssem, recv_sem=rsem, device_id=partner(delta), device_id_type=MESH_ID).start()
        return pltpu.make_async_remote_copy(src_ref=src, dst_ref=dst.at[pl.ds(shift, total)], send_sem=ssem, recv_sem=rsem, device_id=partner(DELTAS[0]), device_id_type=MESH_ID)

    def keep_own(f, x):
        for h in range(2):
            g_ref[h, 24 * f + 4:24 * f + 20, :] = x[:, 128 * h:128 * h + 128]

    def fill(buf, fields, pack, arrays):
        starts, _ = offsets_of(arrays)
        for delta in DELTAS:
            rz, lanes = tile_of(delta)
            row = starts[delta]
            for arr in pack([to_delta(g_ref, f, delta) for f in fields], delta):
                for piece in arr:
                    if arrays is not pos_arrays:
                        buf[row:row + rz, :] = piece
                        row += rz
                    elif delta[0]:
                        buf[row:row + 3, :] = piece[0:3]
                        buf[row + 3:row + 6, :] = piece[5:8]
                        row += 6
                    else:
                        buf[row:row + 14, :] = piece[1:15]
                        row += 14

    def gather(fields, buf, arrays, unpack):
        starts, _ = offsets_of(arrays)
        parts = {}
        for delta in DELTAS:
            rz, lanes = tile_of(delta)
            row = starts[delta]
            arrs = []
            if arrays is pos_arrays:
                for i in range(3):
                    arrs.append([])
                    for j in range(lanes // 128):
                        if delta[0]:
                            row8 = iota((8, 128), 0)
                            arrs[i].append(jnp.where(row8 < 3, buf[row + 8:row + 16, :], jnp.where(row8 >= 5, buf[row + 6:row + 14, :], 0.0)))
                            row += 6
                        else:
                            row16 = iota((16, 128), 0)
                            arrs[i].append(jnp.where((row16 >= 1) & (row16 < 15), buf[row + 7:row + 23, :], 0.0))
                            row += 14
                parts[delta] = arrs
                continue
            for i in range(arrays(delta)):
                arrs.append([buf[row + rz * j:row + rz * j + rz, :] for j in range(lanes // 128)])
                row += rz * lanes // 128
            parts[delta] = unpack(arrs, delta)
        return [merge([g_ref[h, 24 * f + 4:24 * f + 20, :] for h in range(2)], {d: parts[d][i] for d in DELTAS}) for i, f in enumerate(fields)]

    lhs = jnp.concatenate([spread(8 * k + c) for k in range(3) for c in range(3)], axis=0)
    binned = dot_split(lhs, onehot, true)
    pos_own = [binned[16 * c:16 * c + 16] + binned[48 + 16 * c:64 + 16 * c] + binned[96 + 16 * c:112 + 16 * c] for c in range(3)]
    for c in range(3):
        keep_own(c, pos_own[c])
    fill(psend, range(3), same, pos_arrays)
    pl.semaphore_wait(barrier, 7)
    pos_all = exchange(psend, precv, psend_sem, precv_sem, pos_arrays)

    lhs = jnp.concatenate([spread(8 * k + c) for k in range(3, 6) for c in range(3)] + [spread(48), spread(49)], axis=0)
    binned = dot_split(lhs, onehot, true)
    vel_own = [binned[16 * c:16 * c + 16] + binned[48 + 16 * c:64 + 16 * c] + binned[96 + 16 * c:112 + 16 * c] for c in range(3)]
    vel_own.append(binned[144:160] * 128.0 + binned[160:176])
    for c in range(4):
        keep_own(3 + c, vel_own[c])
    fill(vsend, range(3, 7), pack_vel, vel_arrays)
    vel_all = exchange(vsend, vrecv, vsend_sem, vrecv_sem, vel_arrays)

    pos_all.wait_recv()
    fields = gather(range(3), precv, pos_arrays, same)

    present = fields[0] != 0.0
    lane = iota((16, 256), 1)
    frame = [lane & 15, lane >> 4, iota((16, 256), 0)]
    los = [bx, by, bz]
    local = []
    for c in range(3):
        u = fields[c] - los[c].astype(F32) * BRICK
        u = jnp.where(u < -0.5 * BRICK, u + BOX, jnp.where(u >= 1.5 * BRICK, u - BOX, u))
        local.append(jnp.where(present, u, 64.0 + 4.0 * frame[c].astype(F32)))

    def shift_in(s):
        dx, dy = SHIFTS[s]
        for h in range(2):
            left = 32 + 96 * h + 16 * dy + dx
            for c in range(3):
                rolled = pltpu.roll(local[c], (256 - left) % 256, 1)
                t_ref[3 * s + c, pl.ds(h, 16, stride=2), :] = rolled[:, 0:128]

    def keep(f, x):
        for h in range(2):
            rolled = pltpu.roll(x, (256 - 32 - 96 * h) % 256, 1)
            q_ref[f, pl.ds(h, 16, stride=2), :] = rolled[:, 0:128]

    def load(dx, dy, dz):
        s = SHIFTS.index((dx, dy))
        return [t_ref[3 * s + c, 4 + 2 * dz:28 + 2 * dz, :] for c in range(3)]

    low_x = (iota((24, 128), 1) & 15) < 8
    row24 = iota((24, 128), 0)
    low_y = (row24 & 1) == 0
    low_z = row24 < 12

    def pick(mask, p, q):
        return [jnp.where(mask, p[c], q[c]) for c in range(3)]

    def half(dx, dy, dz):
        return dy > 0 or (dy == 0 and (dx > 0 or (dx == 0 and dz > 0)))

    offsets = [(dx, dy, dz) for dx, dy in SHIFTS for dz in range(-2, 3) if (dx, dy, dz) != (0, 0, 0) and (abs(dx) == 2) + (abs(dy) == 2) + (abs(dz) == 2) <= 1]
    first = [functools.partial(load, *d) for d in offsets if half(*d)]
    second = [functools.partial(load, *d) for d in offsets if not half(*d)]
    for dz in range(-1, 2):
        first.append(lambda dz=dz: pick(low_x, load(-2, 2, dz), load(2, 2, dz)))
        second.append(lambda dz=dz: pick(low_x, load(-2, -2, dz), load(2, -2, dz)))
    for dx in range(-1, 2):
        first.append(lambda dx=dx: pick(low_z, load(dx, 2, -2), load(dx, 2, 2)))
        second.append(lambda dx=dx: pick(low_z, load(dx, -2, -2), load(dx, -2, 2)))
    for dy in (1, -1):
        (first if dy == 1 else second).append(lambda dy=dy: pick(low_z, pick(low_x, load(-2, dy, -2), load(2, dy, -2)), pick(low_x, load(-2, dy, 2), load(2, dy, 2))))
    first.append(lambda: pick(low_z, load(2, 0, -2), load(2, 0, 2)))
    second.append(lambda: pick(low_z, load(-2, 0, -2), load(-2, 0, 2)))

    for s, (dx, dy) in enumerate(SHIFTS):
        if dy > 0 or (dy == 0 and dx >= 0):
            shift_in(s)
    mine = load(0, 0, 0)

    def apart(nbr):
        ex, ey, ez = mine[0] - nbr[0], mine[1] - nbr[1], mine[2] - nbr[2]
        r2 = ex * ex + ey * ey + ez * ez
        r2 = jnp.minimum(r2, RCUT * RCUT)
        return ex, ey, ez, r2, lax.rsqrt(r2)

    sw, sr = jnp.zeros((24, 128), F32), jnp.zeros((24, 128), F32)
    for i, nbr in enumerate(first):
        ex, ey, ez, r2, inv = apart(nbr())
        i2 = inv * inv
        i6 = i2 * i2 * i2
        sw = sw + i6 * (i6 - 1.0)
        sr = sr + r2 * inv
        for k, x in enumerate((ex, ey, ez, inv)):
            p_ref[4 * i + k] = x
    keep(0, fields[0])
    lane24 = iota((24, 128), 1)
    x24 = lane24 & 15
    own = (lane24 < 96) & (x24 >= 2) & (x24 < 14) & (q_ref[0, 4:28, :] != 0.0)
    energy = 4.0 * sw - DU_CUT * sr + (RCUT * DU_CUT - U_CUT) * len(first)
    energy = jnp.where(own, energy, 0.0)
    me = bz * 4 + by * 2 + bx
    ebuf[me, :, :] = energy[0:8] + energy[8:16] + energy[16:24]
    for delta in SEND_ORDER:
        pltpu.make_async_remote_copy(src_ref=ebuf.at[me], dst_ref=ebuf.at[me], send_sem=esend_sem, recv_sem=erecv_sem, device_id=partner(delta), device_id_type=MESH_ID).start()
    energy_all = pltpu.make_async_remote_copy(src_ref=ebuf.at[pl.ds(0, 7)], dst_ref=ebuf.at[pl.ds(0, 7)], send_sem=esend_sem, recv_sem=erecv_sem, device_id=partner(DELTAS[0]), device_id_type=MESH_ID)

    vel_all.wait_recv()
    for f, x in enumerate(gather(range(3, 7), vrecv, vel_arrays, unpack_vel)):
        keep(3 + f, x)
    for c in range(1, 3):
        keep(c, fields[c])

    for s, (dx, dy) in enumerate(SHIFTS):
        if not (dy > 0 or (dy == 0 and dx >= 0)):
            shift_in(s)

    def push(acc, ex, ey, ez, inv):
        i2 = inv * inv
        i6 = i2 * i2 * i2
        fr = (i6 * (i6 - 0.5)) * i2 + (DU_CUT / 48.0) * inv
        return (acc[0] + fr * ex, acc[1] + fr * ey, acc[2] + fr * ez)

    acc = tuple(jnp.zeros((24, 128), F32) for _ in range(3))
    for i in range(len(first)):
        acc = push(acc, *(p_ref[4 * i + k] for k in range(4)))
    for nbr in second:
        ex, ey, ez, r2, inv = apart(nbr())
        acc = push(acc, ex, ey, ez, inv)
    force = [48.0 * acc[c] for c in range(3)]

    idv = jnp.where(own, q_ref[6, 4:28, :], -1.0)
    id_int = idv.astype(jnp.int32)
    id_hi = jnp.where(own, id_int >> 7, -1).astype(F32)
    id_lo = jnp.where(own, id_int & 127, -1).astype(F32)

    def flat(x, n):
        return jnp.concatenate([jnp.broadcast_to(x[r:r + 1, :], (n, 128)) for r in range(24)], axis=1)

    hot_hi = jnp.where(flat(id_hi, 128) == iota((128, 3072), 0).astype(F32), 1.0, 0.0).astype(BF16)
    lo_eq = flat(id_lo, 128) == iota((128, 3072), 0).astype(F32)
    hot_lo = jnp.where(lo_eq, 1.0, 0.0).astype(BF16)
    table = dot_split(hot_lo, hot_hi, true).astype(BF16)
    r128, c128 = iota((128, 128), 0), iota((128, 128), 1)
    below = dot_nn(jnp.where(c128 < r128, 1.0, 0.0).astype(BF16), table)
    total = dot_nn(jnp.ones((128, 128), BF16), table).astype(BF16)
    before = dot_nn(total, jnp.where(r128 < c128, 1.0, 0.0).astype(BF16))
    rank_tab = below + before
    tab_hi = jnp.floor(rank_tab * (1.0 / 256.0)) * 256.0
    tab_lo = rank_tab - tab_hi
    tabs = jnp.concatenate([tab_hi, tab_lo], axis=1).astype(BF16)
    hot2 = jnp.concatenate([hot_hi, hot_hi], axis=0)
    looked = jnp.concatenate([dot_nn(tabs, hot2[:, :1536]), dot_nn(tabs, hot2[:, 1536:])], axis=1)
    rank = jnp.sum(jnp.where(lo_eq, looked, 0.0), axis=0, keepdims=True)
    any_own = flat(jnp.where(own, 1.0, 0.0), 1) > 0.5
    rank_hi = jnp.floor(rank * (1.0 / 256.0))
    rank_lo = jnp.where(any_own, rank - 256.0 * rank_hi, -1.0)
    rank_hi = jnp.where(any_own, rank_hi, -1.0)

    hot_slot = jnp.where(jnp.broadcast_to(rank_lo, (256, 3072)) == iota((256, 3072), 0).astype(F32), 1.0, 0.0).astype(BF16)
    hi_mask = jnp.broadcast_to(rank_hi, (8, 3072)) == iota((8, 3072), 0).astype(F32)
    outs = []
    for c in range(3):
        outs += list(split3(q_ref[c, 4:28, :]))
    for c in range(3):
        outs += list(split3(q_ref[3 + c, 4:28, :] + (0.5 * TIME_STEP) * force[c]))
    for c in range(3):
        outs += list(split3(force[c]))
    outs += [id_hi, id_lo, jnp.where(own, 1.0, 0.0)]
    lhs = jnp.concatenate([jnp.where(hi_mask, flat(x, 8), 0.0) for x in outs], axis=0).astype(BF16)
    slots = dot_split(lhs, hot_slot, true)

    def field(i):
        return slots[8 * i:8 * i + 8, :]

    def put(ref, row, x):
        for h in range(7):
            n = 256 if h < 6 else CAP - 1536
            ref[row:row + 1, 256 * h:256 * h + n] = x[h:h + 1, 0:n].astype(ref.dtype)

    for c in range(3):
        put(opos_ref, c, field(3 * c) + field(3 * c + 1) + field(3 * c + 2))
        put(ovel_ref, c, field(9 + 3 * c) + field(10 + 3 * c) + field(11 + 3 * c))
        put(ofrc_ref, c, field(18 + 3 * c) + field(19 + 3 * c) + field(20 + 3 * c))
    put(oid_ref, 0, field(27) * 128.0 + field(28))
    put(oval_ref, 0, field(29))

    for copy in (pos_all, vel_all, energy_all):
        copy.wait_send()
    energy_all.wait_recv()
    acc = ebuf[0]
    for k in range(1, 8):
        acc = acc + ebuf[k]
    oen_ref[...] = jnp.sum(jnp.sum(acc, axis=0, keepdims=True), axis=1, keepdims=True)


def finish(pos_ref, vel_ref, frc_ref, id_ref, val_ref, en_ref, opos_ref, ovel_ref, ofrc_ref, oid_ref, oval_ref, oen_ref):
    opos_ref[...] = pos_ref[...]
    ovel_ref[...] = vel_ref[...]
    ofrc_ref[...] = frc_ref[...]
    oid_ref[...] = id_ref[...].reshape(CAP)
    oval_ref[...] = val_ref[...].reshape(CAP)
    oen_ref[...] = en_ref[...]


def solution(mesh):
    row_spec = P(BRICK_AXES, None)
    flat_spec = P(BRICK_AXES)
    vmem = pl.BlockSpec(memory_space=pltpu.VMEM)

    def local_step(pos, vel, frc, ids, valid):
        f3 = jax.ShapeDtypeStruct((3, CAP), F32)
        i1 = jax.ShapeDtypeStruct((CAP,), jnp.int32)
        outs = pl.pallas_call(
            kernel,
            out_shape=(pltpu.VMEM((3, CAP), F32),) * 3 + (pltpu.VMEM((1, CAP), jnp.int32),) * 2 + (pltpu.VMEM((1, 1), F32),),
            in_specs=[pl.BlockSpec(memory_space=pltpu.HBM)] * 5,
            out_specs=(vmem,) * 6,
            scratch_shapes=[pltpu.VMEM((offsets_of(pos_arrays)[1], 128), F32), pltpu.VMEM((offsets_of(pos_arrays)[1] + 16, 128), F32)] + [pltpu.VMEM((offsets_of(vel_arrays)[1], 128), F32)] * 2 + [
                pltpu.VMEM((3, CAP), F32),
                pltpu.VMEM((3, CAP), F32),
                pltpu.VMEM((3, CAP), F32),
                pltpu.VMEM((CAP,), jnp.int32),
                pltpu.VMEM((CAP,), jnp.int32),
                pltpu.SemaphoreType.DMA((5,)),
                pltpu.VMEM((56, KPAD), F32),
                pltpu.VMEM((2, 168, 128), F32),
                pltpu.VMEM((75, 32, 128), F32),
                pltpu.VMEM((NF, 32, 128), F32),
                pltpu.VMEM((192, 24, 128), F32),
                pltpu.VMEM((8, 8, 128), F32),
                pltpu.SemaphoreType.DMA,
                pltpu.SemaphoreType.DMA,
                pltpu.SemaphoreType.DMA,
                pltpu.SemaphoreType.DMA,
                pltpu.SemaphoreType.DMA,
                pltpu.SemaphoreType.DMA,
            ],
            compiler_params=pltpu.CompilerParams(collective_id=0, has_side_effects=True),
        )(pos.T, vel.T, frc.T, ids, valid)
        outs = pl.pallas_call(
            finish,
            out_shape=(f3, f3, f3, i1, i1, jax.ShapeDtypeStruct((1, 1), F32)),
            in_specs=[vmem] * 6,
            out_specs=(vmem,) * 6,
            compiler_params=pltpu.CompilerParams(vmem_limit_bytes=4 << 20),
        )(*outs)
        return outs[0].T, outs[1].T, outs[2].T, outs[3], outs[4], outs[5][0, 0]

    return jax.shard_map(local_step, mesh=mesh, in_specs=(row_spec, row_spec, row_spec, flat_spec, flat_spec), out_specs=(row_spec, row_spec, row_spec, flat_spec, flat_spec, P()), check_vma=False)
```

```python
import functools

import jax
import jax.numpy as jnp
from jax import lax
from jax.experimental import pallas as pl
from jax.experimental.pallas import tpu as pltpu
from jax.sharding import PartitionSpec as P

TIME_STEP = 0.005
RCUT = 2.5
DENSITY = 0.8442
SPACING = (1.0 / DENSITY) ** (1.0 / 3.0)
SITES = 12
BRICK = SITES * SPACING
BOX = 2.0 * BRICK
BRICK_AXES = ("bz", "by", "bx")
CAP = SITES ** 3
KPAD = 1792
MESH_ID = pl.DeviceIdType.MESH
F32 = jnp.float32
BF16 = jnp.bfloat16
CUT6 = RCUT ** -6
U_CUT = 4.0 * (CUT6 * CUT6 - CUT6)
DU_CUT = (-48.0 * CUT6 * CUT6 + 24.0 * CUT6) / RCUT
DELTAS = [(d >> 2 & 1, d >> 1 & 1, d & 1) for d in range(1, 8)]
SEND_ORDER = [(1, 1, 0), (1, 1, 1), (0, 1, 0), (1, 0, 0), (0, 1, 1), (1, 0, 1), (0, 0, 1)]
SHIFTS = [(dx, dy) for dy in range(-2, 3) for dx in range(-2, 3)]
NF = 7


def iota(shape, dim):
    return lax.broadcasted_iota(jnp.int32, shape, dim)


def split3(x):
    hi = x.astype(BF16).astype(F32)
    rest = x - hi
    mid = rest.astype(BF16).astype(F32)
    return hi, mid, rest - mid


def dot_nt(a, b):
    return lax.dot_general(a, b, (((1,), (1,)), ((), ())), preferred_element_type=F32)


def dot_split(a, b, true):
    cut = a.shape[1] // 512 * 256
    return dot_nt(a[:, :cut], b[:, :cut]) + jnp.where(true, dot_nt(a[:, cut:], b[:, cut:]), 0.0)


def dot_nn(a, b):
    return lax.dot_general(a, b, (((1,), (0,)), ((), ())), preferred_element_type=F32)


def tile_of(delta):
    return 8 if delta[0] else 16, 128 if delta[1] else 256


def pos_arrays(delta):
    return 3


def vel_arrays(delta):
    return 1 if delta[0] or delta[1] else 4


def offsets_of(arrays):
    starts, row = {}, 0
    for delta in DELTAS:
        starts[delta] = row
        row += part_rows(arrays, delta)
    return starts, row


def part_rows(arrays, delta):
    rz, lanes = tile_of(delta)
    if arrays is pos_arrays:
        rz = 6 if delta[0] else 14
    return arrays(delta) * rz * lanes // 128


def to_delta(g_ref, f, delta):
    dz, dy, dx = delta
    first = 24 * f + 4
    halves = []
    for h in range(2):
        if dz:
            halves.append(jnp.where(iota((8, 128), 0) < 4, g_ref[h, first + 12:first + 20, :], g_ref[h, first + 4:first + 12, :]))
        else:
            halves.append(g_ref[h, first:first + 16, :])
    lane = iota(halves[0].shape, 1)
    xf = lane & 15

    def along_x(x, turn):
        if not dx:
            return pltpu.roll(x, turn, 1) if turn else x
        return jnp.where(xf < 3, pltpu.roll(x, (turn + 116) % 128, 1), jnp.where(xf >= 13, pltpu.roll(x, turn + 12, 1), 0.0))

    if dy:
        group = lane >> 4
        return [jnp.where((group == 4) | (group == 5), along_x(halves[0], 64), jnp.where((group == 1) | (group == 2), 0.0, along_x(halves[1], 64)))]
    return [along_x(x, 0) for x in halves]


def wide(b):
    lane = iota(b.shape, 1)
    return [jnp.where(lane < 16, b, 0.0), jnp.where(lane >= 48, b, 0.0)]


def same(f, delta):
    return f


def pack_vel(f, delta):
    dz, dy, _ = delta
    if dz:
        row = iota(f[0][0].shape, 0)
        outs = []
        for j in range(len(f[0])):
            out = jnp.zeros_like(f[0][j])
            for k in range(4):
                out = jnp.where(row == 2 * k, jnp.broadcast_to(f[k][j][6:7], out.shape), out)
                out = jnp.where(row == 2 * k + 1, jnp.broadcast_to(f[k][j][1:2], out.shape), out)
            outs.append(out)
        return [outs]
    if dy:
        f = [x[0] for x in f]
        group = iota(f[0].shape, 1) >> 4
        out = jnp.where((group == 0) | (group == 3), f[0], 0.0)
        out = jnp.where((group == 1) | (group == 4), pltpu.roll(f[1], 16, 1), out)
        out = jnp.where((group == 2) | (group == 5), pltpu.roll(f[2], 32, 1), out)
        out = jnp.where(group == 6, pltpu.roll(f[3], 96, 1), out)
        return [[jnp.where(group == 7, pltpu.roll(f[3], 64, 1), out)]]
    return f


def unpack_vel(a, delta):
    dz, dy, _ = delta
    if dz:
        row = iota(a[0][0].shape, 0)
        return [[jnp.where(row == 6, jnp.broadcast_to(x[2 * k:2 * k + 1], x.shape), jnp.where(row == 1, jnp.broadcast_to(x[2 * k + 1:2 * k + 2], x.shape), 0.0)) for x in a[0]] for k in range(4)]
    if dy:
        x = a[0][0]
        group = iota(x.shape, 1) >> 4
        low, high = group == 0, group == 3
        both = low | high
        last = jnp.where(low, pltpu.roll(x, 32, 1), jnp.where(high, pltpu.roll(x, 64, 1), 0.0))
        return [[jnp.where(both, x, 0.0)], [jnp.where(both, pltpu.roll(x, 112, 1), 0.0)], [jnp.where(both, pltpu.roll(x, 96, 1), 0.0)], [last]]
    return a


def merge_level(own, parts):
    near = wide(parts[(0, 1, 0)][0] + parts[(0, 1, 1)][0])
    return [own[h] + parts[(0, 0, 1)][h] + near[h] for h in range(2)]


def merge_above(own, parts):
    far = wide(parts[(1, 1, 0)][0] + parts[(1, 1, 1)][0])
    return [own[h] + parts[(1, 0, 0)][h] + parts[(1, 0, 1)][h] + far[h] for h in range(2)]


def kernel(pos_hbm, vel_hbm, frc_hbm, id_hbm, val_hbm, opos_ref, ovel_ref, ofrc_ref, oid_ref, oval_ref, oen_ref, *scratch):
    psend, precv, vsend, vrecv, pos_ref, vel_ref, frc_ref, id_ref, val_ref, in_sem, atom_ref, g_ref, t_ref, q_ref, p_ref, ebuf, psend_sem, precv_sem, pabove_sem, vsend_sem, vrecv_sem, esend_sem, erecv_sem = scratch
    loads = [pltpu.make_async_copy(src, dst, in_sem.at[i]) for i, (src, dst) in enumerate(((vel_hbm, vel_ref), (frc_hbm, frc_ref), (pos_hbm, pos_ref), (val_hbm, val_ref), (id_hbm, id_ref)))]
    for copy in loads:
        copy.start()
    bz, by, bx = lax.axis_index("bz"), lax.axis_index("by"), lax.axis_index("bx")

    true = bz >= 0

    def partner(delta):
        return (lax.rem(bz + delta[0], 2), lax.rem(by + delta[1], 2), lax.rem(bx + delta[2], 2))

    barrier = pltpu.get_barrier_semaphore()
    for delta in DELTAS:
        pl.semaphore_signal(barrier, inc=1, device_id=partner(delta), device_id_type=MESH_ID)

    for f in range(NF):
        for h in range(2):
            g_ref[h, 24 * f:24 * f + 4, :] = jnp.zeros((4, 128), F32)
            g_ref[h, 24 * f + 20:24 * f + 24, :] = jnp.zeros((4, 128), F32)

    for copy in loads:
        copy.wait()
    v_half = vel_ref[...] + (0.5 * TIME_STEP) * frc_ref[...]
    moved = pos_ref[...] + TIME_STEP * v_half
    moved = moved - BOX * jnp.floor(moved * (1.0 / BOX))
    axis_row = iota((3, 1), 0)
    coord = jnp.where(axis_row == 0, bx, jnp.where(axis_row == 1, by, bz)).astype(F32)
    brick_lo = coord * BRICK
    rel = moved - brick_lo
    rel = jnp.where(rel < -0.5 * BRICK, rel + BOX, jnp.where(rel >= 1.5 * BRICK, rel - BOX, rel))
    cell = jnp.floor(rel * (1.0 / SPACING)).astype(jnp.int32) + 2
    live = val_ref[...].reshape(1, CAP) == 1
    ids = id_ref[...].reshape(1, CAP)
    atom_ref[:, pl.ds(KPAD - 128, 128)] = jnp.zeros((atom_ref.shape[0], 128), F32)
    zi = jnp.where(live, (cell[2:3, :] - 4) & 15, 0)
    lo = jnp.where(live, ((cell[1:2, :] - 2) & 15) * 16 + cell[0:1, :], 0)
    rows = list(split3(moved)) + list(split3(v_half))
    for k in range(6):
        atom_ref[8 * k:8 * k + 3, 0:CAP] = rows[k]
    atom_ref[48:49, 0:CAP] = (ids >> 7).astype(F32)
    atom_ref[49:50, 0:CAP] = (ids & 127).astype(F32)
    atom_ref[50:51, 0:CAP] = zi.astype(F32)
    atom_ref[51:52, 0:CAP] = lo.astype(F32)

    zrow = atom_ref[50:51, :]
    lrow = atom_ref[51:52, :]
    zmask = jnp.broadcast_to(zrow, (16, KPAD)) == iota((16, KPAD), 0).astype(F32)
    onehot = jnp.where(jnp.broadcast_to(lrow, (256, KPAD)) == iota((256, KPAD), 0).astype(F32), 1.0, 0.0).astype(BF16)

    def spread(row_idx):
        return jnp.where(zmask, jnp.broadcast_to(atom_ref[row_idx:row_idx + 1, :], (16, KPAD)), 0.0).astype(BF16)

    def exchange(src, dst, ssem, rsem, arrays):
        starts, total = offsets_of(arrays)
        shift = 8 if arrays is pos_arrays else 0
        cut = starts[(1, 0, 0)]
        for delta in SEND_ORDER:
            rz, lanes = tile_of(delta)
            part = pl.ds(starts[delta], part_rows(arrays, delta))
            pltpu.make_async_remote_copy(src_ref=src.at[part], dst_ref=dst.at[pl.ds(starts[delta] + shift, part_rows(arrays, delta))], send_sem=ssem, recv_sem=rsem[delta[0]], device_id=partner(delta), device_id_type=MESH_ID).start()
        return [pltpu.make_async_remote_copy(src_ref=src.at[pl.ds(lo, hi - lo)], dst_ref=dst.at[pl.ds(shift + lo, hi - lo)], send_sem=ssem, recv_sem=sem, device_id=partner(DELTAS[0]), device_id_type=MESH_ID) for lo, hi, sem in ((0, cut, rsem[0]), (cut, total, rsem[1]), (0, total, rsem[0]))]

    def keep_own(f, x):
        for h in range(2):
            g_ref[h, 24 * f + 4:24 * f + 20, :] = x[:, 128 * h:128 * h + 128]

    def fill(buf, fields, pack, arrays):
        starts, _ = offsets_of(arrays)
        for delta in DELTAS:
            rz, lanes = tile_of(delta)
            row = starts[delta]
            for arr in pack([to_delta(g_ref, f, delta) for f in fields], delta):
                for piece in arr:
                    if arrays is not pos_arrays:
                        buf[row:row + rz, :] = piece
                        row += rz
                    elif delta[0]:
                        buf[row:row + 6, :] = piece[1:7]
                        row += 6
                    else:
                        buf[row:row + 11, :] = piece[0:11]
                        buf[row + 11:row + 14, :] = piece[13:16]
                        row += 14

    def own_rows(f, start, count):
        return [g_ref[h, 24 * f + 4 + start:24 * f + 4 + start + count, :] for h in range(2)]

    def pos_parts(inner, deltas):
        starts, _ = offsets_of(pos_arrays)
        row8 = iota((8, 128), 0)
        parts = [{} for _ in range(3)]
        for delta in deltas:
            rows = 6 if delta[0] else 14
            row = starts[delta] + 8
            for c in range(3):
                parts[c][delta] = []
                for _ in range(tile_of(delta)[1] // 128):
                    if delta[0]:
                        x = jnp.where((row8 >= 1) & (row8 < 7), precv[row - 1:row + 7, :], 0.0)
                    elif inner:
                        x = precv[row:row + 8, :]
                    else:
                        x = jnp.where(row8 < 3, precv[row + 8:row + 16, :], jnp.where(row8 >= 5, precv[row + 6:row + 14, :], 0.0))
                    parts[c][delta].append(x)
                    row += rows
        return parts

    def vel_fields():
        starts, _ = offsets_of(vel_arrays)
        parts = {}
        for delta in DELTAS:
            rz, lanes = tile_of(delta)
            row = starts[delta]
            arrs = []
            for i in range(vel_arrays(delta)):
                arrs.append([vrecv[row + rz * j:row + rz * j + rz, :] for j in range(lanes // 128)])
                row += rz * lanes // 128
            parts[delta] = unpack_vel(arrs, delta)
        out = []
        for i in range(4):
            mine = {d: parts[d][i] for d in DELTAS}
            level = merge_level(own_rows(3 + i, 0, 16), mine)
            above = merge_above([x[8:16] for x in level], mine)
            out.append([[x[0:8] for x in level], above])
        return out

    lhs = jnp.concatenate([spread(8 * k + c) for k in range(3) for c in range(3)], axis=0)
    binned = dot_split(lhs, onehot, true)
    pos_own = [binned[16 * c:16 * c + 16] + binned[48 + 16 * c:64 + 16 * c] + binned[96 + 16 * c:112 + 16 * c] for c in range(3)]
    for c in range(3):
        keep_own(c, pos_own[c])
    fill(psend, range(3), same, pos_arrays)
    pl.semaphore_wait(barrier, 7)
    pos_all = exchange(psend, precv, psend_sem, (precv_sem, pabove_sem), pos_arrays)

    lhs = jnp.concatenate([spread(8 * k + c) for k in range(3, 6) for c in range(3)] + [spread(48), spread(49)], axis=0)
    binned = dot_split(lhs, onehot, true)
    vel_own = [binned[16 * c:16 * c + 16] + binned[48 + 16 * c:64 + 16 * c] + binned[96 + 16 * c:112 + 16 * c] for c in range(3)]
    vel_own.append(binned[144:160] * 128.0 + binned[160:176])
    for c in range(4):
        keep_own(3 + c, vel_own[c])
    fill(vsend, range(3, 7), pack_vel, vel_arrays)
    vel_all = exchange(vsend, vrecv, vsend_sem, (vrecv_sem, vrecv_sem), vel_arrays)

    los = [bx, by, bz]

    def localise(fields, start):
        out = [[], [], []]
        for h in range(2):
            present = fields[0][h] != 0.0
            lane = iota((8, 128), 1) + 128 * h
            frame = [lane & 15, lane >> 4, iota((8, 128), 0) + start]
            for c in range(3):
                u = fields[c][h] - los[c].astype(F32) * BRICK
                u = jnp.where(u < -0.5 * BRICK, u + BOX, jnp.where(u >= 1.5 * BRICK, u - BOX, u))
                out[c].append(jnp.where(present, u, 64.0 + 4.0 * frame[c].astype(F32)))
        return out

    lane8 = iota((8, 128), 1)

    def put_rows(ref, k, h, x, inner):
        if inner:
            ref[k, pl.ds(8 + h, 8, stride=2), :] = x
        else:
            ref[k, pl.ds(24 + h, 4, stride=2), :] = x[0:4]
            ref[k, pl.ds(h, 4, stride=2), :] = x[4:8]

    def shift_in(s, local, inner):
        dx, dy = SHIFTS[s]
        left = 16 * dy + dx
        for c in range(3):
            a, b = local[c]
            if left:
                a, b = pltpu.roll(a, (-left) % 128, 1), pltpu.roll(b, (-left) % 128, 1)
                here = lane8 < 128 - left if left > 0 else lane8 >= -left
                a, b = jnp.where(here, a, b), jnp.where(here, b, a)
            put_rows(t_ref, 3 * s + c, 0, a, inner)
            put_rows(t_ref, 3 * s + c, 1, b, inner)

    def keep(f, inner_rows, outer_rows):
        for h in range(2):
            put_rows(q_ref, f, h, inner_rows[h], True)
            put_rows(q_ref, f, h, outer_rows[h], False)

    span = [4, 24]

    def load(dx, dy, dz):
        s = SHIFTS.index((dx, dy))
        return [t_ref[3 * s + c, span[0] + 2 * dz:span[0] + 2 * dz + span[1], :] for c in range(3)]

    def low_x():
        return (iota((span[1], 128), 1) & 15) < 8

    def low_y():
        return ((iota((span[1], 128), 0) & 1) == 0) & (iota((span[1], 128), 1) < 96)

    def low_z():
        return iota((span[1], 128), 0) + span[0] < 16

    def pick(mask, p, q):
        m = mask()
        return [jnp.where(m, p[c], q[c]) for c in range(3)]

    def half(dx, dy, dz):
        return dy > 0 or (dy == 0 and (dx > 0 or (dx == 0 and dz > 0)))

    offsets = [(dx, dy, dz) for dx, dy in SHIFTS for dz in range(-2, 3) if (dx, dy, dz) != (0, 0, 0) and (abs(dx) == 2) + (abs(dy) == 2) + (abs(dz) == 2) <= 1]
    first = [functools.partial(load, *d) for d in offsets if half(*d)]
    second = [functools.partial(load, *d) for d in offsets if not half(*d)]
    for dz in range(-1, 2):
        first.append(lambda dz=dz: pick(low_x, load(-2, 2, dz), load(2, 2, dz)))
        second.append(lambda dz=dz: pick(low_x, load(-2, -2, dz), load(2, -2, dz)))
    for dx in range(-1, 2):
        first.append(lambda dx=dx: pick(low_z, load(dx, 2, -2), load(dx, 2, 2)))
        second.append(lambda dx=dx: pick(low_z, load(dx, -2, -2), load(dx, -2, 2)))
    for dy in (1, -1):
        (first if dy == 1 else second).append(lambda dy=dy: pick(low_z, pick(low_x, load(-2, dy, -2), load(2, dy, -2)), pick(low_x, load(-2, dy, 2), load(2, dy, 2))))
    first.append(lambda: pick(low_z, load(2, 0, -2), load(2, 0, 2)))
    second.append(lambda: pick(low_z, load(-2, 0, -2), load(-2, 0, 2)))

    def apart(mine, nbr):
        ex, ey, ez = mine[0] - nbr[0], mine[1] - nbr[1], mine[2] - nbr[2]
        r2 = jnp.minimum(ex * ex + ey * ey + ez * ez, RCUT * RCUT)
        return ex, ey, ez, r2, lax.rsqrt(r2)

    def pair_energy(row):
        span[:] = [row, 8]
        mine = load(0, 0, 0)
        sw, sr = jnp.zeros((8, 128), F32), jnp.zeros((8, 128), F32)
        for i, nbr in enumerate(first):
            ex, ey, ez, r2, inv = apart(mine, nbr())
            i2 = inv * inv
            i6 = i2 * i2 * i2
            sw = sw + i6 * (i6 - 1.0)
            sr = sr + r2 * inv
            for k, x in enumerate((ex, ey, ez, inv)):
                p_ref[4 * i + k, row - 4:row + 4, :] = x
        return 4.0 * sw - DU_CUT * sr + (RCUT * DU_CUT - U_CUT) * len(first)

    early = [s for s, (dx, dy) in enumerate(SHIFTS) if dy > 0 or (dy == 0 and dx >= 0)]
    late = [s for s in range(25) if s not in early]
    pos_all[0].wait_recv()
    parts = pos_parts(True, DELTAS[:3])
    inner = [merge_level(own_rows(c, 0, 8), parts[c]) for c in range(3)]
    inner_local = localise(inner, 0)
    for s in early:
        shift_in(s, inner_local, True)
    e_mid = pair_energy(12)
    pos_all[1].wait_recv()
    parts = pos_parts(False, DELTAS)
    outer = [merge_above(merge_level(own_rows(c, 8, 8), parts[c]), parts[c]) for c in range(3)]
    outer_local = localise(outer, 8)
    for s in early:
        shift_in(s, outer_local, False)
    e_low, e_high = pair_energy(4), pair_energy(20)
    span[:] = [4, 24]
    keep(0, inner[0], outer[0])
    lane24 = iota((24, 128), 1)
    x24 = lane24 & 15
    own = (((iota((24, 128), 0) & 1) == 0) | (lane24 < 64)) & (x24 >= 2) & (x24 < 14) & (q_ref[0, 4:28, :] != 0.0)
    energy = jnp.where(own, jnp.concatenate([e_low, e_mid, e_high], axis=0), 0.0)
    me = bz * 4 + by * 2 + bx
    ebuf[me, :, :] = energy[0:8] + energy[8:16] + energy[16:24]
    for delta in SEND_ORDER:
        pltpu.make_async_remote_copy(src_ref=ebuf.at[me], dst_ref=ebuf.at[me], send_sem=esend_sem, recv_sem=erecv_sem, device_id=partner(delta), device_id_type=MESH_ID).start()
    energy_all = pltpu.make_async_remote_copy(src_ref=ebuf.at[pl.ds(0, 7)], dst_ref=ebuf.at[pl.ds(0, 7)], send_sem=esend_sem, recv_sem=erecv_sem, device_id=partner(DELTAS[0]), device_id_type=MESH_ID)

    vel_all[2].wait_recv()
    for f, (a, b) in enumerate(vel_fields()):
        keep(3 + f, a, b)
    for c in range(1, 3):
        keep(c, inner[c], outer[c])

    for s in late:
        shift_in(s, inner_local, True)
        shift_in(s, outer_local, False)
    mine = load(0, 0, 0)

    def push(acc, ex, ey, ez, inv):
        i2 = inv * inv
        i6 = i2 * i2 * i2
        fr = (i6 * (i6 - 0.5)) * i2 + (DU_CUT / 48.0) * inv
        return (acc[0] + fr * ex, acc[1] + fr * ey, acc[2] + fr * ez)

    acc = tuple(jnp.zeros((24, 128), F32) for _ in range(3))
    for i in range(len(first)):
        acc = push(acc, *(p_ref[4 * i + k] for k in range(4)))
    for nbr in second:
        ex, ey, ez, r2, inv = apart(mine, nbr())
        acc = push(acc, ex, ey, ez, inv)
    force = [48.0 * acc[c] for c in range(3)]

    idv = jnp.where(own, q_ref[6, 4:28, :], -1.0)
    id_int = idv.astype(jnp.int32)
    id_hi = jnp.where(own, id_int >> 7, -1).astype(F32)
    id_lo = jnp.where(own, id_int & 127, -1).astype(F32)

    def flat(x, n):
        return jnp.concatenate([jnp.broadcast_to(x[r:r + 1, :], (n, 128)) for r in range(24)], axis=1)

    hot_hi = jnp.where(flat(id_hi, 128) == iota((128, 3072), 0).astype(F32), 1.0, 0.0).astype(BF16)
    lo_eq = flat(id_lo, 128) == iota((128, 3072), 0).astype(F32)
    hot_lo = jnp.where(lo_eq, 1.0, 0.0).astype(BF16)
    table = dot_split(hot_lo, hot_hi, true).astype(BF16)
    r128, c128 = iota((128, 128), 0), iota((128, 128), 1)
    below = dot_nn(jnp.where(c128 < r128, 1.0, 0.0).astype(BF16), table)
    total = dot_nn(jnp.ones((128, 128), BF16), table).astype(BF16)
    before = dot_nn(total, jnp.where(r128 < c128, 1.0, 0.0).astype(BF16))
    rank_tab = below + before
    tab_hi = jnp.floor(rank_tab * (1.0 / 256.0)) * 256.0
    tab_lo = rank_tab - tab_hi
    tabs = jnp.concatenate([tab_hi, tab_lo], axis=1).astype(BF16)
    hot2 = jnp.concatenate([hot_hi, hot_hi], axis=0)
    looked = jnp.concatenate([dot_nn(tabs, hot2[:, :1536]), dot_nn(tabs, hot2[:, 1536:])], axis=1)
    rank = jnp.sum(jnp.where(lo_eq, looked, 0.0), axis=0, keepdims=True)
    any_own = flat(jnp.where(own, 1.0, 0.0), 1) > 0.5
    rank_hi = jnp.floor(rank * (1.0 / 256.0))
    rank_lo = jnp.where(any_own, rank - 256.0 * rank_hi, -1.0)
    rank_hi = jnp.where(any_own, rank_hi, -1.0)

    hot_slot = jnp.where(jnp.broadcast_to(rank_lo, (256, 3072)) == iota((256, 3072), 0).astype(F32), 1.0, 0.0).astype(BF16)
    hi_mask = jnp.broadcast_to(rank_hi, (8, 3072)) == iota((8, 3072), 0).astype(F32)
    outs = []
    for c in range(3):
        outs += list(split3(q_ref[c, 4:28, :]))
    for c in range(3):
        outs += list(split3(q_ref[3 + c, 4:28, :] + (0.5 * TIME_STEP) * force[c]))
    for c in range(3):
        outs += list(split3(force[c]))
    outs += [id_hi, id_lo, jnp.where(own, 1.0, 0.0)]
    lhs = jnp.concatenate([jnp.where(hi_mask, flat(x, 8), 0.0) for x in outs], axis=0).astype(BF16)
    slots = dot_split(lhs, hot_slot, true)

    def field(i):
        return slots[8 * i:8 * i + 8, :]

    def put(ref, row, x):
        for h in range(7):
            n = 256 if h < 6 else CAP - 1536
            ref[row:row + 1, 256 * h:256 * h + n] = x[h:h + 1, 0:n].astype(ref.dtype)

    for c in range(3):
        put(opos_ref, c, field(3 * c) + field(3 * c + 1) + field(3 * c + 2))
        put(ovel_ref, c, field(9 + 3 * c) + field(10 + 3 * c) + field(11 + 3 * c))
        put(ofrc_ref, c, field(18 + 3 * c) + field(19 + 3 * c) + field(20 + 3 * c))
    put(oid_ref, 0, field(27) * 128.0 + field(28))
    put(oval_ref, 0, field(29))

    for copy in (pos_all[2], vel_all[2], energy_all):
        copy.wait_send()
    energy_all.wait_recv()
    acc = ebuf[0]
    for k in range(1, 8):
        acc = acc + ebuf[k]
    oen_ref[...] = jnp.sum(jnp.sum(acc, axis=0, keepdims=True), axis=1, keepdims=True)


def finish(pos_ref, vel_ref, frc_ref, id_ref, val_ref, en_ref, opos_ref, ovel_ref, ofrc_ref, oid_ref, oval_ref, oen_ref):
    opos_ref[...] = pos_ref[...]
    ovel_ref[...] = vel_ref[...]
    ofrc_ref[...] = frc_ref[...]
    oid_ref[...] = id_ref[...].reshape(CAP)
    oval_ref[...] = val_ref[...].reshape(CAP)
    oen_ref[...] = en_ref[...]


def solution(mesh):
    row_spec = P(BRICK_AXES, None)
    flat_spec = P(BRICK_AXES)
    vmem = pl.BlockSpec(memory_space=pltpu.VMEM)

    def local_step(pos, vel, frc, ids, valid):
        f3 = jax.ShapeDtypeStruct((3, CAP), F32)
        i1 = jax.ShapeDtypeStruct((CAP,), jnp.int32)
        outs = pl.pallas_call(
            kernel,
            out_shape=(pltpu.VMEM((3, CAP), F32),) * 3 + (pltpu.VMEM((1, CAP), jnp.int32),) * 2 + (pltpu.VMEM((1, 1), F32),),
            in_specs=[pl.BlockSpec(memory_space=pltpu.HBM)] * 5,
            out_specs=(vmem,) * 6,
            scratch_shapes=[pltpu.VMEM((offsets_of(pos_arrays)[1], 128), F32), pltpu.VMEM((offsets_of(pos_arrays)[1] + 16, 128), F32)] + [pltpu.VMEM((offsets_of(vel_arrays)[1], 128), F32)] * 2 + [
                pltpu.VMEM((3, CAP), F32),
                pltpu.VMEM((3, CAP), F32),
                pltpu.VMEM((3, CAP), F32),
                pltpu.VMEM((CAP,), jnp.int32),
                pltpu.VMEM((CAP,), jnp.int32),
                pltpu.SemaphoreType.DMA((5,)),
                pltpu.VMEM((56, KPAD), F32),
                pltpu.VMEM((2, 168, 128), F32),
                pltpu.VMEM((75, 32, 128), F32),
                pltpu.VMEM((NF, 32, 128), F32),
                pltpu.VMEM((192, 24, 128), F32),
                pltpu.VMEM((8, 8, 128), F32),
                pltpu.SemaphoreType.DMA,
                pltpu.SemaphoreType.DMA,
                pltpu.SemaphoreType.DMA,
                pltpu.SemaphoreType.DMA,
                pltpu.SemaphoreType.DMA,
                pltpu.SemaphoreType.DMA,
                pltpu.SemaphoreType.DMA,
            ],
            compiler_params=pltpu.CompilerParams(collective_id=0, has_side_effects=True),
        )(pos.T, vel.T, frc.T, ids, valid)
        outs = pl.pallas_call(
            finish,
            out_shape=(f3, f3, f3, i1, i1, jax.ShapeDtypeStruct((1, 1), F32)),
            in_specs=[vmem] * 6,
            out_specs=(vmem,) * 6,
            compiler_params=pltpu.CompilerParams(vmem_limit_bytes=4 << 20),
        )(*outs)
        return outs[0].T, outs[1].T, outs[2].T, outs[3], outs[4], outs[5][0, 0]

    return jax.shard_map(local_step, mesh=mesh, in_specs=(row_spec, row_spec, row_spec, flat_spec, flat_spec), out_specs=(row_spec, row_spec, row_spec, flat_spec, flat_spec, P()), check_vma=False)
```

```python
import functools

import jax
import jax.numpy as jnp
from jax import lax
from jax.experimental import pallas as pl
from jax.experimental.pallas import tpu as pltpu
from jax.sharding import PartitionSpec as P

TIME_STEP = 0.005
RCUT = 2.5
DENSITY = 0.8442
SPACING = (1.0 / DENSITY) ** (1.0 / 3.0)
SITES = 12
BRICK = SITES * SPACING
BOX = 2.0 * BRICK
BRICK_AXES = ("bz", "by", "bx")
CAP = SITES ** 3
KPAD = 1792
MESH_ID = pl.DeviceIdType.MESH
F32 = jnp.float32
BF16 = jnp.bfloat16
CUT6 = RCUT ** -6
U_CUT = 4.0 * (CUT6 * CUT6 - CUT6)
DU_CUT = (-48.0 * CUT6 * CUT6 + 24.0 * CUT6) / RCUT
DELTAS = [(d >> 2 & 1, d >> 1 & 1, d & 1) for d in range(1, 8)]
SEND_ORDER = [(1, 1, 0), (1, 1, 1), (0, 1, 0), (1, 0, 0), (0, 1, 1), (1, 0, 1), (0, 0, 1)]
SHIFTS = [(dx, dy) for dy in range(-2, 3) for dx in range(-2, 3)]
NF = 7


def iota(shape, dim):
    return lax.broadcasted_iota(jnp.int32, shape, dim)


def split3(x):
    hi = x.astype(BF16).astype(F32)
    rest = x - hi
    mid = rest.astype(BF16).astype(F32)
    return hi, mid, rest - mid


def dot_nt(a, b):
    return lax.dot_general(a, b, (((1,), (1,)), ((), ())), preferred_element_type=F32)


def dot_split(a, b, true):
    cut = a.shape[1] // 512 * 256
    return dot_nt(a[:, :cut], b[:, :cut]) + jnp.where(true, dot_nt(a[:, cut:], b[:, cut:]), 0.0)


def dot_nn(a, b):
    return lax.dot_general(a, b, (((1,), (0,)), ((), ())), preferred_element_type=F32)


def tile_of(delta):
    return 8 if delta[0] else 16, 128 if delta[1] else 256


def pos_arrays(delta):
    return 3


def vel_arrays(delta):
    return 1 if delta[0] or delta[1] else 4


def offsets_of(arrays):
    starts, row = {}, 0
    for delta in DELTAS:
        starts[delta] = row
        row += part_rows(arrays, delta)
    return starts, row


def part_rows(arrays, delta):
    rz, lanes = tile_of(delta)
    if arrays is pos_arrays:
        rz = 6 if delta[0] else 14
    return arrays(delta) * rz * lanes // 128


def to_delta(g_ref, f, delta):
    dz, dy, dx = delta
    first = 24 * f + 4
    halves = []
    for h in range(2):
        if dz:
            halves.append(jnp.where(iota((8, 128), 0) < 4, g_ref[h, first + 12:first + 20, :], g_ref[h, first + 4:first + 12, :]))
        else:
            halves.append(g_ref[h, first:first + 16, :])
    lane = iota(halves[0].shape, 1)
    xf = lane & 15

    def along_x(x, turn):
        if not dx:
            return pltpu.roll(x, turn, 1) if turn else x
        return jnp.where(xf < 3, pltpu.roll(x, (turn + 116) % 128, 1), jnp.where(xf >= 13, pltpu.roll(x, turn + 12, 1), 0.0))

    if dy:
        group = lane >> 4
        return [jnp.where((group == 4) | (group == 5), along_x(halves[0], 64), jnp.where((group == 1) | (group == 2), 0.0, along_x(halves[1], 64)))]
    return [along_x(x, 0) for x in halves]


def wide(b):
    lane = iota(b.shape, 1)
    return [jnp.where(lane < 16, b, 0.0), jnp.where(lane >= 48, b, 0.0)]


def same(f, delta):
    return f


def pack_vel(f, delta):
    dz, dy, _ = delta
    if dz:
        row = iota(f[0][0].shape, 0)
        outs = []
        for j in range(len(f[0])):
            out = jnp.zeros_like(f[0][j])
            for k in range(4):
                out = jnp.where(row == 2 * k, jnp.broadcast_to(f[k][j][6:7], out.shape), out)
                out = jnp.where(row == 2 * k + 1, jnp.broadcast_to(f[k][j][1:2], out.shape), out)
            outs.append(out)
        return [outs]
    if dy:
        f = [x[0] for x in f]
        group = iota(f[0].shape, 1) >> 4
        out = jnp.where((group == 0) | (group == 3), f[0], 0.0)
        out = jnp.where((group == 1) | (group == 4), pltpu.roll(f[1], 16, 1), out)
        out = jnp.where((group == 2) | (group == 5), pltpu.roll(f[2], 32, 1), out)
        out = jnp.where(group == 6, pltpu.roll(f[3], 96, 1), out)
        return [[jnp.where(group == 7, pltpu.roll(f[3], 64, 1), out)]]
    return f


def unpack_vel(a, delta):
    dz, dy, _ = delta
    if dz:
        row = iota(a[0][0].shape, 0)
        return [[jnp.where(row == 6, jnp.broadcast_to(x[2 * k:2 * k + 1], x.shape), jnp.where(row == 1, jnp.broadcast_to(x[2 * k + 1:2 * k + 2], x.shape), 0.0)) for x in a[0]] for k in range(4)]
    if dy:
        x = a[0][0]
        group = iota(x.shape, 1) >> 4
        low, high = group == 0, group == 3
        both = low | high
        last = jnp.where(low, pltpu.roll(x, 32, 1), jnp.where(high, pltpu.roll(x, 64, 1), 0.0))
        return [[jnp.where(both, x, 0.0)], [jnp.where(both, pltpu.roll(x, 112, 1), 0.0)], [jnp.where(both, pltpu.roll(x, 96, 1), 0.0)], [last]]
    return a


def merge_level(own, parts):
    near = wide(parts[(0, 1, 0)][0] + parts[(0, 1, 1)][0])
    return [own[h] + parts[(0, 0, 1)][h] + near[h] for h in range(2)]


def merge_above(own, parts):
    far = wide(parts[(1, 1, 0)][0] + parts[(1, 1, 1)][0])
    return [own[h] + parts[(1, 0, 0)][h] + parts[(1, 0, 1)][h] + far[h] for h in range(2)]


def kernel(pos_hbm, vel_hbm, frc_hbm, id_hbm, val_hbm, opos_ref, ovel_ref, ofrc_ref, oid_ref, oval_ref, oen_ref, *scratch):
    psend, precv, vsend, vrecv, pos_ref, vel_ref, frc_ref, id_ref, val_ref, in_sem, atom_ref, g_ref, t_ref, q_ref, p_ref, ebuf, psend_sem, precv_sem, pabove_sem, vsend_sem, vrecv_sem, esend_sem, erecv_sem = scratch
    loads = [pltpu.make_async_copy(src, dst, in_sem.at[i]) for i, (src, dst) in enumerate(((vel_hbm, vel_ref), (frc_hbm, frc_ref), (pos_hbm, pos_ref), (val_hbm, val_ref), (id_hbm, id_ref)))]
    for copy in loads:
        copy.start()
    bz, by, bx = lax.axis_index("bz"), lax.axis_index("by"), lax.axis_index("bx")

    true = bz >= 0

    def partner(delta):
        return (lax.rem(bz + delta[0], 2), lax.rem(by + delta[1], 2), lax.rem(bx + delta[2], 2))

    barrier = pltpu.get_barrier_semaphore()
    for delta in DELTAS:
        pl.semaphore_signal(barrier, inc=1, device_id=partner(delta), device_id_type=MESH_ID)

    for f in range(NF):
        for h in range(2):
            g_ref[h, 24 * f:24 * f + 4, :] = jnp.zeros((4, 128), F32)
            g_ref[h, 24 * f + 20:24 * f + 24, :] = jnp.zeros((4, 128), F32)

    for copy in loads:
        copy.wait()
    v_half = vel_ref[...] + (0.5 * TIME_STEP) * frc_ref[...]
    moved = pos_ref[...] + TIME_STEP * v_half
    moved = moved - BOX * jnp.floor(moved * (1.0 / BOX))
    axis_row = iota((3, 1), 0)
    coord = jnp.where(axis_row == 0, bx, jnp.where(axis_row == 1, by, bz)).astype(F32)
    brick_lo = coord * BRICK
    rel = moved - brick_lo
    rel = jnp.where(rel < -0.5 * BRICK, rel + BOX, jnp.where(rel >= 1.5 * BRICK, rel - BOX, rel))
    cell = jnp.floor(rel * (1.0 / SPACING)).astype(jnp.int32) + 2
    live = val_ref[...].reshape(1, CAP) == 1
    ids = id_ref[...].reshape(1, CAP)
    atom_ref[:, pl.ds(KPAD - 128, 128)] = jnp.zeros((atom_ref.shape[0], 128), F32)
    zi = jnp.where(live, (cell[2:3, :] - 4) & 15, 0)
    lo = jnp.where(live, ((cell[1:2, :] - 2) & 15) * 16 + cell[0:1, :], 0)
    rows = list(split3(moved)) + list(split3(v_half))
    for k in range(6):
        atom_ref[8 * k:8 * k + 3, 0:CAP] = rows[k]
    atom_ref[48:49, 0:CAP] = (ids >> 7).astype(F32)
    atom_ref[49:50, 0:CAP] = (ids & 127).astype(F32)
    atom_ref[50:51, 0:CAP] = zi.astype(F32)
    atom_ref[51:52, 0:CAP] = lo.astype(F32)

    zrow = atom_ref[50:51, :]
    lrow = atom_ref[51:52, :]
    zmask = jnp.broadcast_to(zrow, (16, KPAD)) == iota((16, KPAD), 0).astype(F32)
    onehot = jnp.where(jnp.broadcast_to(lrow, (256, KPAD)) == iota((256, KPAD), 0).astype(F32), 1.0, 0.0).astype(BF16)

    def spread(row_idx):
        return jnp.where(zmask, jnp.broadcast_to(atom_ref[row_idx:row_idx + 1, :], (16, KPAD)), 0.0).astype(BF16)

    def exchange(src, dst, ssem, rsem, arrays):
        starts, total = offsets_of(arrays)
        shift = 8 if arrays is pos_arrays else 0
        cut = starts[(1, 0, 0)]
        for delta in SEND_ORDER:
            rz, lanes = tile_of(delta)
            part = pl.ds(starts[delta], part_rows(arrays, delta))
            pltpu.make_async_remote_copy(src_ref=src.at[part], dst_ref=dst.at[pl.ds(starts[delta] + shift, part_rows(arrays, delta))], send_sem=ssem, recv_sem=rsem[delta[0]], device_id=partner(delta), device_id_type=MESH_ID).start()
        return [pltpu.make_async_remote_copy(src_ref=src.at[pl.ds(lo, hi - lo)], dst_ref=dst.at[pl.ds(shift + lo, hi - lo)], send_sem=ssem, recv_sem=sem, device_id=partner(DELTAS[0]), device_id_type=MESH_ID) for lo, hi, sem in ((0, cut, rsem[0]), (cut, total, rsem[1]), (0, total, rsem[0]))]

    def keep_own(f, x):
        for h in range(2):
            g_ref[h, 24 * f + 4:24 * f + 20, :] = x[:, 128 * h:128 * h + 128]

    def fill(buf, fields, pack, arrays):
        starts, _ = offsets_of(arrays)
        for delta in DELTAS:
            rz, lanes = tile_of(delta)
            row = starts[delta]
            for arr in pack([to_delta(g_ref, f, delta) for f in fields], delta):
                for piece in arr:
                    if arrays is not pos_arrays:
                        buf[row:row + rz, :] = piece
                        row += rz
                    elif delta[0]:
                        buf[row:row + 6, :] = piece[1:7]
                        row += 6
                    else:
                        buf[row:row + 11, :] = piece[0:11]
                        buf[row + 11:row + 14, :] = piece[13:16]
                        row += 14

    def own_rows(f, start, count):
        return [g_ref[h, 24 * f + 4 + start:24 * f + 4 + start + count, :] for h in range(2)]

    def pos_parts(inner, deltas):
        starts, _ = offsets_of(pos_arrays)
        row8 = iota((8, 128), 0)
        parts = [{} for _ in range(3)]
        for delta in deltas:
            rows = 6 if delta[0] else 14
            row = starts[delta] + 8
            for c in range(3):
                parts[c][delta] = []
                for _ in range(tile_of(delta)[1] // 128):
                    if delta[0]:
                        x = jnp.where((row8 >= 1) & (row8 < 7), precv[row - 1:row + 7, :], 0.0)
                    elif inner:
                        x = precv[row:row + 8, :]
                    else:
                        x = jnp.where(row8 < 3, precv[row + 8:row + 16, :], jnp.where(row8 >= 5, precv[row + 6:row + 14, :], 0.0))
                    parts[c][delta].append(x)
                    row += rows
        return parts

    def vel_fields():
        starts, _ = offsets_of(vel_arrays)
        parts = {}
        for delta in DELTAS:
            rz, lanes = tile_of(delta)
            row = starts[delta]
            arrs = []
            for i in range(vel_arrays(delta)):
                arrs.append([vrecv[row + rz * j:row + rz * j + rz, :] for j in range(lanes // 128)])
                row += rz * lanes // 128
            parts[delta] = unpack_vel(arrs, delta)
        out = []
        for i in range(4):
            mine = {d: parts[d][i] for d in DELTAS}
            level = merge_level(own_rows(3 + i, 0, 16), mine)
            above = merge_above([x[8:16] for x in level], mine)
            out.append([[x[0:8] for x in level], above])
        return out

    lhs = jnp.concatenate([spread(8 * k + c) for k in range(3) for c in range(3)], axis=0)
    binned = dot_split(lhs, onehot, true)
    pos_own = [binned[16 * c:16 * c + 16] + binned[48 + 16 * c:64 + 16 * c] + binned[96 + 16 * c:112 + 16 * c] for c in range(3)]
    for c in range(3):
        keep_own(c, pos_own[c])
    fill(psend, range(3), same, pos_arrays)
    pl.semaphore_wait(barrier, 7)
    pos_all = exchange(psend, precv, psend_sem, (precv_sem, pabove_sem), pos_arrays)

    lhs = jnp.concatenate([spread(8 * k + c) for k in range(3, 6) for c in range(3)] + [spread(48), spread(49)], axis=0)
    binned = dot_split(lhs, onehot, true)
    vel_own = [binned[16 * c:16 * c + 16] + binned[48 + 16 * c:64 + 16 * c] + binned[96 + 16 * c:112 + 16 * c] for c in range(3)]
    vel_own.append(binned[144:160] * 128.0 + binned[160:176])
    for c in range(4):
        keep_own(3 + c, vel_own[c])
    fill(vsend, range(3, 7), pack_vel, vel_arrays)
    vel_all = exchange(vsend, vrecv, vsend_sem, (vrecv_sem, vrecv_sem), vel_arrays)

    los = [bx, by, bz]

    def localise(fields, start):
        out = [[], [], []]
        for h in range(2):
            present = fields[0][h] != 0.0
            lane = iota((8, 128), 1) + 128 * h
            frame = [lane & 15, lane >> 4, iota((8, 128), 0) + start]
            for c in range(3):
                u = fields[c][h] - los[c].astype(F32) * BRICK
                u = jnp.where(u < -0.5 * BRICK, u + BOX, jnp.where(u >= 1.5 * BRICK, u - BOX, u))
                out[c].append(jnp.where(present, u, 64.0 + 4.0 * frame[c].astype(F32)))
        return out

    lane8 = iota((8, 128), 1)

    def put_rows(ref, k, h, x, inner):
        if inner:
            ref[k, pl.ds(8 + h, 8, stride=2), :] = x
        else:
            ref[k, pl.ds(24 + h, 4, stride=2), :] = x[0:4]
            ref[k, pl.ds(h, 4, stride=2), :] = x[4:8]

    def shift_in(s, local, inner):
        dx, dy = SHIFTS[s]
        left = 16 * dy + dx
        for c in range(3):
            a, b = local[c]
            if left:
                a, b = pltpu.roll(a, (-left) % 128, 1), pltpu.roll(b, (-left) % 128, 1)
                here = lane8 < 128 - left if left > 0 else lane8 >= -left
                a, b = jnp.where(here, a, b), jnp.where(here, b, a)
            put_rows(t_ref, 3 * s + c, 0, a, inner)
            put_rows(t_ref, 3 * s + c, 1, b, inner)

    def keep(f, inner_rows, outer_rows):
        for h in range(2):
            put_rows(q_ref, f, h, inner_rows[h], True)
            put_rows(q_ref, f, h, outer_rows[h], False)

    span = [4, 24]

    def load(dx, dy, dz):
        s = SHIFTS.index((dx, dy))
        return [t_ref[3 * s + c, span[0] + 2 * dz:span[0] + 2 * dz + span[1], :] for c in range(3)]

    def low_x():
        return (iota((span[1], 128), 1) & 15) < 8

    def low_y():
        return ((iota((span[1], 128), 0) & 1) == 0) & (iota((span[1], 128), 1) < 96)

    def low_z():
        return iota((span[1], 128), 0) + span[0] < 16

    def pick(mask, p, q):
        m = mask()
        return [jnp.where(m, p[c], q[c]) for c in range(3)]

    def half(dx, dy, dz):
        return dy > 0 or (dy == 0 and (dx > 0 or (dx == 0 and dz > 0)))

    offsets = [(dx, dy, dz) for dx, dy in SHIFTS for dz in range(-2, 3) if (dx, dy, dz) != (0, 0, 0) and (abs(dx) == 2) + (abs(dy) == 2) + (abs(dz) == 2) <= 1]
    first = [functools.partial(load, *d) for d in offsets if half(*d)]
    second = [functools.partial(load, *d) for d in offsets if not half(*d)]
    for dz in range(-1, 2):
        first.append(lambda dz=dz: pick(low_x, load(-2, 2, dz), load(2, 2, dz)))
        second.append(lambda dz=dz: pick(low_x, load(-2, -2, dz), load(2, -2, dz)))
    for dx in range(-1, 2):
        first.append(lambda dx=dx: pick(low_z, load(dx, 2, -2), load(dx, 2, 2)))
        second.append(lambda dx=dx: pick(low_z, load(dx, -2, -2), load(dx, -2, 2)))
    for dy in (1, -1):
        (first if dy == 1 else second).append(lambda dy=dy: pick(low_z, pick(low_x, load(-2, dy, -2), load(2, dy, -2)), pick(low_x, load(-2, dy, 2), load(2, dy, 2))))
    first.append(lambda: pick(low_z, load(2, 0, -2), load(2, 0, 2)))
    second.append(lambda: pick(low_z, load(-2, 0, -2), load(-2, 0, 2)))

    def apart(mine, nbr):
        ex, ey, ez = mine[0] - nbr[0], mine[1] - nbr[1], mine[2] - nbr[2]
        r2 = jnp.minimum(ex * ex + ey * ey + ez * ez, RCUT * RCUT)
        return ex, ey, ez, r2, lax.rsqrt(r2)

    def pair_energy(row):
        span[:] = [row, 8]
        mine = load(0, 0, 0)
        sw, sr = jnp.zeros((8, 128), F32), jnp.zeros((8, 128), F32)
        for i, nbr in enumerate(first):
            ex, ey, ez, r2, inv = apart(mine, nbr())
            i2 = inv * inv
            i6 = i2 * i2 * i2
            sw = sw + i6 * (i6 - 1.0)
            sr = sr + r2 * inv
            for k, x in enumerate((ex, ey, ez, inv)):
                p_ref[4 * i + k, row - 4:row + 4, :] = x
        return 4.0 * sw - DU_CUT * sr + (RCUT * DU_CUT - U_CUT) * len(first)

    early = [s for s, (dx, dy) in enumerate(SHIFTS) if dy > 0 or (dy == 0 and dx >= 0)]
    late = [s for s in range(25) if s not in early]
    pos_all[0].wait_recv()
    parts = pos_parts(True, DELTAS[:3])
    inner = [merge_level(own_rows(c, 0, 8), parts[c]) for c in range(3)]
    inner_local = localise(inner, 0)
    for s in early:
        shift_in(s, inner_local, True)
    e_mid = pair_energy(12)
    pos_all[1].wait_recv()
    parts = pos_parts(False, DELTAS)
    outer = [merge_above(merge_level(own_rows(c, 8, 8), parts[c]), parts[c]) for c in range(3)]
    outer_local = localise(outer, 8)
    for s in early:
        shift_in(s, outer_local, False)
    e_low, e_high = pair_energy(4), pair_energy(20)
    span[:] = [4, 24]
    keep(0, inner[0], outer[0])
    lane24 = iota((24, 128), 1)
    x24 = lane24 & 15
    own = (((iota((24, 128), 0) & 1) == 0) | (lane24 < 64)) & (x24 >= 2) & (x24 < 14) & (q_ref[0, 4:28, :] != 0.0)
    energy = jnp.where(own, jnp.concatenate([e_low, e_mid, e_high], axis=0), 0.0)
    me = bz * 4 + by * 2 + bx
    ebuf[me, :, :] = energy[0:8] + energy[8:16] + energy[16:24]
    for delta in SEND_ORDER:
        pltpu.make_async_remote_copy(src_ref=ebuf.at[me], dst_ref=ebuf.at[me], send_sem=esend_sem, recv_sem=erecv_sem, device_id=partner(delta), device_id_type=MESH_ID).start()
    energy_all = pltpu.make_async_remote_copy(src_ref=ebuf.at[pl.ds(0, 7)], dst_ref=ebuf.at[pl.ds(0, 7)], send_sem=esend_sem, recv_sem=erecv_sem, device_id=partner(DELTAS[0]), device_id_type=MESH_ID)

    vel_all[2].wait_recv()
    for f, (a, b) in enumerate(vel_fields()):
        keep(3 + f, a, b)
    for c in range(1, 3):
        keep(c, inner[c], outer[c])

    for s in late:
        shift_in(s, inner_local, True)
        shift_in(s, outer_local, False)
    mine = load(0, 0, 0)

    def push(acc, ex, ey, ez, inv):
        i2 = inv * inv
        i6 = i2 * i2 * i2
        fr = (i6 * (i6 - 0.5)) * i2 + (DU_CUT / 48.0) * inv
        return (acc[0] + fr * ex, acc[1] + fr * ey, acc[2] + fr * ez)

    acc = tuple(jnp.zeros((24, 128), F32) for _ in range(3))
    for i in range(len(first)):
        acc = push(acc, *(p_ref[4 * i + k] for k in range(4)))
    for nbr in second:
        ex, ey, ez, r2, inv = apart(mine, nbr())
        acc = push(acc, ex, ey, ez, inv)
    force = [48.0 * acc[c] for c in range(3)]

    idv = jnp.where(own, q_ref[6, 4:28, :], -1.0)
    id_int = idv.astype(jnp.int32)
    id_hi = jnp.where(own, id_int >> 7, -1).astype(F32)
    id_lo = jnp.where(own, id_int & 127, -1).astype(F32)

    def flat(x, n):
        return jnp.concatenate([jnp.broadcast_to(x[r:r + 1, :], (n, 128)) for r in range(24)], axis=1)

    hot_hi = jnp.where(flat(id_hi, 128) == iota((128, 3072), 0).astype(F32), 1.0, 0.0).astype(BF16)
    lo_eq = flat(id_lo, 128) == iota((128, 3072), 0).astype(F32)
    hot_lo = jnp.where(lo_eq, 1.0, 0.0).astype(BF16)
    table = dot_split(hot_lo, hot_hi, true).astype(BF16)
    r128, c128 = iota((128, 128), 0), iota((128, 128), 1)
    below = dot_nn(jnp.where(c128 < r128, 1.0, 0.0).astype(BF16), table)
    total = dot_nn(jnp.ones((128, 128), BF16), table).astype(BF16)
    before = dot_nn(total, jnp.where(r128 < c128, 1.0, 0.0).astype(BF16))
    rank_tab = below + before
    tab_hi = jnp.floor(rank_tab * (1.0 / 256.0)) * 256.0
    tab_lo = rank_tab - tab_hi
    tabs = jnp.concatenate([tab_hi, tab_lo], axis=1).astype(BF16)
    hot2 = jnp.concatenate([hot_hi, hot_hi], axis=0)
    looked = jnp.concatenate([dot_nn(tabs, hot2[:, :1536]), dot_nn(tabs, hot2[:, 1536:])], axis=1)
    rank = jnp.sum(jnp.where(lo_eq, looked, 0.0), axis=0, keepdims=True)
    any_own = flat(jnp.where(own, 1.0, 0.0), 1) > 0.5
    rank_hi = jnp.floor(rank * (1.0 / 256.0))
    rank_lo = jnp.where(any_own, rank - 256.0 * rank_hi, -1.0)
    rank_hi = jnp.where(any_own, rank_hi, -1.0)

    hot_slot = jnp.where(jnp.broadcast_to(rank_lo, (256, 3072)) == iota((256, 3072), 0).astype(F32), 1.0, 0.0).astype(BF16)
    hi_mask = jnp.broadcast_to(rank_hi, (8, 3072)) == iota((8, 3072), 0).astype(F32)
    outs = []
    for c in range(3):
        outs += list(split3(q_ref[c, 4:28, :]))
    for c in range(3):
        outs += list(split3(q_ref[3 + c, 4:28, :] + (0.5 * TIME_STEP) * force[c]))
    for c in range(3):
        outs += list(split3(force[c]))
    outs += [id_hi, id_lo, jnp.where(own, 1.0, 0.0)]
    lhs = jnp.concatenate([jnp.where(hi_mask, flat(x, 8), 0.0) for x in outs], axis=0).astype(BF16)
    slots = dot_split(lhs, hot_slot, true)

    def field(i):
        return slots[8 * i:8 * i + 8, :]

    def put(ref, row, x):
        for h in range(7):
            n = 256 if h < 6 else CAP - 1536
            ref[row:row + 1, 256 * h:256 * h + n] = x[h:h + 1, 0:n].astype(ref.dtype)

    for c in range(3):
        put(opos_ref, c, field(3 * c) + field(3 * c + 1) + field(3 * c + 2))
        put(ovel_ref, c, field(9 + 3 * c) + field(10 + 3 * c) + field(11 + 3 * c))
        put(ofrc_ref, c, field(18 + 3 * c) + field(19 + 3 * c) + field(20 + 3 * c))
    put(oid_ref, 0, field(27) * 128.0 + field(28))
    put(oval_ref, 0, field(29))

    for copy in (pos_all[2], vel_all[2], energy_all):
        copy.wait_send()
    energy_all.wait_recv()
    acc = ebuf[0]
    for k in range(1, 8):
        acc = acc + ebuf[k]
    oen_ref[...] = acc


def finish(pos_ref, vel_ref, frc_ref, id_ref, val_ref, en_ref, opos_ref, ovel_ref, ofrc_ref, oid_ref, oval_ref, oen_ref):
    opos_ref[...] = pos_ref[...]
    ovel_ref[...] = vel_ref[...]
    ofrc_ref[...] = frc_ref[...]
    oid_ref[...] = id_ref[...].reshape(CAP)
    oval_ref[...] = val_ref[...].reshape(CAP)
    oen_ref[...] = jnp.sum(jnp.sum(en_ref[...], axis=0, keepdims=True), axis=1, keepdims=True)


def solution(mesh):
    row_spec = P(BRICK_AXES, None)
    flat_spec = P(BRICK_AXES)
    vmem = pl.BlockSpec(memory_space=pltpu.VMEM)

    def local_step(pos, vel, frc, ids, valid):
        f3 = jax.ShapeDtypeStruct((3, CAP), F32)
        i1 = jax.ShapeDtypeStruct((CAP,), jnp.int32)
        outs = pl.pallas_call(
            kernel,
            out_shape=(pltpu.VMEM((3, CAP), F32),) * 3 + (pltpu.VMEM((1, CAP), jnp.int32),) * 2 + (pltpu.VMEM((8, 128), F32),),
            in_specs=[pl.BlockSpec(memory_space=pltpu.HBM)] * 5,
            out_specs=(vmem,) * 6,
            scratch_shapes=[pltpu.VMEM((offsets_of(pos_arrays)[1], 128), F32), pltpu.VMEM((offsets_of(pos_arrays)[1] + 16, 128), F32)] + [pltpu.VMEM((offsets_of(vel_arrays)[1], 128), F32)] * 2 + [
                pltpu.VMEM((3, CAP), F32),
                pltpu.VMEM((3, CAP), F32),
                pltpu.VMEM((3, CAP), F32),
                pltpu.VMEM((CAP,), jnp.int32),
                pltpu.VMEM((CAP,), jnp.int32),
                pltpu.SemaphoreType.DMA((5,)),
                pltpu.VMEM((56, KPAD), F32),
                pltpu.VMEM((2, 168, 128), F32),
                pltpu.VMEM((75, 32, 128), F32),
                pltpu.VMEM((NF, 32, 128), F32),
                pltpu.VMEM((192, 24, 128), F32),
                pltpu.VMEM((8, 8, 128), F32),
                pltpu.SemaphoreType.DMA,
                pltpu.SemaphoreType.DMA,
                pltpu.SemaphoreType.DMA,
                pltpu.SemaphoreType.DMA,
                pltpu.SemaphoreType.DMA,
                pltpu.SemaphoreType.DMA,
                pltpu.SemaphoreType.DMA,
            ],
            compiler_params=pltpu.CompilerParams(collective_id=0, has_side_effects=True),
        )(pos.T, vel.T, frc.T, ids, valid)
        outs = pl.pallas_call(
            finish,
            out_shape=(f3, f3, f3, i1, i1, jax.ShapeDtypeStruct((1, 1), F32)),
            in_specs=[vmem] * 6,
            out_specs=(vmem,) * 6,
            compiler_params=pltpu.CompilerParams(vmem_limit_bytes=4 << 20),
        )(*outs)
        return outs[0].T, outs[1].T, outs[2].T, outs[3], outs[4], outs[5][0, 0]

    return jax.shard_map(local_step, mesh=mesh, in_specs=(row_spec, row_spec, row_spec, flat_spec, flat_spec), out_specs=(row_spec, row_spec, row_spec, flat_spec, flat_spec, P()), check_vma=False)
```

```python
import functools

import jax
import jax.numpy as jnp
from jax import lax
from jax.experimental import pallas as pl
from jax.experimental.pallas import tpu as pltpu
from jax.sharding import PartitionSpec as P

TIME_STEP = 0.005
RCUT = 2.5
DENSITY = 0.8442
SPACING = (1.0 / DENSITY) ** (1.0 / 3.0)
SITES = 12
BRICK = SITES * SPACING
BOX = 2.0 * BRICK
BRICK_AXES = ("bz", "by", "bx")
CAP = SITES ** 3
KPAD = 1792
MESH_ID = pl.DeviceIdType.MESH
F32 = jnp.float32
BF16 = jnp.bfloat16
CUT6 = RCUT ** -6
U_CUT = 4.0 * (CUT6 * CUT6 - CUT6)
DU_CUT = (-48.0 * CUT6 * CUT6 + 24.0 * CUT6) / RCUT
DELTAS = [(d >> 2 & 1, d >> 1 & 1, d & 1) for d in range(1, 8)]
SEND_ORDER = [(1, 1, 0), (1, 1, 1), (0, 1, 0), (1, 0, 0), (0, 1, 1), (1, 0, 1), (0, 0, 1)]
POS_ORDER = [(1, 1, 0), (0, 1, 0), (1, 1, 1), (0, 1, 1), (1, 0, 0), (1, 0, 1), (0, 0, 1)]
SHIFTS = [(dx, dy) for dy in range(-2, 3) for dx in range(-2, 3)]
NF = 7


def iota(shape, dim):
    return lax.broadcasted_iota(jnp.int32, shape, dim)


def split3(x):
    hi = x.astype(BF16).astype(F32)
    rest = x - hi
    mid = rest.astype(BF16).astype(F32)
    return hi, mid, rest - mid


def dot_nt(a, b):
    return lax.dot_general(a, b, (((1,), (1,)), ((), ())), preferred_element_type=F32)


def dot_split(a, b, true):
    cut = a.shape[1] // 512 * 256
    return dot_nt(a[:, :cut], b[:, :cut]) + jnp.where(true, dot_nt(a[:, cut:], b[:, cut:]), 0.0)


def dot_nn(a, b):
    return lax.dot_general(a, b, (((1,), (0,)), ((), ())), preferred_element_type=F32)


def tile_of(delta):
    return 8 if delta[0] else 16, 128 if delta[1] else 256


def pos_arrays(delta):
    return 3


def vel_arrays(delta):
    return 1 if delta[0] or delta[1] else 4


def offsets_of(arrays):
    starts, row = {}, 0
    for delta in DELTAS:
        starts[delta] = row
        row += part_rows(arrays, delta)
    return starts, row


def part_rows(arrays, delta):
    rz, lanes = tile_of(delta)
    if arrays is pos_arrays:
        rz = 6 if delta[0] else 14
    return arrays(delta) * rz * lanes // 128


def to_delta(g_ref, f, delta):
    dz, dy, dx = delta
    first = 24 * f + 4
    halves = []
    for h in range(2):
        if dz:
            halves.append(jnp.where(iota((8, 128), 0) < 4, g_ref[h, first + 12:first + 20, :], g_ref[h, first + 4:first + 12, :]))
        else:
            halves.append(g_ref[h, first:first + 16, :])
    lane = iota(halves[0].shape, 1)
    xf = lane & 15

    def along_x(x, turn):
        if not dx:
            return pltpu.roll(x, turn, 1) if turn else x
        return jnp.where(xf < 3, pltpu.roll(x, (turn + 116) % 128, 1), jnp.where(xf >= 13, pltpu.roll(x, turn + 12, 1), 0.0))

    if dy:
        group = lane >> 4
        return [jnp.where((group == 4) | (group == 5), along_x(halves[0], 64), jnp.where((group == 1) | (group == 2), 0.0, along_x(halves[1], 64)))]
    return [along_x(x, 0) for x in halves]


def wide(b):
    lane = iota(b.shape, 1)
    return [jnp.where(lane < 16, b, 0.0), jnp.where(lane >= 48, b, 0.0)]


def same(f, delta):
    return f


def pack_vel(f, delta):
    dz, dy, _ = delta
    if dz:
        row = iota(f[0][0].shape, 0)
        outs = []
        for j in range(len(f[0])):
            out = jnp.zeros_like(f[0][j])
            for k in range(4):
                out = jnp.where(row == 2 * k, jnp.broadcast_to(f[k][j][6:7], out.shape), out)
                out = jnp.where(row == 2 * k + 1, jnp.broadcast_to(f[k][j][1:2], out.shape), out)
            outs.append(out)
        return [outs]
    if dy:
        f = [x[0] for x in f]
        group = iota(f[0].shape, 1) >> 4
        out = jnp.where((group == 0) | (group == 3), f[0], 0.0)
        out = jnp.where((group == 1) | (group == 4), pltpu.roll(f[1], 16, 1), out)
        out = jnp.where((group == 2) | (group == 5), pltpu.roll(f[2], 32, 1), out)
        out = jnp.where(group == 6, pltpu.roll(f[3], 96, 1), out)
        return [[jnp.where(group == 7, pltpu.roll(f[3], 64, 1), out)]]
    return f


def unpack_vel(a, delta):
    dz, dy, _ = delta
    if dz:
        row = iota(a[0][0].shape, 0)
        return [[jnp.where(row == 6, jnp.broadcast_to(x[2 * k:2 * k + 1], x.shape), jnp.where(row == 1, jnp.broadcast_to(x[2 * k + 1:2 * k + 2], x.shape), 0.0)) for x in a[0]] for k in range(4)]
    if dy:
        x = a[0][0]
        group = iota(x.shape, 1) >> 4
        low, high = group == 0, group == 3
        both = low | high
        last = jnp.where(low, pltpu.roll(x, 32, 1), jnp.where(high, pltpu.roll(x, 64, 1), 0.0))
        return [[jnp.where(both, x, 0.0)], [jnp.where(both, pltpu.roll(x, 112, 1), 0.0)], [jnp.where(both, pltpu.roll(x, 96, 1), 0.0)], [last]]
    return a


def merge_level(own, parts):
    near = wide(parts[(0, 1, 0)][0] + parts[(0, 1, 1)][0])
    return [own[h] + parts[(0, 0, 1)][h] + near[h] for h in range(2)]


def merge_above(own, parts):
    far = wide(parts[(1, 1, 0)][0] + parts[(1, 1, 1)][0])
    return [own[h] + parts[(1, 0, 0)][h] + parts[(1, 0, 1)][h] + far[h] for h in range(2)]


def kernel(pos_hbm, vel_hbm, frc_hbm, id_hbm, val_hbm, opos_ref, ovel_ref, ofrc_ref, oid_ref, oval_ref, oen_ref, *scratch):
    psend, precv, vsend, vrecv, pos_ref, vel_ref, frc_ref, id_ref, val_ref, in_sem, atom_ref, g_ref, t_ref, q_ref, p_ref, ebuf, psend_sem, precv_sem, pabove_sem, vsend_sem, vrecv_sem, esend_sem, erecv_sem = scratch
    bz, by, bx = lax.axis_index("bz"), lax.axis_index("by"), lax.axis_index("bx")

    true = bz >= 0

    def partner(delta):
        return (lax.rem(bz + delta[0], 2), lax.rem(by + delta[1], 2), lax.rem(bx + delta[2], 2))

    barrier = pltpu.get_barrier_semaphore()
    for delta in SEND_ORDER:
        pl.semaphore_signal(barrier, inc=1, device_id=partner(delta), device_id_type=MESH_ID)

    loads = [pltpu.make_async_copy(src, dst, in_sem.at[i]) for i, (src, dst) in enumerate(((vel_hbm, vel_ref), (frc_hbm, frc_ref), (pos_hbm, pos_ref), (val_hbm, val_ref), (id_hbm, id_ref)))]
    for copy in loads:
        copy.start()
    for f in range(NF):
        for h in range(2):
            g_ref[h, 24 * f:24 * f + 4, :] = jnp.zeros((4, 128), F32)
            g_ref[h, 24 * f + 20:24 * f + 24, :] = jnp.zeros((4, 128), F32)

    for copy in loads:
        copy.wait()
    v_half = vel_ref[...] + (0.5 * TIME_STEP) * frc_ref[...]
    moved = pos_ref[...] + TIME_STEP * v_half
    moved = moved - BOX * jnp.floor(moved * (1.0 / BOX))
    axis_row = iota((3, 1), 0)
    coord = jnp.where(axis_row == 0, bx, jnp.where(axis_row == 1, by, bz)).astype(F32)
    brick_lo = coord * BRICK
    rel = moved - brick_lo
    rel = jnp.where(rel < -0.5 * BRICK, rel + BOX, jnp.where(rel >= 1.5 * BRICK, rel - BOX, rel))
    cell = jnp.floor(rel * (1.0 / SPACING)).astype(jnp.int32) + 2
    live = val_ref[...].reshape(1, CAP) == 1
    ids = id_ref[...].reshape(1, CAP)
    atom_ref[:, pl.ds(KPAD - 128, 128)] = jnp.zeros((atom_ref.shape[0], 128), F32)
    zi = jnp.where(live, (cell[2:3, :] - 4) & 15, 0)
    lo = jnp.where(live, ((cell[1:2, :] - 2) & 15) * 16 + cell[0:1, :], 0)
    rows = list(split3(moved)) + list(split3(v_half))
    for k in range(6):
        atom_ref[8 * k:8 * k + 3, 0:CAP] = rows[k]
    atom_ref[48:49, 0:CAP] = (ids >> 7).astype(F32)
    atom_ref[49:50, 0:CAP] = (ids & 127).astype(F32)
    atom_ref[50:51, 0:CAP] = zi.astype(F32)
    atom_ref[51:52, 0:CAP] = lo.astype(F32)

    zrow = atom_ref[50:51, :]
    lrow = atom_ref[51:52, :]
    zmask = jnp.broadcast_to(zrow, (16, KPAD)) == iota((16, KPAD), 0).astype(F32)
    onehot = jnp.where(jnp.broadcast_to(lrow, (256, KPAD)) == iota((256, KPAD), 0).astype(F32), 1.0, 0.0).astype(BF16)

    def spread(row_idx):
        return jnp.where(zmask, jnp.broadcast_to(atom_ref[row_idx:row_idx + 1, :], (16, KPAD)), 0.0).astype(BF16)

    def exchange(src, dst, ssem, rsem, arrays):
        starts, total = offsets_of(arrays)
        shift = 8 if arrays is pos_arrays else 0
        cut = starts[(1, 0, 0)]
        for delta in POS_ORDER:
            rz, lanes = tile_of(delta)
            part = pl.ds(starts[delta], part_rows(arrays, delta))
            pltpu.make_async_remote_copy(src_ref=src.at[part], dst_ref=dst.at[pl.ds(starts[delta] + shift, part_rows(arrays, delta))], send_sem=ssem, recv_sem=rsem[delta[0]], device_id=partner(delta), device_id_type=MESH_ID).start()
        return [pltpu.make_async_remote_copy(src_ref=src.at[pl.ds(lo, hi - lo)], dst_ref=dst.at[pl.ds(shift + lo, hi - lo)], send_sem=ssem, recv_sem=sem, device_id=partner(DELTAS[0]), device_id_type=MESH_ID) for lo, hi, sem in ((0, cut, rsem[0]), (cut, total, rsem[1]), (0, total, rsem[0]))]

    def keep_own(f, x):
        for h in range(2):
            g_ref[h, 24 * f + 4:24 * f + 20, :] = x[:, 128 * h:128 * h + 128]

    def fill(buf, fields, pack, arrays):
        starts, _ = offsets_of(arrays)
        for delta in DELTAS:
            rz, lanes = tile_of(delta)
            row = starts[delta]
            for arr in pack([to_delta(g_ref, f, delta) for f in fields], delta):
                for piece in arr:
                    if arrays is not pos_arrays:
                        buf[row:row + rz, :] = piece
                        row += rz
                    elif delta[0]:
                        buf[row:row + 6, :] = piece[1:7]
                        row += 6
                    else:
                        buf[row:row + 11, :] = piece[0:11]
                        buf[row + 11:row + 14, :] = piece[13:16]
                        row += 14

    def own_rows(f, start, count):
        return [g_ref[h, 24 * f + 4 + start:24 * f + 4 + start + count, :] for h in range(2)]

    def pos_parts(inner, deltas):
        starts, _ = offsets_of(pos_arrays)
        row8 = iota((8, 128), 0)
        parts = [{} for _ in range(3)]
        for delta in deltas:
            rows = 6 if delta[0] else 14
            row = starts[delta] + 8
            for c in range(3):
                parts[c][delta] = []
                for _ in range(tile_of(delta)[1] // 128):
                    if delta[0]:
                        x = jnp.where((row8 >= 1) & (row8 < 7), precv[row - 1:row + 7, :], 0.0)
                    elif inner:
                        x = precv[row:row + 8, :]
                    else:
                        x = jnp.where(row8 < 3, precv[row + 8:row + 16, :], jnp.where(row8 >= 5, precv[row + 6:row + 14, :], 0.0))
                    parts[c][delta].append(x)
                    row += rows
        return parts

    def vel_fields():
        starts, _ = offsets_of(vel_arrays)
        parts = {}
        for delta in DELTAS:
            rz, lanes = tile_of(delta)
            row = starts[delta]
            arrs = []
            for i in range(vel_arrays(delta)):
                arrs.append([vrecv[row + rz * j:row + rz * j + rz, :] for j in range(lanes // 128)])
                row += rz * lanes // 128
            parts[delta] = unpack_vel(arrs, delta)
        out = []
        for i in range(4):
            mine = {d: parts[d][i] for d in DELTAS}
            level = merge_level(own_rows(3 + i, 0, 16), mine)
            above = merge_above([x[8:16] for x in level], mine)
            out.append([[x[0:8] for x in level], above])
        return out

    lhs = jnp.concatenate([spread(8 * k + c) for k in range(3) for c in range(3)], axis=0)
    binned = dot_split(lhs, onehot, true)
    pos_own = [binned[16 * c:16 * c + 16] + binned[48 + 16 * c:64 + 16 * c] + binned[96 + 16 * c:112 + 16 * c] for c in range(3)]
    for c in range(3):
        keep_own(c, pos_own[c])
    fill(psend, range(3), same, pos_arrays)
    pl.semaphore_wait(barrier, 7)
    pos_all = exchange(psend, precv, psend_sem, (precv_sem, pabove_sem), pos_arrays)

    lhs = jnp.concatenate([spread(8 * k + c) for k in range(3, 6) for c in range(3)] + [spread(48), spread(49)], axis=0)
    binned = dot_split(lhs, onehot, true)
    vel_own = [binned[16 * c:16 * c + 16] + binned[48 + 16 * c:64 + 16 * c] + binned[96 + 16 * c:112 + 16 * c] for c in range(3)]
    vel_own.append(binned[144:160] * 128.0 + binned[160:176])
    for c in range(4):
        keep_own(3 + c, vel_own[c])
    fill(vsend, range(3, 7), pack_vel, vel_arrays)
    vel_all = exchange(vsend, vrecv, vsend_sem, (vrecv_sem, vrecv_sem), vel_arrays)

    los = [bx, by, bz]

    def localise(fields, start):
        out = [[], [], []]
        for h in range(2):
            present = fields[0][h] != 0.0
            lane = iota((8, 128), 1) + 128 * h
            frame = [lane & 15, lane >> 4, iota((8, 128), 0) + start]
            for c in range(3):
                u = fields[c][h] - los[c].astype(F32) * BRICK
                u = jnp.where(u < -0.5 * BRICK, u + BOX, jnp.where(u >= 1.5 * BRICK, u - BOX, u))
                out[c].append(jnp.where(present, u, 64.0 + 4.0 * frame[c].astype(F32)))
        return out

    lane8 = iota((8, 128), 1)

    def put_rows(ref, k, h, x, inner):
        if inner:
            ref[k, pl.ds(8 + h, 8, stride=2), :] = x
        else:
            ref[k, pl.ds(24 + h, 4, stride=2), :] = x[0:4]
            ref[k, pl.ds(h, 4, stride=2), :] = x[4:8]

    def shift_in(s, local, inner):
        dx, dy = SHIFTS[s]
        left = 16 * dy + dx
        for c in range(3):
            a, b = local[c]
            if left:
                a, b = pltpu.roll(a, (-left) % 128, 1), pltpu.roll(b, (-left) % 128, 1)
                here = lane8 < 128 - left if left > 0 else lane8 >= -left
                a, b = jnp.where(here, a, b), jnp.where(here, b, a)
            put_rows(t_ref, 3 * s + c, 0, a, inner)
            put_rows(t_ref, 3 * s + c, 1, b, inner)

    def keep(f, inner_rows, outer_rows):
        for h in range(2):
            put_rows(q_ref, f, h, inner_rows[h], True)
            put_rows(q_ref, f, h, outer_rows[h], False)

    span = [4, 24]

    def load(dx, dy, dz):
        s = SHIFTS.index((dx, dy))
        return [t_ref[3 * s + c, span[0] + 2 * dz:span[0] + 2 * dz + span[1], :] for c in range(3)]

    def low_x():
        return (iota((span[1], 128), 1) & 15) < 8

    def low_y():
        return ((iota((span[1], 128), 0) & 1) == 0) & (iota((span[1], 128), 1) < 96)

    def low_z():
        return iota((span[1], 128), 0) + span[0] < 16

    def pick(mask, p, q):
        m = mask()
        return [jnp.where(m, p[c], q[c]) for c in range(3)]

    def half(dx, dy, dz):
        return dy > 0 or (dy == 0 and (dx > 0 or (dx == 0 and dz > 0)))

    offsets = [(dx, dy, dz) for dx, dy in SHIFTS for dz in range(-2, 3) if (dx, dy, dz) != (0, 0, 0) and (abs(dx) == 2) + (abs(dy) == 2) + (abs(dz) == 2) <= 1]
    first = [functools.partial(load, *d) for d in offsets if half(*d)]
    second = [functools.partial(load, *d) for d in offsets if not half(*d)]
    for dz in range(-1, 2):
        first.append(lambda dz=dz: pick(low_x, load(-2, 2, dz), load(2, 2, dz)))
        second.append(lambda dz=dz: pick(low_x, load(-2, -2, dz), load(2, -2, dz)))
    for dx in range(-1, 2):
        first.append(lambda dx=dx: pick(low_z, load(dx, 2, -2), load(dx, 2, 2)))
        second.append(lambda dx=dx: pick(low_z, load(dx, -2, -2), load(dx, -2, 2)))
    for dy in (1, -1):
        (first if dy == 1 else second).append(lambda dy=dy: pick(low_z, pick(low_x, load(-2, dy, -2), load(2, dy, -2)), pick(low_x, load(-2, dy, 2), load(2, dy, 2))))
    first.append(lambda: pick(low_z, load(2, 0, -2), load(2, 0, 2)))
    second.append(lambda: pick(low_z, load(-2, 0, -2), load(-2, 0, 2)))

    def apart(mine, nbr):
        ex, ey, ez = mine[0] - nbr[0], mine[1] - nbr[1], mine[2] - nbr[2]
        r2 = jnp.minimum(ex * ex + ey * ey + ez * ez, RCUT * RCUT)
        return ex, ey, ez, r2, lax.rsqrt(r2)

    def pair_energy(row):
        span[:] = [row, 8]
        mine = load(0, 0, 0)
        sw, sr = jnp.zeros((8, 128), F32), jnp.zeros((8, 128), F32)
        for i, nbr in enumerate(first):
            ex, ey, ez, r2, inv = apart(mine, nbr())
            i2 = inv * inv
            i6 = i2 * i2 * i2
            sw = sw + i6 * (i6 - 1.0)
            sr = sr + r2 * inv
            for k, x in enumerate((ex, ey, ez, inv)):
                p_ref[4 * i + k, row - 4:row + 4, :] = x
        return 4.0 * sw - DU_CUT * sr + (RCUT * DU_CUT - U_CUT) * len(first)

    early = [s for s, (dx, dy) in enumerate(SHIFTS) if dy > 0 or (dy == 0 and dx >= 0)]
    late = [s for s in range(25) if s not in early]
    pos_all[0].wait_recv()
    parts = pos_parts(True, DELTAS[:3])
    inner = [merge_level(own_rows(c, 0, 8), parts[c]) for c in range(3)]
    inner_local = localise(inner, 0)
    for s in early:
        shift_in(s, inner_local, True)
    e_mid = pair_energy(12)
    pos_all[1].wait_recv()
    parts = pos_parts(False, DELTAS)
    outer = [merge_above(merge_level(own_rows(c, 8, 8), parts[c]), parts[c]) for c in range(3)]
    outer_local = localise(outer, 8)
    for s in early:
        shift_in(s, outer_local, False)
    e_low, e_high = pair_energy(4), pair_energy(20)
    span[:] = [4, 24]
    keep(0, inner[0], outer[0])
    lane24 = iota((24, 128), 1)
    x24 = lane24 & 15
    own = (((iota((24, 128), 0) & 1) == 0) | (lane24 < 64)) & (x24 >= 2) & (x24 < 14) & (q_ref[0, 4:28, :] != 0.0)
    energy = jnp.where(own, jnp.concatenate([e_low, e_mid, e_high], axis=0), 0.0)
    me = bz * 4 + by * 2 + bx
    ebuf[me, :, :] = energy[0:8] + energy[8:16] + energy[16:24]
    for delta in SEND_ORDER:
        pltpu.make_async_remote_copy(src_ref=ebuf.at[me], dst_ref=ebuf.at[me], send_sem=esend_sem, recv_sem=erecv_sem, device_id=partner(delta), device_id_type=MESH_ID).start()
    energy_all = pltpu.make_async_remote_copy(src_ref=ebuf.at[pl.ds(0, 7)], dst_ref=ebuf.at[pl.ds(0, 7)], send_sem=esend_sem, recv_sem=erecv_sem, device_id=partner(DELTAS[0]), device_id_type=MESH_ID)

    vel_all[2].wait_recv()
    for f, (a, b) in enumerate(vel_fields()):
        keep(3 + f, a, b)
    for c in range(1, 3):
        keep(c, inner[c], outer[c])

    for s in late:
        shift_in(s, inner_local, True)
        shift_in(s, outer_local, False)
    mine = load(0, 0, 0)

    def push(acc, ex, ey, ez, inv):
        i2 = inv * inv
        i6 = i2 * i2 * i2
        fr = (i6 * (i6 - 0.5)) * i2 + (DU_CUT / 48.0) * inv
        return (acc[0] + fr * ex, acc[1] + fr * ey, acc[2] + fr * ez)

    acc = tuple(jnp.zeros((24, 128), F32) for _ in range(3))
    for i in range(len(first)):
        acc = push(acc, *(p_ref[4 * i + k] for k in range(4)))
    for nbr in second:
        ex, ey, ez, r2, inv = apart(mine, nbr())
        acc = push(acc, ex, ey, ez, inv)
    force = [48.0 * acc[c] for c in range(3)]

    idv = jnp.where(own, q_ref[6, 4:28, :], -1.0)
    id_int = idv.astype(jnp.int32)
    id_hi = jnp.where(own, id_int >> 7, -1).astype(F32)
    id_lo = jnp.where(own, id_int & 127, -1).astype(F32)

    def flat(x, n):
        return jnp.concatenate([jnp.broadcast_to(x[r:r + 1, :], (n, 128)) for r in range(24)], axis=1)

    hot_hi = jnp.where(flat(id_hi, 128) == iota((128, 3072), 0).astype(F32), 1.0, 0.0).astype(BF16)
    lo_eq = flat(id_lo, 128) == iota((128, 3072), 0).astype(F32)
    hot_lo = jnp.where(lo_eq, 1.0, 0.0).astype(BF16)
    table = dot_split(hot_lo, hot_hi, true).astype(BF16)
    r128, c128 = iota((128, 128), 0), iota((128, 128), 1)
    below = dot_nn(jnp.where(c128 < r128, 1.0, 0.0).astype(BF16), table)
    total = dot_nn(jnp.ones((128, 128), BF16), table).astype(BF16)
    before = dot_nn(total, jnp.where(r128 < c128, 1.0, 0.0).astype(BF16))
    rank_tab = below + before
    tab_hi = jnp.floor(rank_tab * (1.0 / 256.0)) * 256.0
    tab_lo = rank_tab - tab_hi
    tabs = jnp.concatenate([tab_hi, tab_lo], axis=1).astype(BF16)
    hot2 = jnp.concatenate([hot_hi, hot_hi], axis=0)
    looked = jnp.concatenate([dot_nn(tabs, hot2[:, :1536]), dot_nn(tabs, hot2[:, 1536:])], axis=1)
    rank = jnp.sum(jnp.where(lo_eq, looked, 0.0), axis=0, keepdims=True)
    any_own = flat(jnp.where(own, 1.0, 0.0), 1) > 0.5
    rank_hi = jnp.floor(rank * (1.0 / 256.0))
    rank_lo = jnp.where(any_own, rank - 256.0 * rank_hi, -1.0)
    rank_hi = jnp.where(any_own, rank_hi, -1.0)

    hot_slot = jnp.where(jnp.broadcast_to(rank_lo, (256, 3072)) == iota((256, 3072), 0).astype(F32), 1.0, 0.0).astype(BF16)
    hi_mask = jnp.broadcast_to(rank_hi, (8, 3072)) == iota((8, 3072), 0).astype(F32)
    outs = []
    for c in range(3):
        outs += list(split3(q_ref[c, 4:28, :]))
    for c in range(3):
        outs += list(split3(q_ref[3 + c, 4:28, :] + (0.5 * TIME_STEP) * force[c]))
    for c in range(3):
        outs += list(split3(force[c]))
    outs += [id_hi, id_lo, jnp.where(own, 1.0, 0.0)]
    lhs = jnp.concatenate([jnp.where(hi_mask, flat(x, 8), 0.0) for x in outs], axis=0).astype(BF16)
    slots = dot_split(lhs, hot_slot, true)

    def field(i):
        return slots[8 * i:8 * i + 8, :]

    def put(ref, row, x):
        for h in range(7):
            n = 256 if h < 6 else CAP - 1536
            ref[row:row + 1, 256 * h:256 * h + n] = x[h:h + 1, 0:n].astype(ref.dtype)

    for c in range(3):
        put(opos_ref, c, field(3 * c) + field(3 * c + 1) + field(3 * c + 2))
        put(ovel_ref, c, field(9 + 3 * c) + field(10 + 3 * c) + field(11 + 3 * c))
        put(ofrc_ref, c, field(18 + 3 * c) + field(19 + 3 * c) + field(20 + 3 * c))
    put(oid_ref, 0, field(27) * 128.0 + field(28))
    put(oval_ref, 0, field(29))

    for copy in (pos_all[2], vel_all[2], energy_all):
        copy.wait_send()
    energy_all.wait_recv()
    acc = ebuf[0]
    for k in range(1, 8):
        acc = acc + ebuf[k]
    oen_ref[...] = acc


def finish(pos_ref, vel_ref, frc_ref, id_ref, val_ref, en_ref, opos_ref, ovel_ref, ofrc_ref, oid_ref, oval_ref, oen_ref):
    opos_ref[...] = pos_ref[...]
    ovel_ref[...] = vel_ref[...]
    ofrc_ref[...] = frc_ref[...]
    oid_ref[...] = id_ref[...].reshape(CAP)
    oval_ref[...] = val_ref[...].reshape(CAP)
    oen_ref[...] = jnp.sum(jnp.sum(en_ref[...], axis=0, keepdims=True), axis=1, keepdims=True)


def solution(mesh):
    row_spec = P(BRICK_AXES, None)
    flat_spec = P(BRICK_AXES)
    vmem = pl.BlockSpec(memory_space=pltpu.VMEM)

    def local_step(pos, vel, frc, ids, valid):
        f3 = jax.ShapeDtypeStruct((3, CAP), F32)
        i1 = jax.ShapeDtypeStruct((CAP,), jnp.int32)
        outs = pl.pallas_call(
            kernel,
            out_shape=(pltpu.VMEM((3, CAP), F32),) * 3 + (pltpu.VMEM((1, CAP), jnp.int32),) * 2 + (pltpu.VMEM((8, 128), F32),),
            in_specs=[pl.BlockSpec(memory_space=pltpu.HBM)] * 5,
            out_specs=(vmem,) * 6,
            scratch_shapes=[pltpu.VMEM((offsets_of(pos_arrays)[1], 128), F32), pltpu.VMEM((offsets_of(pos_arrays)[1] + 16, 128), F32)] + [pltpu.VMEM((offsets_of(vel_arrays)[1], 128), F32)] * 2 + [
                pltpu.VMEM((3, CAP), F32),
                pltpu.VMEM((3, CAP), F32),
                pltpu.VMEM((3, CAP), F32),
                pltpu.VMEM((CAP,), jnp.int32),
                pltpu.VMEM((CAP,), jnp.int32),
                pltpu.SemaphoreType.DMA((5,)),
                pltpu.VMEM((56, KPAD), F32),
                pltpu.VMEM((2, 168, 128), F32),
                pltpu.VMEM((75, 32, 128), F32),
                pltpu.VMEM((NF, 32, 128), F32),
                pltpu.VMEM((192, 24, 128), F32),
                pltpu.VMEM((8, 8, 128), F32),
                pltpu.SemaphoreType.DMA,
                pltpu.SemaphoreType.DMA,
                pltpu.SemaphoreType.DMA,
                pltpu.SemaphoreType.DMA,
                pltpu.SemaphoreType.DMA,
                pltpu.SemaphoreType.DMA,
                pltpu.SemaphoreType.DMA,
            ],
            compiler_params=pltpu.CompilerParams(collective_id=0, has_side_effects=True),
        )(pos.T, vel.T, frc.T, ids, valid)
        outs = pl.pallas_call(
            finish,
            out_shape=(f3, f3, f3, i1, i1, jax.ShapeDtypeStruct((1, 1), F32)),
            in_specs=[vmem] * 6,
            out_specs=(vmem,) * 6,
            compiler_params=pltpu.CompilerParams(vmem_limit_bytes=4 << 20),
        )(*outs)
        return outs[0].T, outs[1].T, outs[2].T, outs[3], outs[4], outs[5][0, 0]

    return jax.shard_map(local_step, mesh=mesh, in_specs=(row_spec, row_spec, row_spec, flat_spec, flat_spec), out_specs=(row_spec, row_spec, row_spec, flat_spec, flat_spec, P()), check_vma=False)
```

```python
import functools

import jax
import jax.numpy as jnp
from jax import lax
from jax.experimental import pallas as pl
from jax.experimental.pallas import tpu as pltpu
from jax.sharding import PartitionSpec as P

TIME_STEP = 0.005
RCUT = 2.5
DENSITY = 0.8442
SPACING = (1.0 / DENSITY) ** (1.0 / 3.0)
SITES = 12
BRICK = SITES * SPACING
BOX = 2.0 * BRICK
BRICK_AXES = ("bz", "by", "bx")
CAP = SITES ** 3
KPAD = 1792
MESH_ID = pl.DeviceIdType.MESH
F32 = jnp.float32
BF16 = jnp.bfloat16
CUT6 = RCUT ** -6
U_CUT = 4.0 * (CUT6 * CUT6 - CUT6)
DU_CUT = (-48.0 * CUT6 * CUT6 + 24.0 * CUT6) / RCUT
DELTAS = [(d >> 2 & 1, d >> 1 & 1, d & 1) for d in range(1, 8)]
SEND_ORDER = [(1, 1, 0), (1, 1, 1), (0, 1, 0), (1, 0, 0), (0, 1, 1), (1, 0, 1), (0, 0, 1)]
POS_ORDER = [(1, 1, 0), (0, 1, 0), (1, 1, 1), (0, 1, 1), (1, 0, 0), (1, 0, 1), (0, 0, 1)]
SHIFTS = [(dx, dy) for dy in range(-2, 3) for dx in range(-2, 3)]
NF = 7


def iota(shape, dim):
    return lax.broadcasted_iota(jnp.int32, shape, dim)


def split3(x):
    hi = x.astype(BF16).astype(F32)
    rest = x - hi
    mid = rest.astype(BF16).astype(F32)
    return hi, mid, rest - mid


def dot_nt(a, b):
    return lax.dot_general(a, b, (((1,), (1,)), ((), ())), preferred_element_type=F32)


def dot_split(a, b, true):
    cut = a.shape[1] // 512 * 256
    return dot_nt(a[:, :cut], b[:, :cut]) + jnp.where(true, dot_nt(a[:, cut:], b[:, cut:]), 0.0)


def dot_nn(a, b):
    return lax.dot_general(a, b, (((1,), (0,)), ((), ())), preferred_element_type=F32)


def tile_of(delta):
    return 8 if delta[0] else 16, 128 if delta[1] else 256


def pos_arrays(delta):
    return 3


def vel_arrays(delta):
    return 1 if delta[0] or delta[1] else 4


def offsets_of(arrays):
    starts, row = {}, 0
    for delta in DELTAS:
        starts[delta] = row
        row += part_rows(arrays, delta)
    return starts, row


def part_rows(arrays, delta):
    rz, lanes = tile_of(delta)
    if arrays is pos_arrays:
        rz = 6 if delta[0] else 8 if delta == (0, 1, 1) else 14
    return arrays(delta) * rz * lanes // 128


def to_delta(g_ref, f, delta):
    dz, dy, dx = delta
    first = 24 * f + 4
    halves = []
    for h in range(2):
        if dz:
            halves.append(jnp.where(iota((8, 128), 0) < 4, g_ref[h, first + 12:first + 20, :], g_ref[h, first + 4:first + 12, :]))
        else:
            halves.append(g_ref[h, first:first + 16, :])
    lane = iota(halves[0].shape, 1)
    xf = lane & 15

    def along_x(x, turn):
        if not dx:
            return pltpu.roll(x, turn, 1) if turn else x
        return jnp.where(xf < 3, pltpu.roll(x, (turn + 116) % 128, 1), jnp.where(xf >= 13, pltpu.roll(x, turn + 12, 1), 0.0))

    if dy:
        group = lane >> 4
        return [jnp.where((group == 4) | (group == 5), along_x(halves[0], 64), jnp.where((group == 1) | (group == 2), 0.0, along_x(halves[1], 64)))]
    return [along_x(x, 0) for x in halves]


def folded(g_ref, f):
    first = 24 * f + 4
    row, moved = iota((8, 128), 0), (iota((8, 128), 1) - 6) & 127
    xf, group = moved & 15, moved >> 4
    outer = [jnp.where(row < 3, g_ref[h, first + 8:first + 16, :], g_ref[h, first + 10:first + 18, :]) for h in range(2)]

    def along_x(x):
        return jnp.where(xf < 3, pltpu.roll(x, 58, 1), jnp.where(xf >= 13, pltpu.roll(x, 82, 1), 0.0))

    out = jnp.where((group == 4) | (group == 5), along_x(outer[0]), jnp.where((group == 1) | (group == 2), 0.0, along_x(outer[1])))
    return to_delta(g_ref, f, (0, 1, 1))[0][0:8] + jnp.where(row < 6, out, 0.0)


def wide(b):
    lane = iota(b.shape, 1)
    return [jnp.where(lane < 16, b, 0.0), jnp.where(lane >= 48, b, 0.0)]


def same(f, delta):
    return f


def pack_vel(f, delta):
    dz, dy, _ = delta
    if dz:
        row = iota(f[0][0].shape, 0)
        outs = []
        for j in range(len(f[0])):
            out = jnp.zeros_like(f[0][j])
            for k in range(4):
                out = jnp.where(row == 2 * k, jnp.broadcast_to(f[k][j][6:7], out.shape), out)
                out = jnp.where(row == 2 * k + 1, jnp.broadcast_to(f[k][j][1:2], out.shape), out)
            outs.append(out)
        return [outs]
    if dy:
        f = [x[0] for x in f]
        group = iota(f[0].shape, 1) >> 4
        out = jnp.where((group == 0) | (group == 3), f[0], 0.0)
        out = jnp.where((group == 1) | (group == 4), pltpu.roll(f[1], 16, 1), out)
        out = jnp.where((group == 2) | (group == 5), pltpu.roll(f[2], 32, 1), out)
        out = jnp.where(group == 6, pltpu.roll(f[3], 96, 1), out)
        return [[jnp.where(group == 7, pltpu.roll(f[3], 64, 1), out)]]
    return f


def unpack_vel(a, delta):
    dz, dy, _ = delta
    if dz:
        row = iota(a[0][0].shape, 0)
        return [[jnp.where(row == 6, jnp.broadcast_to(x[2 * k:2 * k + 1], x.shape), jnp.where(row == 1, jnp.broadcast_to(x[2 * k + 1:2 * k + 2], x.shape), 0.0)) for x in a[0]] for k in range(4)]
    if dy:
        x = a[0][0]
        group = iota(x.shape, 1) >> 4
        low, high = group == 0, group == 3
        both = low | high
        last = jnp.where(low, pltpu.roll(x, 32, 1), jnp.where(high, pltpu.roll(x, 64, 1), 0.0))
        return [[jnp.where(both, x, 0.0)], [jnp.where(both, pltpu.roll(x, 112, 1), 0.0)], [jnp.where(both, pltpu.roll(x, 96, 1), 0.0)], [last]]
    return a


def merge_level(own, parts):
    near = wide(parts[(0, 1, 0)][0] + parts[(0, 1, 1)][0])
    return [own[h] + parts[(0, 0, 1)][h] + near[h] for h in range(2)]


def merge_above(own, parts):
    far = wide(parts[(1, 1, 0)][0] + parts[(1, 1, 1)][0])
    return [own[h] + parts[(1, 0, 0)][h] + parts[(1, 0, 1)][h] + far[h] for h in range(2)]


def kernel(pos_hbm, vel_hbm, frc_hbm, id_hbm, val_hbm, opos_ref, ovel_ref, ofrc_ref, oid_ref, oval_ref, oen_ref, *scratch):
    psend, precv, vsend, vrecv, pos_ref, vel_ref, frc_ref, id_ref, val_ref, in_sem, atom_ref, g_ref, t_ref, q_ref, p_ref, ebuf, psend_sem, precv_sem, pabove_sem, vsend_sem, vrecv_sem, esend_sem, erecv_sem = scratch
    bz, by, bx = lax.axis_index("bz"), lax.axis_index("by"), lax.axis_index("bx")

    true = bz >= 0

    def partner(delta):
        return (lax.rem(bz + delta[0], 2), lax.rem(by + delta[1], 2), lax.rem(bx + delta[2], 2))

    barrier = pltpu.get_barrier_semaphore()
    for delta in SEND_ORDER:
        pl.semaphore_signal(barrier, inc=1, device_id=partner(delta), device_id_type=MESH_ID)

    loads = [pltpu.make_async_copy(src, dst, in_sem.at[i]) for i, (src, dst) in enumerate(((vel_hbm, vel_ref), (frc_hbm, frc_ref), (pos_hbm, pos_ref), (val_hbm, val_ref), (id_hbm, id_ref)))]
    for copy in loads:
        copy.start()
    for f in range(NF):
        for h in range(2):
            g_ref[h, 24 * f:24 * f + 4, :] = jnp.zeros((4, 128), F32)
            g_ref[h, 24 * f + 20:24 * f + 24, :] = jnp.zeros((4, 128), F32)

    for copy in loads:
        copy.wait()
    v_half = vel_ref[...] + (0.5 * TIME_STEP) * frc_ref[...]
    moved = pos_ref[...] + TIME_STEP * v_half
    moved = moved - BOX * jnp.floor(moved * (1.0 / BOX))
    axis_row = iota((3, 1), 0)
    coord = jnp.where(axis_row == 0, bx, jnp.where(axis_row == 1, by, bz)).astype(F32)
    brick_lo = coord * BRICK
    rel = moved - brick_lo
    rel = jnp.where(rel < -0.5 * BRICK, rel + BOX, jnp.where(rel >= 1.5 * BRICK, rel - BOX, rel))
    cell = jnp.floor(rel * (1.0 / SPACING)).astype(jnp.int32) + 2
    live = val_ref[...].reshape(1, CAP) == 1
    ids = id_ref[...].reshape(1, CAP)
    atom_ref[:, pl.ds(KPAD - 128, 128)] = jnp.zeros((atom_ref.shape[0], 128), F32)
    zi = jnp.where(live, (cell[2:3, :] - 4) & 15, 0)
    lo = jnp.where(live, ((cell[1:2, :] - 2) & 15) * 16 + cell[0:1, :], 0)
    rows = list(split3(moved)) + list(split3(v_half))
    for k in range(6):
        atom_ref[8 * k:8 * k + 3, 0:CAP] = rows[k]
    atom_ref[48:49, 0:CAP] = (ids >> 7).astype(F32)
    atom_ref[49:50, 0:CAP] = (ids & 127).astype(F32)
    atom_ref[50:51, 0:CAP] = zi.astype(F32)
    atom_ref[51:52, 0:CAP] = lo.astype(F32)

    zrow = atom_ref[50:51, :]
    lrow = atom_ref[51:52, :]
    zmask = jnp.broadcast_to(zrow, (16, KPAD)) == iota((16, KPAD), 0).astype(F32)
    onehot = jnp.where(jnp.broadcast_to(lrow, (256, KPAD)) == iota((256, KPAD), 0).astype(F32), 1.0, 0.0).astype(BF16)

    def spread(row_idx):
        return jnp.where(zmask, jnp.broadcast_to(atom_ref[row_idx:row_idx + 1, :], (16, KPAD)), 0.0).astype(BF16)

    def exchange(src, dst, ssem, rsem, arrays):
        starts, total = offsets_of(arrays)
        shift = 8 if arrays is pos_arrays else 0
        cut = starts[(1, 0, 0)]
        for delta in POS_ORDER:
            rz, lanes = tile_of(delta)
            part = pl.ds(starts[delta], part_rows(arrays, delta))
            pltpu.make_async_remote_copy(src_ref=src.at[part], dst_ref=dst.at[pl.ds(starts[delta] + shift, part_rows(arrays, delta))], send_sem=ssem, recv_sem=rsem[delta[0]], device_id=partner(delta), device_id_type=MESH_ID).start()
        return [pltpu.make_async_remote_copy(src_ref=src.at[pl.ds(lo, hi - lo)], dst_ref=dst.at[pl.ds(shift + lo, hi - lo)], send_sem=ssem, recv_sem=sem, device_id=partner(DELTAS[0]), device_id_type=MESH_ID) for lo, hi, sem in ((0, cut, rsem[0]), (cut, total, rsem[1]), (0, total, rsem[0]))]

    def keep_own(f, x):
        for h in range(2):
            g_ref[h, 24 * f + 4:24 * f + 20, :] = x[:, 128 * h:128 * h + 128]

    def fill(buf, fields, pack, arrays):
        starts, _ = offsets_of(arrays)
        for delta in DELTAS:
            rz, lanes = tile_of(delta)
            row = starts[delta]
            if arrays is pos_arrays and delta == (0, 1, 1):
                for f in fields:
                    buf[row + 8 * f:row + 8 * f + 8, :] = folded(g_ref, f)
                continue
            for arr in pack([to_delta(g_ref, f, delta) for f in fields], delta):
                for piece in arr:
                    if arrays is not pos_arrays:
                        buf[row:row + rz, :] = piece
                        row += rz
                    elif delta[0]:
                        buf[row:row + 6, :] = piece[1:7]
                        row += 6
                    else:
                        buf[row:row + 11, :] = piece[0:11]
                        buf[row + 11:row + 14, :] = piece[13:16]
                        row += 14

    def own_rows(f, start, count):
        return [g_ref[h, 24 * f + 4 + start:24 * f + 4 + start + count, :] for h in range(2)]

    def pos_parts(inner, deltas):
        starts, _ = offsets_of(pos_arrays)
        row8 = iota((8, 128), 0)
        parts = [{} for _ in range(3)]
        for delta in deltas:
            rows = 6 if delta[0] else 8 if delta == (0, 1, 1) else 14
            row = starts[delta] + 8
            for c in range(3):
                parts[c][delta] = []
                for _ in range(tile_of(delta)[1] // 128):
                    if delta[0]:
                        x = jnp.where((row8 >= 1) & (row8 < 7), precv[row - 1:row + 7, :], 0.0)
                    elif delta == (0, 1, 1):
                        xf = iota((8, 128), 1) & 15
                        x = precv[row:row + 8, :]
                        if not inner:
                            x = pltpu.roll(jnp.where(row8 < 3, x, precv[row - 2:row + 6, :]), 122, 1)
                        x = jnp.where(((xf < 3) | (xf >= 13)) & (inner | (row8 < 3) | (row8 >= 5)), x, 0.0)
                    elif inner:
                        x = precv[row:row + 8, :]
                    else:
                        x = jnp.where(row8 < 3, precv[row + 8:row + 16, :], jnp.where(row8 >= 5, precv[row + 6:row + 14, :], 0.0))
                    parts[c][delta].append(x)
                    row += rows
        return parts

    def vel_fields():
        starts, _ = offsets_of(vel_arrays)
        parts = {}
        for delta in DELTAS:
            rz, lanes = tile_of(delta)
            row = starts[delta]
            arrs = []
            for i in range(vel_arrays(delta)):
                arrs.append([vrecv[row + rz * j:row + rz * j + rz, :] for j in range(lanes // 128)])
                row += rz * lanes // 128
            parts[delta] = unpack_vel(arrs, delta)
        out = []
        for i in range(4):
            mine = {d: parts[d][i] for d in DELTAS}
            level = merge_level(own_rows(3 + i, 0, 16), mine)
            above = merge_above([x[8:16] for x in level], mine)
            out.append([[x[0:8] for x in level], above])
        return out

    lhs = jnp.concatenate([spread(8 * k + c) for k in range(3) for c in range(3)], axis=0)
    binned = dot_split(lhs, onehot, true)
    pos_own = [binned[16 * c:16 * c + 16] + binned[48 + 16 * c:64 + 16 * c] + binned[96 + 16 * c:112 + 16 * c] for c in range(3)]
    for c in range(3):
        keep_own(c, pos_own[c])
    fill(psend, range(3), same, pos_arrays)
    pl.semaphore_wait(barrier, 7)
    pos_all = exchange(psend, precv, psend_sem, (precv_sem, pabove_sem), pos_arrays)

    lhs = jnp.concatenate([spread(8 * k + c) for k in range(3, 6) for c in range(3)] + [spread(48), spread(49)], axis=0)
    binned = dot_split(lhs, onehot, true)
    vel_own = [binned[16 * c:16 * c + 16] + binned[48 + 16 * c:64 + 16 * c] + binned[96 + 16 * c:112 + 16 * c] for c in range(3)]
    vel_own.append(binned[144:160] * 128.0 + binned[160:176])
    for c in range(4):
        keep_own(3 + c, vel_own[c])
    fill(vsend, range(3, 7), pack_vel, vel_arrays)
    vel_all = exchange(vsend, vrecv, vsend_sem, (vrecv_sem, vrecv_sem), vel_arrays)

    los = [bx, by, bz]

    def localise(fields, start):
        out = [[], [], []]
        for h in range(2):
            present = fields[0][h] != 0.0
            lane = iota((8, 128), 1) + 128 * h
            frame = [lane & 15, lane >> 4, iota((8, 128), 0) + start]
            for c in range(3):
                u = fields[c][h] - los[c].astype(F32) * BRICK
                u = jnp.where(u < -0.5 * BRICK, u + BOX, jnp.where(u >= 1.5 * BRICK, u - BOX, u))
                out[c].append(jnp.where(present, u, 64.0 + 4.0 * frame[c].astype(F32)))
        return out

    lane8 = iota((8, 128), 1)

    def put_rows(ref, k, h, x, inner):
        if inner:
            ref[k, pl.ds(8 + h, 8, stride=2), :] = x
        else:
            ref[k, pl.ds(24 + h, 4, stride=2), :] = x[0:4]
            ref[k, pl.ds(h, 4, stride=2), :] = x[4:8]

    def shift_in(s, local, inner):
        dx, dy = SHIFTS[s]
        left = 16 * dy + dx
        for c in range(3):
            a, b = local[c]
            if left:
                a, b = pltpu.roll(a, (-left) % 128, 1), pltpu.roll(b, (-left) % 128, 1)
                here = lane8 < 128 - left if left > 0 else lane8 >= -left
                a, b = jnp.where(here, a, b), jnp.where(here, b, a)
            put_rows(t_ref, 3 * s + c, 0, a, inner)
            put_rows(t_ref, 3 * s + c, 1, b, inner)

    def keep(f, inner_rows, outer_rows):
        for h in range(2):
            put_rows(q_ref, f, h, inner_rows[h], True)
            put_rows(q_ref, f, h, outer_rows[h], False)

    span = [4, 24]
    row8 = iota((8, 128), 0)

    def load(dx, dy, dz):
        s = SHIFTS.index((dx, dy))
        if span[0] is None:
            return [jnp.where(row8 < 4, t_ref[3 * s + c, 4 + 2 * dz:12 + 2 * dz, :], t_ref[3 * s + c, 20 + 2 * dz:28 + 2 * dz, :]) for c in range(3)]
        return [t_ref[3 * s + c, span[0] + 2 * dz:span[0] + 2 * dz + span[1], :] for c in range(3)]

    def low_x():
        return (iota((span[1], 128), 1) & 15) < 8

    def low_y():
        return ((iota((span[1], 128), 0) & 1) == 0) & (iota((span[1], 128), 1) < 96)

    def low_z():
        return row8 < 4 if span[0] is None else iota((span[1], 128), 0) + span[0] < 16

    def pick(mask, p, q):
        m = mask()
        return [jnp.where(m, p[c], q[c]) for c in range(3)]

    def half(dx, dy, dz):
        return dy > 0 or (dy == 0 and (dx > 0 or (dx == 0 and dz > 0)))

    offsets = [(dx, dy, dz) for dx, dy in SHIFTS for dz in range(-2, 3) if (dx, dy, dz) != (0, 0, 0) and (abs(dx) == 2) + (abs(dy) == 2) + (abs(dz) == 2) <= 1]
    first = [functools.partial(load, *d) for d in offsets if half(*d)]
    second = [functools.partial(load, *d) for d in offsets if not half(*d)]
    for dz in range(-1, 2):
        first.append(lambda dz=dz: pick(low_x, load(-2, 2, dz), load(2, 2, dz)))
        second.append(lambda dz=dz: pick(low_x, load(-2, -2, dz), load(2, -2, dz)))
    for dx in range(-1, 2):
        first.append(lambda dx=dx: pick(low_z, load(dx, 2, -2), load(dx, 2, 2)))
        second.append(lambda dx=dx: pick(low_z, load(dx, -2, -2), load(dx, -2, 2)))
    for dy in (1, -1):
        (first if dy == 1 else second).append(lambda dy=dy: pick(low_z, pick(low_x, load(-2, dy, -2), load(2, dy, -2)), pick(low_x, load(-2, dy, 2), load(2, dy, 2))))
    first.append(lambda: pick(low_z, load(2, 0, -2), load(2, 0, 2)))
    second.append(lambda: pick(low_z, load(-2, 0, -2), load(-2, 0, 2)))

    def apart(mine, nbr):
        ex, ey, ez = mine[0] - nbr[0], mine[1] - nbr[1], mine[2] - nbr[2]
        r2 = jnp.minimum(ex * ex + ey * ey + ez * ez, RCUT * RCUT)
        return ex, ey, ez, r2, lax.rsqrt(r2)

    def pair_energy(row):
        span[:] = [row, 8]
        mine = load(0, 0, 0)
        sw, sr = jnp.zeros((8, 128), F32), jnp.zeros((8, 128), F32)
        for i, nbr in enumerate(first):
            ex, ey, ez, r2, inv = apart(mine, nbr())
            i2 = inv * inv
            i6 = i2 * i2 * i2
            sw = sw + i6 * (i6 - 1.0)
            sr = sr + r2 * inv
        return 4.0 * sw - DU_CUT * sr + (RCUT * DU_CUT - U_CUT) * len(first)

    early = [s for s, (dx, dy) in enumerate(SHIFTS) if dy > 0 or (dy == 0 and dx >= 0)]
    late = [s for s in range(25) if s not in early]
    pos_all[0].wait_recv()
    parts = pos_parts(True, DELTAS[:3])
    inner = [merge_level(own_rows(c, 0, 8), parts[c]) for c in range(3)]
    inner_local = localise(inner, 0)
    for s in early:
        shift_in(s, inner_local, True)
    parts = pos_parts(False, DELTAS[:3])
    outer = [merge_level(own_rows(c, 8, 8), parts[c]) for c in range(3)]
    outer_local = localise(outer, 8)
    for s in early:
        shift_in(s, outer_local, False)
    middle = [pair_energy(8), pair_energy(16)]
    pos_all[1].wait_recv()
    parts = pos_parts(False, DELTAS[3:])
    outer = [merge_above(outer[c], parts[c]) for c in range(3)]
    outer_local = localise(outer, 8)
    for s in early:
        shift_in(s, outer_local, False)
    edges = pair_energy(None)
    span[:] = [4, 24]
    keep(0, inner[0], outer[0])
    lane24 = iota((24, 128), 1)
    x24 = lane24 & 15
    own = (((iota((24, 128), 0) & 1) == 0) | (lane24 < 64)) & (x24 >= 2) & (x24 < 14) & (q_ref[0, 4:28, :] != 0.0)
    energy = jnp.where(own, jnp.concatenate([edges[0:4]] + middle + [edges[4:8]], axis=0), 0.0)
    me = bz * 4 + by * 2 + bx
    ebuf[me, :, :] = energy[0:8] + energy[8:16] + energy[16:24]
    for delta in SEND_ORDER:
        pltpu.make_async_remote_copy(src_ref=ebuf.at[me], dst_ref=ebuf.at[me], send_sem=esend_sem, recv_sem=erecv_sem, device_id=partner(delta), device_id_type=MESH_ID).start()
    energy_all = pltpu.make_async_remote_copy(src_ref=ebuf.at[pl.ds(0, 7)], dst_ref=ebuf.at[pl.ds(0, 7)], send_sem=esend_sem, recv_sem=erecv_sem, device_id=partner(DELTAS[0]), device_id_type=MESH_ID)

    vel_all[2].wait_recv()
    for f, (a, b) in enumerate(vel_fields()):
        keep(3 + f, a, b)
    for c in range(1, 3):
        keep(c, inner[c], outer[c])

    for s in late:
        shift_in(s, inner_local, True)
        shift_in(s, outer_local, False)
    mine = load(0, 0, 0)

    def push(acc, ex, ey, ez, inv):
        i2 = inv * inv
        i6 = i2 * i2 * i2
        fr = (i6 * (i6 - 0.5)) * i2 + (DU_CUT / 48.0) * inv
        return (acc[0] + fr * ex, acc[1] + fr * ey, acc[2] + fr * ez)

    acc = tuple(jnp.zeros((24, 128), F32) for _ in range(3))
    for nbr in first + second:
        ex, ey, ez, r2, inv = apart(mine, nbr())
        acc = push(acc, ex, ey, ez, inv)
    force = [48.0 * acc[c] for c in range(3)]

    idv = jnp.where(own, q_ref[6, 4:28, :], -1.0)
    id_int = idv.astype(jnp.int32)
    id_hi = jnp.where(own, id_int >> 7, -1).astype(F32)
    id_lo = jnp.where(own, id_int & 127, -1).astype(F32)

    def flat(x, n):
        return jnp.concatenate([jnp.broadcast_to(x[r:r + 1, :], (n, 128)) for r in range(24)], axis=1)

    hot_hi = jnp.where(flat(id_hi, 128) == iota((128, 3072), 0).astype(F32), 1.0, 0.0).astype(BF16)
    lo_eq = flat(id_lo, 128) == iota((128, 3072), 0).astype(F32)
    hot_lo = jnp.where(lo_eq, 1.0, 0.0).astype(BF16)
    table = dot_split(hot_lo, hot_hi, true).astype(BF16)
    r128, c128 = iota((128, 128), 0), iota((128, 128), 1)
    below = dot_nn(jnp.where(c128 < r128, 1.0, 0.0).astype(BF16), table)
    total = dot_nn(jnp.ones((128, 128), BF16), table).astype(BF16)
    before = dot_nn(total, jnp.where(r128 < c128, 1.0, 0.0).astype(BF16))
    rank_tab = below + before
    tab_hi = jnp.floor(rank_tab * (1.0 / 256.0)) * 256.0
    tab_lo = rank_tab - tab_hi
    tabs = jnp.concatenate([tab_hi, tab_lo], axis=1).astype(BF16)
    hot2 = jnp.concatenate([hot_hi, hot_hi], axis=0)
    looked = jnp.concatenate([dot_nn(tabs, hot2[:, :1536]), dot_nn(tabs, hot2[:, 1536:])], axis=1)
    rank = jnp.sum(jnp.where(lo_eq, looked, 0.0), axis=0, keepdims=True)
    any_own = flat(jnp.where(own, 1.0, 0.0), 1) > 0.5
    rank_hi = jnp.floor(rank * (1.0 / 256.0))
    rank_lo = jnp.where(any_own, rank - 256.0 * rank_hi, -1.0)
    rank_hi = jnp.where(any_own, rank_hi, -1.0)

    hot_slot = jnp.where(jnp.broadcast_to(rank_lo, (256, 3072)) == iota((256, 3072), 0).astype(F32), 1.0, 0.0).astype(BF16)
    hi_mask = jnp.broadcast_to(rank_hi, (8, 3072)) == iota((8, 3072), 0).astype(F32)
    outs = []
    for c in range(3):
        outs += list(split3(q_ref[c, 4:28, :]))
    for c in range(3):
        outs += list(split3(q_ref[3 + c, 4:28, :] + (0.5 * TIME_STEP) * force[c]))
    for c in range(3):
        outs += list(split3(force[c]))
    outs += [id_hi, id_lo, jnp.where(own, 1.0, 0.0)]
    lhs = jnp.concatenate([jnp.where(hi_mask, flat(x, 8), 0.0) for x in outs], axis=0).astype(BF16)
    slots = dot_split(lhs, hot_slot, true)

    def field(i):
        return slots[8 * i:8 * i + 8, :]

    def put(ref, row, x):
        for h in range(7):
            n = 256 if h < 6 else CAP - 1536
            ref[row:row + 1, 256 * h:256 * h + n] = x[h:h + 1, 0:n].astype(ref.dtype)

    for c in range(3):
        put(opos_ref, c, field(3 * c) + field(3 * c + 1) + field(3 * c + 2))
        put(ovel_ref, c, field(9 + 3 * c) + field(10 + 3 * c) + field(11 + 3 * c))
        put(ofrc_ref, c, field(18 + 3 * c) + field(19 + 3 * c) + field(20 + 3 * c))
    put(oid_ref, 0, field(27) * 128.0 + field(28))
    put(oval_ref, 0, field(29))

    for copy in (pos_all[2], vel_all[2], energy_all):
        copy.wait_send()
    energy_all.wait_recv()
    acc = ebuf[0]
    for k in range(1, 8):
        acc = acc + ebuf[k]
    oen_ref[...] = acc


def finish(pos_ref, vel_ref, frc_ref, id_ref, val_ref, en_ref, opos_ref, ovel_ref, ofrc_ref, oid_ref, oval_ref, oen_ref):
    opos_ref[...] = pos_ref[...]
    ovel_ref[...] = vel_ref[...]
    ofrc_ref[...] = frc_ref[...]
    oid_ref[...] = id_ref[...].reshape(CAP)
    oval_ref[...] = val_ref[...].reshape(CAP)
    oen_ref[...] = jnp.sum(jnp.sum(en_ref[...], axis=0, keepdims=True), axis=1, keepdims=True)


def solution(mesh):
    row_spec = P(BRICK_AXES, None)
    flat_spec = P(BRICK_AXES)
    vmem = pl.BlockSpec(memory_space=pltpu.VMEM)

    def local_step(pos, vel, frc, ids, valid):
        f3 = jax.ShapeDtypeStruct((3, CAP), F32)
        i1 = jax.ShapeDtypeStruct((CAP,), jnp.int32)
        outs = pl.pallas_call(
            kernel,
            out_shape=(pltpu.VMEM((3, CAP), F32),) * 3 + (pltpu.VMEM((1, CAP), jnp.int32),) * 2 + (pltpu.VMEM((8, 128), F32),),
            in_specs=[pl.BlockSpec(memory_space=pltpu.HBM)] * 5,
            out_specs=(vmem,) * 6,
            scratch_shapes=[pltpu.VMEM((offsets_of(pos_arrays)[1], 128), F32), pltpu.VMEM((offsets_of(pos_arrays)[1] + 16, 128), F32)] + [pltpu.VMEM((offsets_of(vel_arrays)[1], 128), F32)] * 2 + [
                pltpu.VMEM((3, CAP), F32),
                pltpu.VMEM((3, CAP), F32),
                pltpu.VMEM((3, CAP), F32),
                pltpu.VMEM((CAP,), jnp.int32),
                pltpu.VMEM((CAP,), jnp.int32),
                pltpu.SemaphoreType.DMA((5,)),
                pltpu.VMEM((56, KPAD), F32),
                pltpu.VMEM((2, 168, 128), F32),
                pltpu.VMEM((75, 32, 128), F32),
                pltpu.VMEM((NF, 32, 128), F32),
                pltpu.VMEM((8, 24, 128), F32),
                pltpu.VMEM((8, 8, 128), F32),
                pltpu.SemaphoreType.DMA,
                pltpu.SemaphoreType.DMA,
                pltpu.SemaphoreType.DMA,
                pltpu.SemaphoreType.DMA,
                pltpu.SemaphoreType.DMA,
                pltpu.SemaphoreType.DMA,
                pltpu.SemaphoreType.DMA,
            ],
            compiler_params=pltpu.CompilerParams(collective_id=0, has_side_effects=True),
        )(pos.T, vel.T, frc.T, ids, valid)
        outs = pl.pallas_call(
            finish,
            out_shape=(f3, f3, f3, i1, i1, jax.ShapeDtypeStruct((1, 1), F32)),
            in_specs=[vmem] * 6,
            out_specs=(vmem,) * 6,
            compiler_params=pltpu.CompilerParams(vmem_limit_bytes=4 << 20),
        )(*outs)
        return outs[0].T, outs[1].T, outs[2].T, outs[3], outs[4], outs[5][0, 0]

    return jax.shard_map(local_step, mesh=mesh, in_specs=(row_spec, row_spec, row_spec, flat_spec, flat_spec), out_specs=(row_spec, row_spec, row_spec, flat_spec, flat_spec, P()), check_vma=False)
```

```python
import functools

import jax
import jax.numpy as jnp
from jax import lax
from jax.experimental import pallas as pl
from jax.experimental.pallas import tpu as pltpu
from jax.sharding import PartitionSpec as P

TIME_STEP = 0.005
RCUT = 2.5
DENSITY = 0.8442
SPACING = (1.0 / DENSITY) ** (1.0 / 3.0)
SITES = 12
BRICK = SITES * SPACING
BOX = 2.0 * BRICK
BRICK_AXES = ("bz", "by", "bx")
CAP = SITES ** 3
KPAD = 1792
MESH_ID = pl.DeviceIdType.MESH
F32 = jnp.float32
BF16 = jnp.bfloat16
CUT6 = RCUT ** -6
U_CUT = 4.0 * (CUT6 * CUT6 - CUT6)
DU_CUT = (-48.0 * CUT6 * CUT6 + 24.0 * CUT6) / RCUT
DELTAS = [(d >> 2 & 1, d >> 1 & 1, d & 1) for d in range(1, 8)]
SEND_ORDER = [(1, 1, 0), (1, 1, 1), (0, 1, 0), (1, 0, 0), (0, 1, 1), (1, 0, 1), (0, 0, 1)]
POS_ORDER = [(1, 1, 0), (0, 1, 0), (1, 1, 1), (0, 1, 1), (1, 0, 0), (1, 0, 1), (0, 0, 1)]
SHIFTS = [(dx, dy) for dy in range(-2, 3) for dx in range(-2, 3)]
NF = 7


def iota(shape, dim):
    return lax.broadcasted_iota(jnp.int32, shape, dim)


def split3(x):
    hi = x.astype(BF16).astype(F32)
    rest = x - hi
    mid = rest.astype(BF16).astype(F32)
    return hi, mid, rest - mid


def dot_nt(a, b):
    return lax.dot_general(a, b, (((1,), (1,)), ((), ())), preferred_element_type=F32)


def dot_split(a, b, true):
    cut = a.shape[1] // 512 * 256
    return dot_nt(a[:, :cut], b[:, :cut]) + jnp.where(true, dot_nt(a[:, cut:], b[:, cut:]), 0.0)


def dot_nn(a, b):
    return lax.dot_general(a, b, (((1,), (0,)), ((), ())), preferred_element_type=F32)


def tile_of(delta):
    return 8 if delta[0] else 16, 128 if delta[1] else 256


def pos_arrays(delta):
    return 3


def vel_arrays(delta):
    return 1 if delta[0] or delta[1] else 4


def offsets_of(arrays):
    starts, row = {}, 0
    for delta in DELTAS:
        starts[delta] = row
        row += part_rows(arrays, delta)
    return starts, row


def part_rows(arrays, delta):
    rz, lanes = tile_of(delta)
    if arrays is pos_arrays:
        rz = 6 if delta[0] else 8 if delta == (0, 1, 1) else 14
    return arrays(delta) * rz * lanes // 128


def to_delta(g_ref, f, delta):
    dz, dy, dx = delta
    first = 24 * f + 4
    halves = []
    for h in range(2):
        if dz:
            halves.append(jnp.where(iota((8, 128), 0) < 4, g_ref[h, first + 12:first + 20, :], g_ref[h, first + 4:first + 12, :]))
        else:
            halves.append(g_ref[h, first:first + 16, :])
    lane = iota(halves[0].shape, 1)
    xf = lane & 15

    def along_x(x, turn):
        if not dx:
            return pltpu.roll(x, turn, 1) if turn else x
        return jnp.where(xf < 3, pltpu.roll(x, (turn + 116) % 128, 1), jnp.where(xf >= 13, pltpu.roll(x, turn + 12, 1), 0.0))

    if dy:
        group = lane >> 4
        return [jnp.where((group == 4) | (group == 5), along_x(halves[0], 64), jnp.where((group == 1) | (group == 2), 0.0, along_x(halves[1], 64)))]
    return [along_x(x, 0) for x in halves]


def folded(g_ref, f):
    first = 24 * f + 4
    row, moved = iota((8, 128), 0), (iota((8, 128), 1) - 6) & 127
    xf, group = moved & 15, moved >> 4
    outer = [jnp.where(row < 3, g_ref[h, first + 8:first + 16, :], g_ref[h, first + 10:first + 18, :]) for h in range(2)]

    def along_x(x):
        return jnp.where(xf < 3, pltpu.roll(x, 58, 1), jnp.where(xf >= 13, pltpu.roll(x, 82, 1), 0.0))

    out = jnp.where((group == 4) | (group == 5), along_x(outer[0]), jnp.where((group == 1) | (group == 2), 0.0, along_x(outer[1])))
    return to_delta(g_ref, f, (0, 1, 1))[0][0:8] + jnp.where(row < 6, out, 0.0)


def wide(b):
    lane = iota(b.shape, 1)
    return [jnp.where(lane < 16, b, 0.0), jnp.where(lane >= 48, b, 0.0)]


def same(f, delta):
    return f


def pack_vel(f, delta):
    dz, dy, _ = delta
    if dz:
        row = iota(f[0][0].shape, 0)
        outs = []
        for j in range(len(f[0])):
            out = jnp.zeros_like(f[0][j])
            for k in range(4):
                out = jnp.where(row == 2 * k, jnp.broadcast_to(f[k][j][6:7], out.shape), out)
                out = jnp.where(row == 2 * k + 1, jnp.broadcast_to(f[k][j][1:2], out.shape), out)
            outs.append(out)
        return [outs]
    if dy:
        f = [x[0] for x in f]
        group = iota(f[0].shape, 1) >> 4
        out = jnp.where((group == 0) | (group == 3), f[0], 0.0)
        out = jnp.where((group == 1) | (group == 4), pltpu.roll(f[1], 16, 1), out)
        out = jnp.where((group == 2) | (group == 5), pltpu.roll(f[2], 32, 1), out)
        out = jnp.where(group == 6, pltpu.roll(f[3], 96, 1), out)
        return [[jnp.where(group == 7, pltpu.roll(f[3], 64, 1), out)]]
    return f


def unpack_vel(a, delta):
    dz, dy, _ = delta
    if dz:
        row = iota(a[0][0].shape, 0)
        return [[jnp.where(row == 6, jnp.broadcast_to(x[2 * k:2 * k + 1], x.shape), jnp.where(row == 1, jnp.broadcast_to(x[2 * k + 1:2 * k + 2], x.shape), 0.0)) for x in a[0]] for k in range(4)]
    if dy:
        x = a[0][0]
        group = iota(x.shape, 1) >> 4
        low, high = group == 0, group == 3
        both = low | high
        last = jnp.where(low, pltpu.roll(x, 32, 1), jnp.where(high, pltpu.roll(x, 64, 1), 0.0))
        return [[jnp.where(both, x, 0.0)], [jnp.where(both, pltpu.roll(x, 112, 1), 0.0)], [jnp.where(both, pltpu.roll(x, 96, 1), 0.0)], [last]]
    return a


def merge_level(own, parts):
    near = wide(parts[(0, 1, 0)][0] + parts[(0, 1, 1)][0])
    return [own[h] + parts[(0, 0, 1)][h] + near[h] for h in range(2)]


def merge_above(own, parts):
    far = wide(parts[(1, 1, 0)][0] + parts[(1, 1, 1)][0])
    return [own[h] + parts[(1, 0, 0)][h] + parts[(1, 0, 1)][h] + far[h] for h in range(2)]


def kernel(pos_hbm, vel_hbm, frc_hbm, id_hbm, val_hbm, opos_ref, ovel_ref, ofrc_ref, oid_ref, oval_ref, oen_ref, *scratch):
    send_ref, precv, vrecv, in_ref, id_ref, val_ref, in_sem, atom_ref, g_ref, t_ref, q_ref, p_ref, ebuf, send_sem, precv_sem, pabove_sem, vrecv_sem, erecv_sem = scratch
    pos_rows, vel_rows = offsets_of(pos_arrays)[1], offsets_of(vel_arrays)[1]
    psend, vsend = send_ref.at[pl.ds(0, pos_rows)], send_ref.at[pl.ds(pos_rows, vel_rows)]
    vel_ref, frc_ref, pos_ref = (in_ref.at[k] for k in range(3))
    bz, by, bx = lax.axis_index("bz"), lax.axis_index("by"), lax.axis_index("bx")

    true = bz >= 0

    def partner(delta):
        return (lax.rem(bz + delta[0], 2), lax.rem(by + delta[1], 2), lax.rem(bx + delta[2], 2))

    barrier = pltpu.get_barrier_semaphore()
    for delta in SEND_ORDER:
        pl.semaphore_signal(barrier, inc=1, device_id=partner(delta), device_id_type=MESH_ID)

    loads = [pltpu.make_async_copy(src, dst, in_sem.at[max(i - 2, 0)]) for i, (src, dst) in enumerate(((vel_hbm, vel_ref), (frc_hbm, frc_ref), (pos_hbm, pos_ref), (val_hbm, val_ref), (id_hbm, id_ref)))]
    for copy in loads:
        copy.start()
    for f in range(NF):
        for h in range(2):
            g_ref[h, 24 * f:24 * f + 4, :] = jnp.zeros((4, 128), F32)
            g_ref[h, 24 * f + 20:24 * f + 24, :] = jnp.zeros((4, 128), F32)

    for copy in [pltpu.make_async_copy(in_ref, in_ref, in_sem.at[0])] + loads[3:]:
        copy.wait()
    v_half = vel_ref[...] + (0.5 * TIME_STEP) * frc_ref[...]
    moved = pos_ref[...] + TIME_STEP * v_half
    moved = moved - BOX * jnp.floor(moved * (1.0 / BOX))
    axis_row = iota((3, 1), 0)
    coord = jnp.where(axis_row == 0, bx, jnp.where(axis_row == 1, by, bz)).astype(F32)
    brick_lo = coord * BRICK
    rel = moved - brick_lo
    rel = jnp.where(rel < -0.5 * BRICK, rel + BOX, jnp.where(rel >= 1.5 * BRICK, rel - BOX, rel))
    cell = jnp.floor(rel * (1.0 / SPACING)).astype(jnp.int32) + 2
    live = val_ref[...].reshape(1, CAP) == 1
    ids = id_ref[...].reshape(1, CAP)
    atom_ref[:, pl.ds(KPAD - 128, 128)] = jnp.zeros((atom_ref.shape[0], 128), F32)
    zi = jnp.where(live, (cell[2:3, :] - 4) & 15, 0)
    lo = jnp.where(live, ((cell[1:2, :] - 2) & 15) * 16 + cell[0:1, :], 0)
    rows = list(split3(moved)) + list(split3(v_half))
    for k in range(6):
        atom_ref[8 * k:8 * k + 3, 0:CAP] = rows[k]
    atom_ref[48:49, 0:CAP] = (ids >> 7).astype(F32)
    atom_ref[49:50, 0:CAP] = (ids & 127).astype(F32)
    atom_ref[50:51, 0:CAP] = zi.astype(F32)
    atom_ref[51:52, 0:CAP] = lo.astype(F32)

    zrow = atom_ref[50:51, :]
    lrow = atom_ref[51:52, :]
    zmask = jnp.broadcast_to(zrow, (16, KPAD)) == iota((16, KPAD), 0).astype(F32)
    onehot = jnp.where(jnp.broadcast_to(lrow, (256, KPAD)) == iota((256, KPAD), 0).astype(F32), 1.0, 0.0).astype(BF16)

    def spread(row_idx):
        return jnp.where(zmask, jnp.broadcast_to(atom_ref[row_idx:row_idx + 1, :], (16, KPAD)), 0.0).astype(BF16)

    def exchange(src, dst, ssem, rsem, arrays):
        starts, total = offsets_of(arrays)
        shift = 8 if arrays is pos_arrays else 0
        cut = starts[(1, 0, 0)]
        for delta in POS_ORDER:
            rz, lanes = tile_of(delta)
            part = pl.ds(starts[delta], part_rows(arrays, delta))
            pltpu.make_async_remote_copy(src_ref=src.at[part], dst_ref=dst.at[pl.ds(starts[delta] + shift, part_rows(arrays, delta))], send_sem=ssem, recv_sem=rsem[delta[0]], device_id=partner(delta), device_id_type=MESH_ID).start()
        return [pltpu.make_async_remote_copy(src_ref=src.at[pl.ds(lo, hi - lo)], dst_ref=dst.at[pl.ds(shift + lo, hi - lo)], send_sem=ssem, recv_sem=sem, device_id=partner(DELTAS[0]), device_id_type=MESH_ID) for lo, hi, sem in ((0, cut, rsem[0]), (cut, total, rsem[1]), (0, total, rsem[0]))]

    def keep_own(f, x):
        for h in range(2):
            g_ref[h, 24 * f + 4:24 * f + 20, :] = x[:, 128 * h:128 * h + 128]

    def fill(buf, fields, pack, arrays):
        starts, _ = offsets_of(arrays)
        for delta in DELTAS:
            rz, lanes = tile_of(delta)
            row = starts[delta]
            if arrays is pos_arrays and delta == (0, 1, 1):
                for f in fields:
                    buf[row + 8 * f:row + 8 * f + 8, :] = folded(g_ref, f)
                continue
            for arr in pack([to_delta(g_ref, f, delta) for f in fields], delta):
                for piece in arr:
                    if arrays is not pos_arrays:
                        buf[row:row + rz, :] = piece
                        row += rz
                    elif delta[0]:
                        buf[row:row + 6, :] = piece[1:7]
                        row += 6
                    else:
                        buf[row:row + 11, :] = piece[0:11]
                        buf[row + 11:row + 14, :] = piece[13:16]
                        row += 14

    def own_rows(f, start, count):
        return [g_ref[h, 24 * f + 4 + start:24 * f + 4 + start + count, :] for h in range(2)]

    def pos_parts(inner, deltas):
        starts, _ = offsets_of(pos_arrays)
        row8 = iota((8, 128), 0)
        parts = [{} for _ in range(3)]
        for delta in deltas:
            rows = 6 if delta[0] else 8 if delta == (0, 1, 1) else 14
            row = starts[delta] + 8
            for c in range(3):
                parts[c][delta] = []
                for _ in range(tile_of(delta)[1] // 128):
                    if delta[0]:
                        x = jnp.where((row8 >= 1) & (row8 < 7), precv[row - 1:row + 7, :], 0.0)
                    elif delta == (0, 1, 1):
                        xf = iota((8, 128), 1) & 15
                        x = precv[row:row + 8, :]
                        if not inner:
                            x = pltpu.roll(jnp.where(row8 < 3, x, precv[row - 2:row + 6, :]), 122, 1)
                        x = jnp.where(((xf < 3) | (xf >= 13)) & (inner | (row8 < 3) | (row8 >= 5)), x, 0.0)
                    elif inner:
                        x = precv[row:row + 8, :]
                    else:
                        x = jnp.where(row8 < 3, precv[row + 8:row + 16, :], jnp.where(row8 >= 5, precv[row + 6:row + 14, :], 0.0))
                    parts[c][delta].append(x)
                    row += rows
        return parts

    def vel_fields():
        starts, _ = offsets_of(vel_arrays)
        parts = {}
        for delta in DELTAS:
            rz, lanes = tile_of(delta)
            row = starts[delta]
            arrs = []
            for i in range(vel_arrays(delta)):
                arrs.append([vrecv[row + rz * j:row + rz * j + rz, :] for j in range(lanes // 128)])
                row += rz * lanes // 128
            parts[delta] = unpack_vel(arrs, delta)
        out = []
        for i in range(4):
            mine = {d: parts[d][i] for d in DELTAS}
            level = merge_level(own_rows(3 + i, 0, 16), mine)
            above = merge_above([x[8:16] for x in level], mine)
            out.append([[x[0:8] for x in level], above])
        return out

    lhs = jnp.concatenate([spread(8 * k + c) for k in range(3) for c in range(3)], axis=0)
    binned = dot_split(lhs, onehot, true)
    pos_own = [binned[16 * c:16 * c + 16] + binned[48 + 16 * c:64 + 16 * c] + binned[96 + 16 * c:112 + 16 * c] for c in range(3)]
    for c in range(3):
        keep_own(c, pos_own[c])
    fill(psend, range(3), same, pos_arrays)
    pl.semaphore_wait(barrier, 7)
    pos_all = exchange(psend, precv, send_sem, (precv_sem, pabove_sem), pos_arrays)

    lhs = jnp.concatenate([spread(8 * k + c) for k in range(3, 6) for c in range(3)] + [spread(48), spread(49)], axis=0)
    binned = dot_split(lhs, onehot, true)
    vel_own = [binned[16 * c:16 * c + 16] + binned[48 + 16 * c:64 + 16 * c] + binned[96 + 16 * c:112 + 16 * c] for c in range(3)]
    vel_own.append(binned[144:160] * 128.0 + binned[160:176])
    for c in range(4):
        keep_own(3 + c, vel_own[c])
    fill(vsend, range(3, 7), pack_vel, vel_arrays)
    vel_all = exchange(vsend, vrecv, send_sem, (vrecv_sem, vrecv_sem), vel_arrays)

    los = [bx, by, bz]

    def localise(fields, start):
        out = [[], [], []]
        for h in range(2):
            present = fields[0][h] != 0.0
            lane = iota((8, 128), 1) + 128 * h
            frame = [lane & 15, lane >> 4, iota((8, 128), 0) + start]
            for c in range(3):
                u = fields[c][h] - los[c].astype(F32) * BRICK
                u = jnp.where(u < -0.5 * BRICK, u + BOX, jnp.where(u >= 1.5 * BRICK, u - BOX, u))
                out[c].append(jnp.where(present, u, 64.0 + 4.0 * frame[c].astype(F32)))
        return out

    lane8 = iota((8, 128), 1)

    def put_rows(ref, k, h, x, inner):
        if inner:
            ref[k, pl.ds(8 + h, 8, stride=2), :] = x
        else:
            ref[k, pl.ds(24 + h, 4, stride=2), :] = x[0:4]
            ref[k, pl.ds(h, 4, stride=2), :] = x[4:8]

    def shift_in(s, local, inner):
        dx, dy = SHIFTS[s]
        left = 16 * dy + dx
        for c in range(3):
            a, b = local[c]
            if left:
                a, b = pltpu.roll(a, (-left) % 128, 1), pltpu.roll(b, (-left) % 128, 1)
                here = lane8 < 128 - left if left > 0 else lane8 >= -left
                a, b = jnp.where(here, a, b), jnp.where(here, b, a)
            put_rows(t_ref, 3 * s + c, 0, a, inner)
            put_rows(t_ref, 3 * s + c, 1, b, inner)

    def keep(f, inner_rows, outer_rows):
        for h in range(2):
            put_rows(q_ref, f, h, inner_rows[h], True)
            put_rows(q_ref, f, h, outer_rows[h], False)

    span = [4, 24]
    row8 = iota((8, 128), 0)

    def load(dx, dy, dz):
        s = SHIFTS.index((dx, dy))
        if span[0] is None:
            return [jnp.where(row8 < 4, t_ref[3 * s + c, 4 + 2 * dz:12 + 2 * dz, :], t_ref[3 * s + c, 20 + 2 * dz:28 + 2 * dz, :]) for c in range(3)]
        return [t_ref[3 * s + c, span[0] + 2 * dz:span[0] + 2 * dz + span[1], :] for c in range(3)]

    def low_x():
        return (iota((span[1], 128), 1) & 15) < 8

    def low_y():
        return ((iota((span[1], 128), 0) & 1) == 0) & (iota((span[1], 128), 1) < 96)

    def low_z():
        return row8 < 4 if span[0] is None else iota((span[1], 128), 0) + span[0] < 16

    def pick(mask, p, q):
        m = mask()
        return [jnp.where(m, p[c], q[c]) for c in range(3)]

    def half(dx, dy, dz):
        return dy > 0 or (dy == 0 and (dx > 0 or (dx == 0 and dz > 0)))

    offsets = [(dx, dy, dz) for dx, dy in SHIFTS for dz in range(-2, 3) if (dx, dy, dz) != (0, 0, 0) and (abs(dx) == 2) + (abs(dy) == 2) + (abs(dz) == 2) <= 1]
    first = [functools.partial(load, *d) for d in offsets if half(*d)]
    second = [functools.partial(load, *d) for d in offsets if not half(*d)]
    for dz in range(-1, 2):
        first.append(lambda dz=dz: pick(low_x, load(-2, 2, dz), load(2, 2, dz)))
        second.append(lambda dz=dz: pick(low_x, load(-2, -2, dz), load(2, -2, dz)))
    for dx in range(-1, 2):
        first.append(lambda dx=dx: pick(low_z, load(dx, 2, -2), load(dx, 2, 2)))
        second.append(lambda dx=dx: pick(low_z, load(dx, -2, -2), load(dx, -2, 2)))
    for dy in (1, -1):
        (first if dy == 1 else second).append(lambda dy=dy: pick(low_z, pick(low_x, load(-2, dy, -2), load(2, dy, -2)), pick(low_x, load(-2, dy, 2), load(2, dy, 2))))
    first.append(lambda: pick(low_z, load(2, 0, -2), load(2, 0, 2)))
    second.append(lambda: pick(low_z, load(-2, 0, -2), load(-2, 0, 2)))

    def apart(mine, nbr):
        ex, ey, ez = mine[0] - nbr[0], mine[1] - nbr[1], mine[2] - nbr[2]
        r2 = jnp.minimum(ex * ex + ey * ey + ez * ez, RCUT * RCUT)
        return ex, ey, ez, r2, lax.rsqrt(r2)

    def pair_energy(row):
        span[:] = [row, 8]
        mine = load(0, 0, 0)
        sw, sr = jnp.zeros((8, 128), F32), jnp.zeros((8, 128), F32)
        for i, nbr in enumerate(first):
            ex, ey, ez, r2, inv = apart(mine, nbr())
            i2 = inv * inv
            i6 = i2 * i2 * i2
            sw = sw + i6 * (i6 - 1.0)
            sr = sr + r2 * inv
        return 4.0 * sw - DU_CUT * sr + (RCUT * DU_CUT - U_CUT) * len(first)

    early = [s for s, (dx, dy) in enumerate(SHIFTS) if dy > 0 or (dy == 0 and dx >= 0)]
    late = [s for s in range(25) if s not in early]
    pos_all[0].wait_recv()
    parts = pos_parts(True, DELTAS[:3])
    inner = [merge_level(own_rows(c, 0, 8), parts[c]) for c in range(3)]
    inner_local = localise(inner, 0)
    for s in early:
        shift_in(s, inner_local, True)
    parts = pos_parts(False, DELTAS[:3])
    outer = [merge_level(own_rows(c, 8, 8), parts[c]) for c in range(3)]
    outer_local = localise(outer, 8)
    for s in early:
        shift_in(s, outer_local, False)
    middle = [pair_energy(8), pair_energy(16)]
    pos_all[1].wait_recv()
    parts = pos_parts(False, DELTAS[3:])
    outer = [merge_above(outer[c], parts[c]) for c in range(3)]
    outer_local = localise(outer, 8)
    for s in early:
        shift_in(s, outer_local, False)
    edges = pair_energy(None)
    span[:] = [4, 24]
    keep(0, inner[0], outer[0])
    lane24 = iota((24, 128), 1)
    x24 = lane24 & 15
    own = (((iota((24, 128), 0) & 1) == 0) | (lane24 < 64)) & (x24 >= 2) & (x24 < 14) & (q_ref[0, 4:28, :] != 0.0)
    energy = jnp.where(own, jnp.concatenate([edges[0:4]] + middle + [edges[4:8]], axis=0), 0.0)
    me = bz * 4 + by * 2 + bx
    ebuf[me, :, :] = energy[0:8] + energy[8:16] + energy[16:24]
    for delta in SEND_ORDER:
        pltpu.make_async_remote_copy(src_ref=ebuf.at[me], dst_ref=ebuf.at[me], send_sem=send_sem, recv_sem=erecv_sem, device_id=partner(delta), device_id_type=MESH_ID).start()
    energy_all = pltpu.make_async_remote_copy(src_ref=ebuf.at[pl.ds(0, 7)], dst_ref=ebuf.at[pl.ds(0, 7)], send_sem=send_sem, recv_sem=erecv_sem, device_id=partner(DELTAS[0]), device_id_type=MESH_ID)

    vel_all[2].wait_recv()
    for f, (a, b) in enumerate(vel_fields()):
        keep(3 + f, a, b)
    for c in range(1, 3):
        keep(c, inner[c], outer[c])

    for s in late:
        shift_in(s, inner_local, True)
        shift_in(s, outer_local, False)
    mine = load(0, 0, 0)

    def push(acc, ex, ey, ez, inv):
        i2 = inv * inv
        i6 = i2 * i2 * i2
        fr = (i6 * (i6 - 0.5)) * i2 + (DU_CUT / 48.0) * inv
        return (acc[0] + fr * ex, acc[1] + fr * ey, acc[2] + fr * ez)

    acc = tuple(jnp.zeros((24, 128), F32) for _ in range(3))
    for nbr in first + second:
        ex, ey, ez, r2, inv = apart(mine, nbr())
        acc = push(acc, ex, ey, ez, inv)
    force = [48.0 * acc[c] for c in range(3)]

    idv = jnp.where(own, q_ref[6, 4:28, :], -1.0)
    id_int = idv.astype(jnp.int32)
    id_hi = jnp.where(own, id_int >> 7, -1).astype(F32)
    id_lo = jnp.where(own, id_int & 127, -1).astype(F32)

    def flat(x, n):
        return jnp.concatenate([jnp.broadcast_to(x[r:r + 1, :], (n, 128)) for r in range(24)], axis=1)

    hot_hi = jnp.where(flat(id_hi, 128) == iota((128, 3072), 0).astype(F32), 1.0, 0.0).astype(BF16)
    lo_eq = flat(id_lo, 128) == iota((128, 3072), 0).astype(F32)
    hot_lo = jnp.where(lo_eq, 1.0, 0.0).astype(BF16)
    table = dot_split(hot_lo, hot_hi, true).astype(BF16)
    r128, c128 = iota((128, 128), 0), iota((128, 128), 1)
    below = dot_nn(jnp.where(c128 < r128, 1.0, 0.0).astype(BF16), table)
    total = dot_nn(jnp.ones((128, 128), BF16), table).astype(BF16)
    before = dot_nn(total, jnp.where(r128 < c128, 1.0, 0.0).astype(BF16))
    rank_tab = below + before
    tab_hi = jnp.floor(rank_tab * (1.0 / 256.0)) * 256.0
    tab_lo = rank_tab - tab_hi
    tabs = jnp.concatenate([tab_hi, tab_lo], axis=1).astype(BF16)
    hot2 = jnp.concatenate([hot_hi, hot_hi], axis=0)
    looked = jnp.concatenate([dot_nn(tabs, hot2[:, :1536]), dot_nn(tabs, hot2[:, 1536:])], axis=1)
    rank = jnp.sum(jnp.where(lo_eq, looked, 0.0), axis=0, keepdims=True)
    any_own = flat(jnp.where(own, 1.0, 0.0), 1) > 0.5
    rank_hi = jnp.floor(rank * (1.0 / 256.0))
    rank_lo = jnp.where(any_own, rank - 256.0 * rank_hi, -1.0)
    rank_hi = jnp.where(any_own, rank_hi, -1.0)

    hot_slot = jnp.where(jnp.broadcast_to(rank_lo, (256, 3072)) == iota((256, 3072), 0).astype(F32), 1.0, 0.0).astype(BF16)
    hi_mask = jnp.broadcast_to(rank_hi, (8, 3072)) == iota((8, 3072), 0).astype(F32)
    outs = []
    for c in range(3):
        outs += list(split3(q_ref[c, 4:28, :]))
    for c in range(3):
        outs += list(split3(q_ref[3 + c, 4:28, :] + (0.5 * TIME_STEP) * force[c]))
    for c in range(3):
        outs += list(split3(force[c]))
    outs += [id_hi, id_lo, jnp.where(own, 1.0, 0.0)]
    lhs = jnp.concatenate([jnp.where(hi_mask, flat(x, 8), 0.0) for x in outs], axis=0).astype(BF16)
    slots = dot_split(lhs, hot_slot, true)

    def field(i):
        return slots[8 * i:8 * i + 8, :]

    def put(ref, row, x):
        for h in range(7):
            n = 256 if h < 6 else CAP - 1536
            ref[row:row + 1, 256 * h:256 * h + n] = x[h:h + 1, 0:n].astype(ref.dtype)

    for c in range(3):
        put(opos_ref, c, field(3 * c) + field(3 * c + 1) + field(3 * c + 2))
        put(ovel_ref, c, field(9 + 3 * c) + field(10 + 3 * c) + field(11 + 3 * c))
        put(ofrc_ref, c, field(18 + 3 * c) + field(19 + 3 * c) + field(20 + 3 * c))
    put(oid_ref, 0, field(27) * 128.0 + field(28))
    put(oval_ref, 0, field(29))

    pltpu.make_async_remote_copy(src_ref=send_ref, dst_ref=send_ref, send_sem=send_sem, recv_sem=precv_sem, device_id=partner(DELTAS[0]), device_id_type=MESH_ID).wait_send()
    energy_all.wait_recv()
    acc = ebuf[0]
    for k in range(1, 8):
        acc = acc + ebuf[k]
    oen_ref[...] = acc


def finish(pos_ref, vel_ref, frc_ref, id_ref, val_ref, en_ref, opos_ref, ovel_ref, ofrc_ref, oid_ref, oval_ref, oen_ref):
    opos_ref[...] = pos_ref[...]
    ovel_ref[...] = vel_ref[...]
    ofrc_ref[...] = frc_ref[...]
    oid_ref[...] = id_ref[...].reshape(CAP)
    oval_ref[...] = val_ref[...].reshape(CAP)
    oen_ref[...] = jnp.sum(jnp.sum(en_ref[...], axis=0, keepdims=True), axis=1, keepdims=True)


def solution(mesh):
    row_spec = P(BRICK_AXES, None)
    flat_spec = P(BRICK_AXES)
    vmem = pl.BlockSpec(memory_space=pltpu.VMEM)

    def local_step(pos, vel, frc, ids, valid):
        f3 = jax.ShapeDtypeStruct((3, CAP), F32)
        i1 = jax.ShapeDtypeStruct((CAP,), jnp.int32)
        outs = pl.pallas_call(
            kernel,
            out_shape=(pltpu.VMEM((3, CAP), F32),) * 3 + (pltpu.VMEM((1, CAP), jnp.int32),) * 2 + (pltpu.VMEM((8, 128), F32),),
            in_specs=[pl.BlockSpec(memory_space=pltpu.HBM)] * 5,
            out_specs=(vmem,) * 6,
            scratch_shapes=[pltpu.VMEM((offsets_of(pos_arrays)[1] + offsets_of(vel_arrays)[1] + 56, 128), F32), pltpu.VMEM((offsets_of(pos_arrays)[1] + 16, 128), F32), pltpu.VMEM((offsets_of(vel_arrays)[1], 128), F32)] + [
                pltpu.VMEM((3, 3, CAP), F32),
                pltpu.VMEM((CAP,), jnp.int32),
                pltpu.VMEM((CAP,), jnp.int32),
                pltpu.SemaphoreType.DMA((3,)),
                pltpu.VMEM((56, KPAD), F32),
                pltpu.VMEM((2, 168, 128), F32),
                pltpu.VMEM((75, 32, 128), F32),
                pltpu.VMEM((NF, 32, 128), F32),
                pltpu.VMEM((8, 24, 128), F32),
                pltpu.VMEM((8, 8, 128), F32),
                pltpu.SemaphoreType.DMA,
                pltpu.SemaphoreType.DMA,
                pltpu.SemaphoreType.DMA,
                pltpu.SemaphoreType.DMA,
                pltpu.SemaphoreType.DMA,
            ],
            compiler_params=pltpu.CompilerParams(collective_id=0, has_side_effects=True),
        )(pos.T, vel.T, frc.T, ids, valid)
        outs = pl.pallas_call(
            finish,
            out_shape=(f3, f3, f3, i1, i1, jax.ShapeDtypeStruct((1, 1), F32)),
            in_specs=[vmem] * 6,
            out_specs=(vmem,) * 6,
            compiler_params=pltpu.CompilerParams(vmem_limit_bytes=4 << 20),
        )(*outs)
        return outs[0].T, outs[1].T, outs[2].T, outs[3], outs[4], outs[5][0, 0]

    return jax.shard_map(local_step, mesh=mesh, in_specs=(row_spec, row_spec, row_spec, flat_spec, flat_spec), out_specs=(row_spec, row_spec, row_spec, flat_spec, flat_spec, P()), check_vma=False)
```

```python
import functools

import jax
import jax.numpy as jnp
from jax import lax
from jax.experimental import pallas as pl
from jax.experimental.pallas import tpu as pltpu
from jax.sharding import PartitionSpec as P

TIME_STEP = 0.005
RCUT = 2.5
DENSITY = 0.8442
SPACING = (1.0 / DENSITY) ** (1.0 / 3.0)
SITES = 12
BRICK = SITES * SPACING
BOX = 2.0 * BRICK
BRICK_AXES = ("bz", "by", "bx")
CAP = SITES ** 3
KPAD = 1792
MESH_ID = pl.DeviceIdType.MESH
F32 = jnp.float32
BF16 = jnp.bfloat16
CUT6 = RCUT ** -6
U_CUT = 4.0 * (CUT6 * CUT6 - CUT6)
DU_CUT = (-48.0 * CUT6 * CUT6 + 24.0 * CUT6) / RCUT
DELTAS = [(d >> 2 & 1, d >> 1 & 1, d & 1) for d in range(1, 8)]
SEND_ORDER = [(1, 1, 0), (1, 1, 1), (0, 1, 0), (1, 0, 0), (0, 1, 1), (1, 0, 1), (0, 0, 1)]
POS_ORDER = [(1, 1, 0), (0, 1, 0), (1, 1, 1), (0, 1, 1), (1, 0, 0), (1, 0, 1), (0, 0, 1)]
SHIFTS = [(dx, dy) for dy in range(-2, 3) for dx in range(-2, 3)]
NF = 7


def iota(shape, dim):
    return lax.broadcasted_iota(jnp.int32, shape, dim)


def split3(x):
    hi = x.astype(BF16).astype(F32)
    rest = x - hi
    mid = rest.astype(BF16).astype(F32)
    return hi, mid, rest - mid


def dot_nt(a, b):
    return lax.dot_general(a, b, (((1,), (1,)), ((), ())), preferred_element_type=F32)


def dot_split(a, b, true):
    cut = a.shape[1] // 512 * 256
    return dot_nt(a[:, :cut], b[:, :cut]) + jnp.where(true, dot_nt(a[:, cut:], b[:, cut:]), 0.0)


def dot_nn(a, b):
    return lax.dot_general(a, b, (((1,), (0,)), ((), ())), preferred_element_type=F32)


def tile_of(delta):
    return 8 if delta[0] else 16, 128 if delta[1] else 256


def pos_arrays(delta):
    return 3


def vel_arrays(delta):
    return 1 if delta[0] or delta[1] else 4


def offsets_of(arrays):
    starts, row = {}, 0
    for delta in DELTAS:
        starts[delta] = row
        row += part_rows(arrays, delta)
    return starts, row


def part_rows(arrays, delta):
    rz, lanes = tile_of(delta)
    if arrays is pos_arrays:
        rz = 6 if delta[0] else 8 if delta == (0, 1, 1) else 14
    return arrays(delta) * rz * lanes // 128


def to_delta(g_ref, f, delta):
    dz, dy, dx = delta
    first = 24 * f + 4
    halves = []
    for h in range(2):
        if dz:
            halves.append(jnp.where(iota((8, 128), 0) < 4, g_ref[h, first + 12:first + 20, :], g_ref[h, first + 4:first + 12, :]))
        else:
            halves.append(g_ref[h, first:first + 16, :])
    lane = iota(halves[0].shape, 1)
    xf = lane & 15

    def along_x(x, turn):
        if not dx:
            return pltpu.roll(x, turn, 1) if turn else x
        return jnp.where(xf < 3, pltpu.roll(x, (turn + 116) % 128, 1), jnp.where(xf >= 13, pltpu.roll(x, turn + 12, 1), 0.0))

    if dy:
        group = lane >> 4
        return [jnp.where((group == 4) | (group == 5), along_x(halves[0], 64), jnp.where((group == 1) | (group == 2), 0.0, along_x(halves[1], 64)))]
    return [along_x(x, 0) for x in halves]


def folded(g_ref, f):
    first = 24 * f + 4
    row, moved = iota((8, 128), 0), (iota((8, 128), 1) - 6) & 127
    xf, group = moved & 15, moved >> 4
    outer = [jnp.where(row < 3, g_ref[h, first + 8:first + 16, :], g_ref[h, first + 10:first + 18, :]) for h in range(2)]

    def along_x(x):
        return jnp.where(xf < 3, pltpu.roll(x, 58, 1), jnp.where(xf >= 13, pltpu.roll(x, 82, 1), 0.0))

    out = jnp.where((group == 4) | (group == 5), along_x(outer[0]), jnp.where((group == 1) | (group == 2), 0.0, along_x(outer[1])))
    return to_delta(g_ref, f, (0, 1, 1))[0][0:8] + jnp.where(row < 6, out, 0.0)


def wide(b):
    lane = iota(b.shape, 1)
    return [jnp.where(lane < 16, b, 0.0), jnp.where(lane >= 48, b, 0.0)]


def same(f, delta):
    return f


def pack_vel(f, delta):
    dz, dy, _ = delta
    if dz:
        row = iota(f[0][0].shape, 0)
        outs = []
        for j in range(len(f[0])):
            out = jnp.zeros_like(f[0][j])
            for k in range(4):
                out = jnp.where(row == 2 * k, jnp.broadcast_to(f[k][j][6:7], out.shape), out)
                out = jnp.where(row == 2 * k + 1, jnp.broadcast_to(f[k][j][1:2], out.shape), out)
            outs.append(out)
        return [outs]
    if dy:
        f = [x[0] for x in f]
        group = iota(f[0].shape, 1) >> 4
        out = jnp.where((group == 0) | (group == 3), f[0], 0.0)
        out = jnp.where((group == 1) | (group == 4), pltpu.roll(f[1], 16, 1), out)
        out = jnp.where((group == 2) | (group == 5), pltpu.roll(f[2], 32, 1), out)
        out = jnp.where(group == 6, pltpu.roll(f[3], 96, 1), out)
        return [[jnp.where(group == 7, pltpu.roll(f[3], 64, 1), out)]]
    return f


def unpack_vel(a, delta):
    dz, dy, _ = delta
    if dz:
        row = iota(a[0][0].shape, 0)
        return [[jnp.where(row == 6, jnp.broadcast_to(x[2 * k:2 * k + 1], x.shape), jnp.where(row == 1, jnp.broadcast_to(x[2 * k + 1:2 * k + 2], x.shape), 0.0)) for x in a[0]] for k in range(4)]
    if dy:
        x = a[0][0]
        group = iota(x.shape, 1) >> 4
        low, high = group == 0, group == 3
        both = low | high
        last = jnp.where(low, pltpu.roll(x, 32, 1), jnp.where(high, pltpu.roll(x, 64, 1), 0.0))
        return [[jnp.where(both, x, 0.0)], [jnp.where(both, pltpu.roll(x, 112, 1), 0.0)], [jnp.where(both, pltpu.roll(x, 96, 1), 0.0)], [last]]
    return a


def merge_level(own, parts):
    near = wide(parts[(0, 1, 0)][0] + parts[(0, 1, 1)][0])
    return [own[h] + parts[(0, 0, 1)][h] + near[h] for h in range(2)]


def merge_above(own, parts):
    far = wide(parts[(1, 1, 0)][0] + parts[(1, 1, 1)][0])
    return [own[h] + parts[(1, 0, 0)][h] + parts[(1, 0, 1)][h] + far[h] for h in range(2)]


def kernel(pos_hbm, vel_hbm, frc_hbm, id_hbm, val_hbm, opos_ref, ovel_ref, ofrc_ref, oid_ref, oval_ref, oen_ref, *scratch):
    send_ref, precv, vrecv, in_ref, id_ref, val_ref, in_sem, atom_ref, g_ref, t_ref, q_ref, p_ref, ebuf, send_sem, precv_sem, pabove_sem, vrecv_sem, erecv_sem = scratch
    pos_rows, vel_rows = offsets_of(pos_arrays)[1], offsets_of(vel_arrays)[1]
    psend, vsend = send_ref.at[pl.ds(0, pos_rows)], send_ref.at[pl.ds(pos_rows, vel_rows)]
    vel_ref, frc_ref, pos_ref = (in_ref.at[k] for k in range(3))
    bz, by, bx = lax.axis_index("bz"), lax.axis_index("by"), lax.axis_index("bx")

    true = bz >= 0

    def partner(delta):
        return (lax.rem(bz + delta[0], 2), lax.rem(by + delta[1], 2), lax.rem(bx + delta[2], 2))

    barrier = pltpu.get_barrier_semaphore()
    for delta in SEND_ORDER:
        pl.semaphore_signal(barrier, inc=1, device_id=partner(delta), device_id_type=MESH_ID)

    loads = [pltpu.make_async_copy(src, dst, in_sem.at[max(i - 2, 0)]) for i, (src, dst) in enumerate(((vel_hbm, vel_ref), (frc_hbm, frc_ref), (pos_hbm, pos_ref), (val_hbm, val_ref), (id_hbm, id_ref)))]
    for copy in loads:
        copy.start()
    for copy in [pltpu.make_async_copy(in_ref, in_ref, in_sem.at[0])] + loads[3:]:
        copy.wait()
    v_half = vel_ref[...] + (0.5 * TIME_STEP) * frc_ref[...]
    moved = pos_ref[...] + TIME_STEP * v_half
    moved = moved - BOX * jnp.floor(moved * (1.0 / BOX))
    axis_row = iota((3, 1), 0)
    coord = jnp.where(axis_row == 0, bx, jnp.where(axis_row == 1, by, bz)).astype(F32)
    brick_lo = coord * BRICK
    rel = moved - brick_lo
    rel = jnp.where(rel < -0.5 * BRICK, rel + BOX, jnp.where(rel >= 1.5 * BRICK, rel - BOX, rel))
    cell = jnp.floor(rel * (1.0 / SPACING)).astype(jnp.int32) + 2
    live = val_ref[...].reshape(1, CAP) == 1
    ids = id_ref[...].reshape(1, CAP)
    atom_ref[:, pl.ds(KPAD - 128, 128)] = jnp.zeros((atom_ref.shape[0], 128), F32)
    for f in range(NF):
        for h in range(2):
            g_ref[h, 24 * f:24 * f + 4, :] = jnp.zeros((4, 128), F32)
            g_ref[h, 24 * f + 20:24 * f + 24, :] = jnp.zeros((4, 128), F32)
    zi = jnp.where(live, (cell[2:3, :] - 4) & 15, 0)
    lo = jnp.where(live, ((cell[1:2, :] - 2) & 15) * 16 + cell[0:1, :], 0)
    rows = list(split3(moved)) + list(split3(v_half))
    for k in range(6):
        atom_ref[8 * k:8 * k + 3, 0:CAP] = rows[k]
    atom_ref[48:49, 0:CAP] = (ids >> 7).astype(F32)
    atom_ref[49:50, 0:CAP] = (ids & 127).astype(F32)
    atom_ref[50:51, 0:CAP] = zi.astype(F32)
    atom_ref[51:52, 0:CAP] = lo.astype(F32)

    zrow = atom_ref[50:51, :]
    lrow = atom_ref[51:52, :]
    zmask = jnp.broadcast_to(zrow, (16, KPAD)) == iota((16, KPAD), 0).astype(F32)
    onehot = jnp.where(jnp.broadcast_to(lrow, (256, KPAD)) == iota((256, KPAD), 0).astype(F32), 1.0, 0.0).astype(BF16)

    def spread(row_idx):
        return jnp.where(zmask, jnp.broadcast_to(atom_ref[row_idx:row_idx + 1, :], (16, KPAD)), 0.0).astype(BF16)

    def exchange(src, dst, ssem, rsem, arrays):
        starts, total = offsets_of(arrays)
        shift = 8 if arrays is pos_arrays else 0
        cut = starts[(1, 0, 0)]
        for delta in POS_ORDER:
            rz, lanes = tile_of(delta)
            part = pl.ds(starts[delta], part_rows(arrays, delta))
            pltpu.make_async_remote_copy(src_ref=src.at[part], dst_ref=dst.at[pl.ds(starts[delta] + shift, part_rows(arrays, delta))], send_sem=ssem, recv_sem=rsem[delta[0]], device_id=partner(delta), device_id_type=MESH_ID).start()
        return [pltpu.make_async_remote_copy(src_ref=src.at[pl.ds(lo, hi - lo)], dst_ref=dst.at[pl.ds(shift + lo, hi - lo)], send_sem=ssem, recv_sem=sem, device_id=partner(DELTAS[0]), device_id_type=MESH_ID) for lo, hi, sem in ((0, cut, rsem[0]), (cut, total, rsem[1]), (0, total, rsem[0]))]

    def keep_own(f, x):
        for h in range(2):
            g_ref[h, 24 * f + 4:24 * f + 20, :] = x[:, 128 * h:128 * h + 128]

    def fill(buf, fields, pack, arrays):
        starts, _ = offsets_of(arrays)
        for delta in DELTAS:
            rz, lanes = tile_of(delta)
            row = starts[delta]
            if arrays is pos_arrays and delta == (0, 1, 1):
                for f in fields:
                    buf[row + 8 * f:row + 8 * f + 8, :] = folded(g_ref, f)
                continue
            for arr in pack([to_delta(g_ref, f, delta) for f in fields], delta):
                for piece in arr:
                    if arrays is not pos_arrays:
                        buf[row:row + rz, :] = piece
                        row += rz
                    elif delta[0]:
                        buf[row:row + 6, :] = piece[1:7]
                        row += 6
                    else:
                        buf[row:row + 11, :] = piece[0:11]
                        buf[row + 11:row + 14, :] = piece[13:16]
                        row += 14

    def own_rows(f, start, count):
        return [g_ref[h, 24 * f + 4 + start:24 * f + 4 + start + count, :] for h in range(2)]

    def pos_parts(inner, deltas):
        starts, _ = offsets_of(pos_arrays)
        row8 = iota((8, 128), 0)
        parts = [{} for _ in range(3)]
        for delta in deltas:
            rows = 6 if delta[0] else 8 if delta == (0, 1, 1) else 14
            row = starts[delta] + 8
            for c in range(3):
                parts[c][delta] = []
                for _ in range(tile_of(delta)[1] // 128):
                    if delta[0]:
                        x = jnp.where((row8 >= 1) & (row8 < 7), precv[row - 1:row + 7, :], 0.0)
                    elif delta == (0, 1, 1):
                        xf = iota((8, 128), 1) & 15
                        x = precv[row:row + 8, :]
                        if not inner:
                            x = pltpu.roll(jnp.where(row8 < 3, x, precv[row - 2:row + 6, :]), 122, 1)
                        x = jnp.where(((xf < 3) | (xf >= 13)) & (inner | (row8 < 3) | (row8 >= 5)), x, 0.0)
                    elif inner:
                        x = precv[row:row + 8, :]
                    else:
                        x = jnp.where(row8 < 3, precv[row + 8:row + 16, :], jnp.where(row8 >= 5, precv[row + 6:row + 14, :], 0.0))
                    parts[c][delta].append(x)
                    row += rows
        return parts

    def vel_fields():
        starts, _ = offsets_of(vel_arrays)
        parts = {}
        for delta in DELTAS:
            rz, lanes = tile_of(delta)
            row = starts[delta]
            arrs = []
            for i in range(vel_arrays(delta)):
                arrs.append([vrecv[row + rz * j:row + rz * j + rz, :] for j in range(lanes // 128)])
                row += rz * lanes // 128
            parts[delta] = unpack_vel(arrs, delta)
        out = []
        for i in range(4):
            mine = {d: parts[d][i] for d in DELTAS}
            level = merge_level(own_rows(3 + i, 0, 16), mine)
            above = merge_above([x[8:16] for x in level], mine)
            out.append([[x[0:8] for x in level], above])
        return out

    lhs = jnp.concatenate([spread(8 * k + c) for k in range(3) for c in range(3)], axis=0)
    binned = dot_split(lhs, onehot, true)
    pos_own = [binned[16 * c:16 * c + 16] + binned[48 + 16 * c:64 + 16 * c] + binned[96 + 16 * c:112 + 16 * c] for c in range(3)]
    for c in range(3):
        keep_own(c, pos_own[c])
    fill(psend, range(3), same, pos_arrays)
    pl.semaphore_wait(barrier, 7)
    pos_all = exchange(psend, precv, send_sem, (precv_sem, pabove_sem), pos_arrays)

    lhs = jnp.concatenate([spread(8 * k + c) for k in range(3, 6) for c in range(3)] + [spread(48), spread(49)], axis=0)
    binned = dot_split(lhs, onehot, true)
    vel_own = [binned[16 * c:16 * c + 16] + binned[48 + 16 * c:64 + 16 * c] + binned[96 + 16 * c:112 + 16 * c] for c in range(3)]
    vel_own.append(binned[144:160] * 128.0 + binned[160:176])
    for c in range(4):
        keep_own(3 + c, vel_own[c])
    fill(vsend, range(3, 7), pack_vel, vel_arrays)
    vel_all = exchange(vsend, vrecv, send_sem, (vrecv_sem, vrecv_sem), vel_arrays)

    los = [bx, by, bz]

    def localise(fields, start):
        out = [[], [], []]
        for h in range(2):
            present = fields[0][h] != 0.0
            lane = iota((8, 128), 1) + 128 * h
            frame = [lane & 15, lane >> 4, iota((8, 128), 0) + start]
            for c in range(3):
                u = fields[c][h] - los[c].astype(F32) * BRICK
                u = jnp.where(u < -0.5 * BRICK, u + BOX, jnp.where(u >= 1.5 * BRICK, u - BOX, u))
                out[c].append(jnp.where(present, u, 64.0 + 4.0 * frame[c].astype(F32)))
        return out

    lane8 = iota((8, 128), 1)

    def put_rows(ref, k, h, x, inner):
        if inner:
            ref[k, pl.ds(8 + h, 8, stride=2), :] = x
        else:
            ref[k, pl.ds(24 + h, 4, stride=2), :] = x[0:4]
            ref[k, pl.ds(h, 4, stride=2), :] = x[4:8]

    def shift_in(s, local, inner):
        dx, dy = SHIFTS[s]
        left = 16 * dy + dx
        for c in range(3):
            a, b = local[c]
            if left:
                a, b = pltpu.roll(a, (-left) % 128, 1), pltpu.roll(b, (-left) % 128, 1)
                here = lane8 < 128 - left if left > 0 else lane8 >= -left
                a, b = jnp.where(here, a, b), jnp.where(here, b, a)
            put_rows(t_ref, 3 * s + c, 0, a, inner)
            put_rows(t_ref, 3 * s + c, 1, b, inner)

    def keep(f, inner_rows, outer_rows):
        for h in range(2):
            put_rows(q_ref, f, h, inner_rows[h], True)
            put_rows(q_ref, f, h, outer_rows[h], False)

    span = [4, 24]
    row8 = iota((8, 128), 0)

    def load(dx, dy, dz):
        s = SHIFTS.index((dx, dy))
        if span[0] is None:
            return [jnp.where(row8 < 4, t_ref[3 * s + c, 4 + 2 * dz:12 + 2 * dz, :], t_ref[3 * s + c, 20 + 2 * dz:28 + 2 * dz, :]) for c in range(3)]
        return [t_ref[3 * s + c, span[0] + 2 * dz:span[0] + 2 * dz + span[1], :] for c in range(3)]

    def low_x():
        return (iota((span[1], 128), 1) & 15) < 8

    def low_y():
        return ((iota((span[1], 128), 0) & 1) == 0) & (iota((span[1], 128), 1) < 96)

    def low_z():
        return row8 < 4 if span[0] is None else iota((span[1], 128), 0) + span[0] < 16

    def pick(mask, p, q):
        m = mask()
        return [jnp.where(m, p[c], q[c]) for c in range(3)]

    def half(dx, dy, dz):
        return dy > 0 or (dy == 0 and (dx > 0 or (dx == 0 and dz > 0)))

    offsets = [(dx, dy, dz) for dx, dy in SHIFTS for dz in range(-2, 3) if (dx, dy, dz) != (0, 0, 0) and (abs(dx) == 2) + (abs(dy) == 2) + (abs(dz) == 2) <= 1]
    first = [functools.partial(load, *d) for d in offsets if half(*d)]
    second = [functools.partial(load, *d) for d in offsets if not half(*d)]
    for dz in range(-1, 2):
        first.append(lambda dz=dz: pick(low_x, load(-2, 2, dz), load(2, 2, dz)))
        second.append(lambda dz=dz: pick(low_x, load(-2, -2, dz), load(2, -2, dz)))
    for dx in range(-1, 2):
        first.append(lambda dx=dx: pick(low_z, load(dx, 2, -2), load(dx, 2, 2)))
        second.append(lambda dx=dx: pick(low_z, load(dx, -2, -2), load(dx, -2, 2)))
    for dy in (1, -1):
        (first if dy == 1 else second).append(lambda dy=dy: pick(low_z, pick(low_x, load(-2, dy, -2), load(2, dy, -2)), pick(low_x, load(-2, dy, 2), load(2, dy, 2))))
    first.append(lambda: pick(low_z, load(2, 0, -2), load(2, 0, 2)))
    second.append(lambda: pick(low_z, load(-2, 0, -2), load(-2, 0, 2)))

    def apart(mine, nbr):
        ex, ey, ez = mine[0] - nbr[0], mine[1] - nbr[1], mine[2] - nbr[2]
        r2 = jnp.minimum(ex * ex + ey * ey + ez * ez, RCUT * RCUT)
        return ex, ey, ez, r2, lax.rsqrt(r2)

    def pair_energy(row):
        span[:] = [row, 8]
        mine = load(0, 0, 0)
        sw, sr = jnp.zeros((8, 128), F32), jnp.zeros((8, 128), F32)
        for i, nbr in enumerate(first):
            ex, ey, ez, r2, inv = apart(mine, nbr())
            i2 = inv * inv
            i6 = i2 * i2 * i2
            sw = sw + i6 * (i6 - 1.0)
            sr = sr + r2 * inv
        return 4.0 * sw - DU_CUT * sr + (RCUT * DU_CUT - U_CUT) * len(first)

    early = [s for s, (dx, dy) in enumerate(SHIFTS) if dy > 0 or (dy == 0 and dx >= 0)]
    late = [s for s in range(25) if s not in early]
    pos_all[0].wait_recv()
    parts = pos_parts(True, DELTAS[:3])
    inner = [merge_level(own_rows(c, 0, 8), parts[c]) for c in range(3)]
    inner_local = localise(inner, 0)
    for s in early:
        shift_in(s, inner_local, True)
    parts = pos_parts(False, DELTAS[:3])
    outer = [merge_level(own_rows(c, 8, 8), parts[c]) for c in range(3)]
    outer_local = localise(outer, 8)
    for s in early:
        shift_in(s, outer_local, False)
    middle = [pair_energy(8), pair_energy(16)]
    pos_all[1].wait_recv()
    parts = pos_parts(False, DELTAS[3:])
    outer = [merge_above(outer[c], parts[c]) for c in range(3)]
    outer_local = localise(outer, 8)
    for s in early:
        shift_in(s, outer_local, False)
    edges = pair_energy(None)
    span[:] = [4, 24]
    keep(0, inner[0], outer[0])
    lane24 = iota((24, 128), 1)
    x24 = lane24 & 15
    own = (((iota((24, 128), 0) & 1) == 0) | (lane24 < 64)) & (x24 >= 2) & (x24 < 14) & (q_ref[0, 4:28, :] != 0.0)
    energy = jnp.where(own, jnp.concatenate([edges[0:4]] + middle + [edges[4:8]], axis=0), 0.0)
    me = bz * 4 + by * 2 + bx
    ebuf[me, :, :] = energy[0:8] + energy[8:16] + energy[16:24]
    for delta in SEND_ORDER:
        pltpu.make_async_remote_copy(src_ref=ebuf.at[me], dst_ref=ebuf.at[me], send_sem=send_sem, recv_sem=erecv_sem, device_id=partner(delta), device_id_type=MESH_ID).start()
    energy_all = pltpu.make_async_remote_copy(src_ref=ebuf.at[pl.ds(0, 7)], dst_ref=ebuf.at[pl.ds(0, 7)], send_sem=send_sem, recv_sem=erecv_sem, device_id=partner(DELTAS[0]), device_id_type=MESH_ID)

    vel_all[2].wait_recv()
    for f, (a, b) in enumerate(vel_fields()):
        keep(3 + f, a, b)
    for c in range(1, 3):
        keep(c, inner[c], outer[c])

    for s in late:
        shift_in(s, inner_local, True)
        shift_in(s, outer_local, False)
    mine = load(0, 0, 0)

    def push(acc, ex, ey, ez, inv):
        i2 = inv * inv
        i6 = i2 * i2 * i2
        fr = (i6 * (i6 - 0.5)) * i2 + (DU_CUT / 48.0) * inv
        return (acc[0] + fr * ex, acc[1] + fr * ey, acc[2] + fr * ez)

    acc = tuple(jnp.zeros((24, 128), F32) for _ in range(3))
    for nbr in first + second:
        ex, ey, ez, r2, inv = apart(mine, nbr())
        acc = push(acc, ex, ey, ez, inv)
    force = [48.0 * acc[c] for c in range(3)]

    idv = jnp.where(own, q_ref[6, 4:28, :], -1.0)
    id_int = idv.astype(jnp.int32)
    id_hi = jnp.where(own, id_int >> 7, -1).astype(F32)
    id_lo = jnp.where(own, id_int & 127, -1).astype(F32)

    def flat(x, n):
        return jnp.concatenate([jnp.broadcast_to(x[r:r + 1, :], (n, 128)) for r in range(24)], axis=1)

    hot_hi = jnp.where(flat(id_hi, 128) == iota((128, 3072), 0).astype(F32), 1.0, 0.0).astype(BF16)
    lo_eq = flat(id_lo, 128) == iota((128, 3072), 0).astype(F32)
    hot_lo = jnp.where(lo_eq, 1.0, 0.0).astype(BF16)
    table = dot_split(hot_lo, hot_hi, true).astype(BF16)
    r128, c128 = iota((128, 128), 0), iota((128, 128), 1)
    below = dot_nn(jnp.where(c128 < r128, 1.0, 0.0).astype(BF16), table)
    total = dot_nn(jnp.ones((128, 128), BF16), table).astype(BF16)
    before = dot_nn(total, jnp.where(r128 < c128, 1.0, 0.0).astype(BF16))
    rank_tab = below + before
    tab_hi = jnp.floor(rank_tab * (1.0 / 256.0)) * 256.0
    tab_lo = rank_tab - tab_hi
    tabs = jnp.concatenate([tab_hi, tab_lo], axis=1).astype(BF16)
    hot2 = jnp.concatenate([hot_hi, hot_hi], axis=0)
    looked = jnp.concatenate([dot_nn(tabs, hot2[:, :1536]), dot_nn(tabs, hot2[:, 1536:])], axis=1)
    rank = jnp.sum(jnp.where(lo_eq, looked, 0.0), axis=0, keepdims=True)
    any_own = flat(jnp.where(own, 1.0, 0.0), 1) > 0.5
    rank_hi = jnp.floor(rank * (1.0 / 256.0))
    rank_lo = jnp.where(any_own, rank - 256.0 * rank_hi, -1.0)
    rank_hi = jnp.where(any_own, rank_hi, -1.0)

    hot_slot = jnp.where(jnp.broadcast_to(rank_lo, (256, 3072)) == iota((256, 3072), 0).astype(F32), 1.0, 0.0).astype(BF16)
    hi_mask = jnp.broadcast_to(rank_hi, (8, 3072)) == iota((8, 3072), 0).astype(F32)
    outs = []
    for c in range(3):
        outs += list(split3(q_ref[c, 4:28, :]))
    for c in range(3):
        outs += list(split3(q_ref[3 + c, 4:28, :] + (0.5 * TIME_STEP) * force[c]))
    for c in range(3):
        outs += list(split3(force[c]))
    outs += [id_hi, id_lo, jnp.where(own, 1.0, 0.0)]
    lhs = jnp.concatenate([jnp.where(hi_mask, flat(x, 8), 0.0) for x in outs], axis=0).astype(BF16)
    slots = dot_split(lhs, hot_slot, true)

    def field(i):
        return slots[8 * i:8 * i + 8, :]

    def put(ref, row, x):
        for h in range(7):
            n = 256 if h < 6 else CAP - 1536
            ref[row:row + 1, 256 * h:256 * h + n] = x[h:h + 1, 0:n].astype(ref.dtype)

    for c in range(3):
        put(opos_ref, c, field(3 * c) + field(3 * c + 1) + field(3 * c + 2))
        put(ovel_ref, c, field(9 + 3 * c) + field(10 + 3 * c) + field(11 + 3 * c))
        put(ofrc_ref, c, field(18 + 3 * c) + field(19 + 3 * c) + field(20 + 3 * c))
    put(oid_ref, 0, field(27) * 128.0 + field(28))
    put(oval_ref, 0, field(29))

    pltpu.make_async_remote_copy(src_ref=send_ref, dst_ref=send_ref, send_sem=send_sem, recv_sem=precv_sem, device_id=partner(DELTAS[0]), device_id_type=MESH_ID).wait_send()
    energy_all.wait_recv()
    acc = ebuf[0]
    for k in range(1, 8):
        acc = acc + ebuf[k]
    oen_ref[...] = acc


def finish(pos_ref, vel_ref, frc_ref, id_ref, val_ref, en_ref, opos_ref, ovel_ref, ofrc_ref, oid_ref, oval_ref, oen_ref):
    opos_ref[...] = pos_ref[...]
    ovel_ref[...] = vel_ref[...]
    ofrc_ref[...] = frc_ref[...]
    oid_ref[...] = id_ref[...].reshape(CAP)
    oval_ref[...] = val_ref[...].reshape(CAP)
    oen_ref[...] = jnp.sum(jnp.sum(en_ref[...], axis=0, keepdims=True), axis=1, keepdims=True)


def solution(mesh):
    row_spec = P(BRICK_AXES, None)
    flat_spec = P(BRICK_AXES)
    vmem = pl.BlockSpec(memory_space=pltpu.VMEM)

    def local_step(pos, vel, frc, ids, valid):
        f3 = jax.ShapeDtypeStruct((3, CAP), F32)
        i1 = jax.ShapeDtypeStruct((CAP,), jnp.int32)
        outs = pl.pallas_call(
            kernel,
            out_shape=(pltpu.VMEM((3, CAP), F32),) * 3 + (pltpu.VMEM((1, CAP), jnp.int32),) * 2 + (pltpu.VMEM((8, 128), F32),),
            in_specs=[pl.BlockSpec(memory_space=pltpu.HBM)] * 5,
            out_specs=(vmem,) * 6,
            scratch_shapes=[pltpu.VMEM((offsets_of(pos_arrays)[1] + offsets_of(vel_arrays)[1] + 56, 128), F32), pltpu.VMEM((offsets_of(pos_arrays)[1] + 16, 128), F32), pltpu.VMEM((offsets_of(vel_arrays)[1], 128), F32)] + [
                pltpu.VMEM((3, 3, CAP), F32),
                pltpu.VMEM((CAP,), jnp.int32),
                pltpu.VMEM((CAP,), jnp.int32),
                pltpu.SemaphoreType.DMA((3,)),
                pltpu.VMEM((56, KPAD), F32),
                pltpu.VMEM((2, 168, 128), F32),
                pltpu.VMEM((75, 32, 128), F32),
                pltpu.VMEM((NF, 32, 128), F32),
                pltpu.VMEM((8, 24, 128), F32),
                pltpu.VMEM((8, 8, 128), F32),
                pltpu.SemaphoreType.DMA,
                pltpu.SemaphoreType.DMA,
                pltpu.SemaphoreType.DMA,
                pltpu.SemaphoreType.DMA,
                pltpu.SemaphoreType.DMA,
            ],
            compiler_params=pltpu.CompilerParams(collective_id=0, has_side_effects=True),
        )(pos.T, vel.T, frc.T, ids, valid)
        outs = pl.pallas_call(
            finish,
            out_shape=(f3, f3, f3, i1, i1, jax.ShapeDtypeStruct((1, 1), F32)),
            in_specs=[vmem] * 6,
            out_specs=(vmem,) * 6,
            compiler_params=pltpu.CompilerParams(vmem_limit_bytes=4 << 20),
        )(*outs)
        return outs[0].T, outs[1].T, outs[2].T, outs[3], outs[4], outs[5][0, 0]

    return jax.shard_map(local_step, mesh=mesh, in_specs=(row_spec, row_spec, row_spec, flat_spec, flat_spec), out_specs=(row_spec, row_spec, row_spec, flat_spec, flat_spec, P()), check_vma=False)
```
